16 devices in a mesh: ep: 16 (over z, y, x, core).
Axes of the slice: x: 2, y: 2, z: 2, core: 2. Of those that a mesh axis runs over, the one named last changes fastest.
Arguments:
- x_tokens: bfloat16 [131072, 384], P('ep')
- w_router: float32 [384, 32], replicated
- expert_idx: int32 [131072], P('ep')
- w_in: bfloat16 [32, 384, 1536], P('ep')
- w_out: bfloat16 [32, 1536, 384], P('ep')
- grad_y: bfloat16 [131072, 384], P('ep')
Outputs:
- output 1: bfloat16 [131072, 384], P('ep')
- output 2: float32 [32, 384, 1536], P('ep')
- output 3: float32 [32, 1536, 384], P('ep')
- output 4: float32 [384, 32], replicated
- output 5: float32 [], replicated
- output 6: float32 [], replicated
All inputs are finite; a program needn't handle non-finite values.
Results may differ from the reference program's by a relative error of at most 0.0126676.
Values are sent between devices in bfloat16 or wider.
A program may use at most 1 GiB of HBM per device.

```python
import jax
import jax.numpy as jnp
from jax import lax

D = 384
FF = 1536
EXPERTS = 32
TOKENS = 8192
GROUPS = 16

CAPACITY = (5 * TOKENS + 4 * EXPERTS - 1) // (4 * EXPERTS)
TOTAL_TOK = GROUPS * TOKENS
N_SLOTS = EXPERTS * CAPACITY
AUX_WEIGHT = 0.01
Z_WEIGHT = 0.001
LOGIT_SCALE = 1.5


def draw_routes(route_key):
    key_perm, key_hot, key_tok = jax.random.split(route_key, 3)
    expert_perm = jax.random.permutation(key_perm, EXPERTS)
    hot_expert = jax.random.randint(key_hot, (GROUPS,), 0, EXPERTS)
    n_hot = TOKENS // 4
    n_rest = TOKENS - n_hot - EXPERTS

    def one_group(group_id):
        key_a, key_b, key_c = jax.random.split(jax.random.fold_in(key_tok, group_id), 3)
        first_pick = jax.random.randint(key_a, (n_rest,), 0, EXPERTS)
        second_pick = jax.random.randint(key_b, (n_rest,), 0, EXPERTS)
        skewed = expert_perm[jnp.minimum(first_pick, second_pick)].astype(jnp.int32)
        hot_rows = jnp.full((n_hot,), hot_expert[group_id], jnp.int32)
        listed = jnp.concatenate([hot_rows, jnp.arange(EXPERTS, dtype=jnp.int32), skewed])
        return listed[jax.random.permutation(key_c, TOKENS)]

    return jax.vmap(one_group)(jnp.arange(GROUPS)).reshape(TOTAL_TOK).astype(jnp.int32)


def setup_inputs(seed: int = 0) -> dict:
    base_key = jax.random.key(seed)
    key_x, key_router, key_in, key_out, key_gy, key_route = jax.random.split(base_key, 6)
    x_tokens = jax.random.normal(key_x, (TOTAL_TOK, D), jnp.float32).astype(jnp.bfloat16)
    w_router = jax.random.normal(key_router, (D, EXPERTS), jnp.float32) * (LOGIT_SCALE * D ** -0.5)
    w_in = (jax.random.normal(key_in, (EXPERTS, D, FF), jnp.float32) * D ** -0.5).astype(jnp.bfloat16)
    w_out = (jax.random.normal(key_out, (EXPERTS, FF, D), jnp.float32) * FF ** -0.5).astype(jnp.bfloat16)
    grad_y = jax.random.normal(key_gy, (TOTAL_TOK, D), jnp.float32).astype(jnp.bfloat16)
    expert_idx = draw_routes(key_route)
    return {'x_tokens': x_tokens, 'w_router': w_router, 'expert_idx': expert_idx, 'w_in': w_in, 'w_out': w_out, 'grad_y': grad_y}


def router_group(x_group, w_router, idx_group):
    logits = jnp.dot(x_group.astype(jnp.float32), w_router)
    router_prob = jax.nn.softmax(logits, axis=-1)
    log_norm = jax.nn.logsumexp(logits, axis=-1)
    onehot = (idx_group[:, None] == jnp.arange(EXPERTS)[None, :]).astype(jnp.int32)
    position = jnp.sum(jnp.cumsum(onehot, axis=0) * onehot, axis=1) - 1
    tok_slot = jnp.where(position < CAPACITY, idx_group * CAPACITY + position, N_SLOTS)
    onehot_f = onehot.astype(jnp.float32)
    gate_val = jnp.sum(router_prob * onehot_f, axis=-1)
    return router_prob, log_norm, onehot_f, gate_val, tok_slot


def reference(x_tokens, w_router, expert_idx, w_in, w_out, grad_y):
    x_groups = x_tokens.reshape(GROUPS, TOKENS, D)
    idx_groups = expert_idx.reshape(GROUPS, TOKENS)
    gy_groups = grad_y.reshape(GROUPS, TOKENS, D)

    def first_pass(operands):
        x_group, idx_group, gy_group = operands
        router_prob, log_norm, onehot_f, gate_val, tok_slot = router_group(x_group, w_router, idx_group)
        scaled = (gate_val[:, None] * gy_group.astype(jnp.float32)).astype(jnp.bfloat16)
        empty_buf = jnp.zeros((N_SLOTS + 1, D), jnp.bfloat16)
        sent_rows = empty_buf.at[tok_slot].set(x_group)[:N_SLOTS]
        sent_grad = empty_buf.at[tok_slot].set(scaled)[:N_SLOTS]
        route_stats = jnp.concatenate([jnp.sum(onehot_f, axis=0), jnp.sum(router_prob, axis=0), jnp.sum(log_norm * log_norm)[None]])
        return sent_rows, sent_grad, route_stats

    sent_rows, sent_grad, route_stats = lax.map(first_pass, (x_groups, idx_groups, gy_groups))
    rows_all = sent_rows.reshape(GROUPS, EXPERTS, CAPACITY, D).transpose(1, 0, 2, 3).reshape(EXPERTS, GROUPS * CAPACITY, D)
    grads_all = sent_grad.reshape(GROUPS, EXPERTS, CAPACITY, D).transpose(1, 0, 2, 3).reshape(EXPERTS, GROUPS * CAPACITY, D)

    def expert_pass(operands):
        recv_rows, recv_grad, w_first, w_second = operands
        pre_act = jnp.dot(recv_rows, w_first, preferred_element_type=jnp.float32)
        hidden = jnp.maximum(pre_act, 0.0).astype(jnp.bfloat16)
        expert_out = jnp.dot(hidden, w_second, preferred_element_type=jnp.float32).astype(jnp.bfloat16)
        d_hidden = jnp.dot(recv_grad, w_second.T, preferred_element_type=jnp.float32)
        d_pre = jnp.where(hidden > 0, d_hidden, 0.0).astype(jnp.bfloat16)
        grad_out_e = jnp.dot(hidden.T, recv_grad, preferred_element_type=jnp.float32)
        grad_in_e = jnp.dot(recv_rows.T, d_pre, preferred_element_type=jnp.float32)
        d_rows = jnp.dot(d_pre, w_first.T, preferred_element_type=jnp.float32).astype(jnp.bfloat16)
        return expert_out, d_rows, grad_in_e, grad_out_e

    expert_out, d_rows, grad_w_in, grad_w_out = lax.map(expert_pass, (rows_all, grads_all, w_in, w_out))
    out_groups = expert_out.reshape(EXPERTS, GROUPS, CAPACITY, D).transpose(1, 0, 2, 3).reshape(GROUPS, N_SLOTS, D)
    back_groups = d_rows.reshape(EXPERTS, GROUPS, CAPACITY, D).transpose(1, 0, 2, 3).reshape(GROUPS, N_SLOTS, D)

    totals = jnp.sum(route_stats, axis=0)
    load_frac = totals[:EXPERTS] / TOTAL_TOK
    mean_prob = totals[EXPERTS:2 * EXPERTS] / TOTAL_TOK
    aux_loss = AUX_WEIGHT * EXPERTS * jnp.sum(load_frac * mean_prob)
    z_loss = Z_WEIGHT * totals[2 * EXPERTS] / TOTAL_TOK
    aux_vec = AUX_WEIGHT * EXPERTS * load_frac / TOTAL_TOK
    z_coef = 2.0 * Z_WEIGHT / TOTAL_TOK
    pad_row = jnp.zeros((1, D), jnp.bfloat16)

    def second_pass(operands):
        x_group, idx_group, gy_group, out_group, back_group = operands
        router_prob, log_norm, onehot_f, gate_val, tok_slot = router_group(x_group, w_router, idx_group)
        out_tok = jnp.concatenate([out_group, pad_row])[tok_slot]
        back_tok = jnp.concatenate([back_group, pad_row])[tok_slot]
        d_gate = jnp.sum(out_tok.astype(jnp.float32) * gy_group.astype(jnp.float32), axis=-1)
        spread = jnp.sum(router_prob * aux_vec[None, :], axis=-1, keepdims=True)
        d_logits = ((gate_val * d_gate)[:, None] * (onehot_f - router_prob)
                    + router_prob * (aux_vec[None, :] - spread)
                    + (z_coef * log_norm)[:, None] * router_prob)
        grad_x = (back_tok.astype(jnp.float32) + jnp.dot(d_logits, w_router.T)).astype(jnp.bfloat16)
        part_router = jnp.dot(x_group.astype(jnp.float32).T, d_logits)
        return grad_x, part_router

    grad_x, parts_router = lax.map(second_pass, (x_groups, idx_groups, gy_groups, out_groups, back_groups))
    return grad_x.reshape(TOTAL_TOK, D), grad_w_in, grad_w_out, jnp.sum(parts_router, axis=0), aux_loss, z_loss
```

```python
import functools

import jax
import jax.numpy as jnp
from jax import lax
from jax.experimental import pallas as pl
from jax.experimental.pallas import tpu as pltpu
from jax.sharding import PartitionSpec as P

AUX_WEIGHT = 0.01
Z_WEIGHT = 0.001
MESH = pl.DeviceIdType.MESH
F_CHUNK = 512


def route_slots(idx_group, num_experts, capacity):
    tokens = idx_group.shape[0]
    n_slots = num_experts * capacity
    onehot = (idx_group[:, None] == jnp.arange(num_experts, dtype=jnp.int32)[None, :]).astype(jnp.int32)
    position = jnp.sum(jnp.cumsum(onehot, axis=0) * onehot, axis=1) - 1
    tok_slot = jnp.where(position < capacity, idx_group * capacity + position, n_slots)
    slot_tok = jnp.full((n_slots,), tokens, jnp.int32).at[tok_slot].set(jnp.arange(tokens, dtype=jnp.int32), mode='drop')
    return onehot.astype(jnp.float32), tok_slot, slot_tok


def gather_rows(source, row_index):
    return jnp.take(source, row_index, axis=0, mode='fill', fill_value=0)


def router_grad(router_prob, onehot, gate_val, d_gate, log_norm, aux_vec, z_coef):
    spread = jnp.sum(router_prob * aux_vec, axis=-1, keepdims=True)
    return ((gate_val * d_gate)[..., None] * (onehot - router_prob)
            + router_prob * (aux_vec - spread)
            + (z_coef * log_norm)[..., None] * router_prob)


def nt_dot(a, b):
    return lax.dot_general(a, b, (((1,), (1,)), ((), ())), preferred_element_type=jnp.float32)


def exchange_kernel(n, n_local, xd_ref, gate_ref, w_in_ref, w_out_ref,
                    gw_in_ref, gw_out_t_ref, back_ref, g_back_ref,
                    xr, gate_r, g_s,
                    fwd_send, fwd_recv, gate_send, gate_recv,
                    ret_send, ret_recv, g_send, g_recv, loc_sem):
    me = lax.axis_index('ep')
    cap, d_model = xr.shape[3], xr.shape[4]
    d_ff = w_in_ref.shape[2]

    def peer_of(k):
        out = 0
        bit = 1
        while bit < n:
            mine = (me // bit) % 2
            flip = (k // bit) % 2
            out = out + bit * (mine + flip - 2 * mine * flip)
            bit *= 2
        return out

    half = n // 2

    def rel_of(j):
        return (j % half) * 2 + j // half

    def fwd_copy(k, e, peer):
        return pltpu.make_async_remote_copy(
            src_ref=xd_ref.at[peer, e], dst_ref=xr.at[k, e],
            send_sem=fwd_send.at[k * n_local + e], recv_sem=fwd_recv.at[k * n_local + e],
            device_id=(peer,), device_id_type=MESH)

    def gate_copy(k, peer):
        return pltpu.make_async_remote_copy(
            src_ref=gate_ref.at[peer], dst_ref=gate_r.at[k],
            send_sem=gate_send.at[k], recv_sem=gate_recv.at[k],
            device_id=(peer,), device_id_type=MESH)

    def ret_copy(k, e, peer):
        return pltpu.make_async_remote_copy(
            src_ref=xr.at[k, e, 0], dst_ref=back_ref.at[me, e],
            send_sem=ret_send.at[k * n_local + e], recv_sem=ret_recv.at[k * n_local + e],
            device_id=(peer,), device_id_type=MESH)

    def g_copy(k, peer):
        return pltpu.make_async_remote_copy(
            src_ref=g_s.at[k], dst_ref=g_back_ref.at[me],
            send_sem=g_send.at[k], recv_sem=g_recv.at[k],
            device_id=(peer,), device_id_type=MESH)

    own_in = [pltpu.make_async_copy(xd_ref.at[me, e], xr.at[0, e], loc_sem.at[e]) for e in range(n_local)]
    own_gate = pltpu.make_async_copy(gate_ref.at[me], gate_r.at[0], loc_sem.at[n_local])
    for c in own_in:
        c.start()
    own_gate.start()

    def issue(j, carry):
        k = rel_of(j)
        peer = peer_of(k)
        gate_copy(k, peer).start()
        for e in range(n_local):
            fwd_copy(k, e, peer).start()
        return carry

    lax.fori_loop(1, n, issue, 0)

    gw_in_ref[...] = jnp.zeros_like(gw_in_ref)
    gw_out_t_ref[...] = jnp.zeros_like(gw_out_t_ref)
    g_s[...] = jnp.zeros_like(g_s)
    for c in own_in:
        c.wait()
    own_gate.wait()

    lanes = gate_r.shape[2]

    def tile(k, e):
        eye = (lax.broadcasted_iota(jnp.int32, (cap, lanes), 0)
               == lax.broadcasted_iota(jnp.int32, (cap, lanes), 1))
        rows = xr[k, e, 0]
        dy = xr[k, e, 1].astype(jnp.float32)
        gate_row = gate_r[k, pl.ds(e, 1), :]
        gate_col = jnp.sum(jnp.where(eye, gate_row, 0.0), axis=1, keepdims=True)
        grad = (gate_col * dy).astype(jnp.bfloat16)
        rows_t = rows.T
        grad_t = grad.T
        out = jnp.zeros((cap, d_model), jnp.float32)
        d_rows = jnp.zeros((cap, d_model), jnp.float32)
        for f in range(0, d_ff, F_CHUNK):
            fs = pl.ds(f, F_CHUNK)
            w_a = w_in_ref[e, :, fs]
            w_b = w_out_ref[e, fs, :]
            pre = jnp.dot(rows, w_a, preferred_element_type=jnp.float32)
            hid = jnp.maximum(pre, 0.0).astype(jnp.bfloat16)
            out = out + jnp.dot(hid, w_b, preferred_element_type=jnp.float32)
            d_hid = nt_dot(grad, w_b)
            d_pre = jnp.where(hid.astype(jnp.float32) > 0, d_hid, 0.0).astype(jnp.bfloat16)
            gw_out_t_ref[e, :, fs] += jnp.dot(grad_t, hid, preferred_element_type=jnp.float32)
            gw_in_ref[e, :, fs] += jnp.dot(rows_t, d_pre, preferred_element_type=jnp.float32)
            d_rows = d_rows + nt_dot(d_pre, w_a)
        out = out.astype(jnp.bfloat16).astype(jnp.float32)
        g_col = jnp.sum(out * dy, axis=1, keepdims=True)
        g_s[k, pl.ds(e, 1), :] = jnp.sum(jnp.where(eye, g_col, 0.0), axis=0, keepdims=True)
        xr[k, e, 0] = d_rows.astype(jnp.bfloat16)

    def step(t, carry):
        j = t // n_local
        e = t % n_local
        k = rel_of(j)
        peer = peer_of(k)

        @pl.when(j > 0)
        def _():
            @pl.when(e == 0)
            def _():
                gate_copy(k, peer).wait_recv()
            fwd_copy(k, e, peer).wait_recv()

        tile(k, e)

        @pl.when(j > 0)
        def _():
            ret_copy(k, e, peer).start()

            @pl.when(e == n_local - 1)
            def _():
                g_copy(k, peer).start()
        return carry

    lax.fori_loop(0, n * n_local, step, 0)

    own_out = [pltpu.make_async_copy(xr.at[0, e, 0], back_ref.at[me, e], loc_sem.at[e]) for e in range(n_local)]
    own_g = pltpu.make_async_copy(g_s.at[0], g_back_ref.at[me], loc_sem.at[n_local])
    for c in own_out:
        c.start()
    own_g.start()
    for c in own_out:
        c.wait()
    own_g.wait()

    def drain(j, carry):
        k = rel_of(j)
        peer = peer_of(k)
        gate_copy(k, peer).wait_send()
        g_copy(k, peer).wait()
        for e in range(n_local):
            fwd_copy(k, e, peer).wait_send()
            ret_copy(k, e, peer).wait()
        return carry

    lax.fori_loop(1, n, drain, 0)


def exchange(xd, gates, w_in, w_out, n_dev):
    n_local, d_model, d_ff = w_in.shape
    cap = xd.shape[3]
    lanes = gates.shape[2]
    any_spec = pl.BlockSpec(memory_space=pl.ANY)
    vmem_spec = pl.BlockSpec(memory_space=pltpu.VMEM)
    pairs = n_dev * n_local
    dma = pltpu.SemaphoreType.DMA
    return pl.pallas_call(
        functools.partial(exchange_kernel, n_dev, n_local),
        out_shape=(jax.ShapeDtypeStruct((n_local, d_model, d_ff), jnp.float32),
                   jax.ShapeDtypeStruct((n_local, d_model, d_ff), jnp.float32),
                   jax.ShapeDtypeStruct((n_dev, n_local, cap, d_model), jnp.bfloat16),
                   jax.ShapeDtypeStruct((n_dev, 8, lanes), jnp.float32)),
        in_specs=[any_spec, any_spec, vmem_spec, vmem_spec],
        out_specs=(vmem_spec, vmem_spec, any_spec, any_spec),
        scratch_shapes=[
            pltpu.VMEM((n_dev, n_local, 2, cap, d_model), jnp.bfloat16),
            pltpu.VMEM((n_dev, 8, lanes), jnp.float32),
            pltpu.VMEM((n_dev, 8, lanes), jnp.float32),
            dma((pairs,)), dma((pairs,)), dma((n_dev,)), dma((n_dev,)),
            dma((pairs,)), dma((pairs,)), dma((n_dev,)), dma((n_dev,)),
            dma((n_local + 1,)),
        ],
        compiler_params=pltpu.CompilerParams(has_side_effects=True, vmem_limit_bytes=60 * 1024 * 1024),
        name='exchange',
    )(xd, gates, w_in, w_out)


def solution(mesh):
    n_dev = mesh.shape['ep']

    def expert_layer(x_tokens, w_router, expert_idx, w_in, w_out, grad_y):
        tokens, d_model = x_tokens.shape
        n_local = w_in.shape[0]
        num_experts = n_local * n_dev
        capacity = (5 * tokens + 4 * num_experts - 1) // (4 * num_experts)
        total_tok = tokens * n_dev
        lanes = -(-capacity // 128) * 128
        onehot, tok_slot, slot_tok = route_slots(expert_idx, num_experts, capacity)
        logits = jnp.dot(x_tokens, w_router, preferred_element_type=jnp.float32)
        router_prob = jax.nn.softmax(logits, axis=-1)
        log_norm = jax.nn.logsumexp(logits, axis=-1)
        gate_val = jnp.sum(router_prob * onehot, axis=-1)
        route_stats = jnp.concatenate([jnp.sum(onehot, axis=0), jnp.sum(router_prob, axis=0), jnp.sum(log_norm * log_norm)[None]])
        route_stats = lax.psum(route_stats, 'ep')

        slot_shape = (n_dev, n_local, 1, capacity, d_model)
        xd = jnp.concatenate([gather_rows(x_tokens, slot_tok).reshape(slot_shape),
                              gather_rows(grad_y, slot_tok).reshape(slot_shape)], axis=2)
        gate_slot = gather_rows(gate_val, slot_tok).reshape(n_dev, n_local, capacity)
        gates = jnp.pad(gate_slot, ((0, 0), (0, 8 - n_local), (0, lanes - capacity)))
        grad_w_in, grad_w_out_t, back, g_back = exchange(xd, gates, w_in, w_out, n_dev)
        grad_w_out = jnp.swapaxes(grad_w_out_t, 1, 2)
        d_gate = gather_rows(g_back[:, :n_local, :capacity].reshape(num_experts * capacity), tok_slot)
        dx_expert = gather_rows(back.reshape(num_experts * capacity, d_model), tok_slot)

        load_frac = route_stats[:num_experts] / total_tok
        mean_prob = route_stats[num_experts:2 * num_experts] / total_tok
        aux_loss = AUX_WEIGHT * num_experts * jnp.sum(load_frac * mean_prob)
        z_loss = Z_WEIGHT * route_stats[2 * num_experts] / total_tok
        aux_vec = AUX_WEIGHT * num_experts * load_frac / total_tok
        d_logits = router_grad(router_prob, onehot, gate_val, d_gate, log_norm, aux_vec, 2.0 * Z_WEIGHT / total_tok)
        dx_router = jnp.einsum('se,de->sd', d_logits, w_router)
        grad_x = (dx_expert.astype(jnp.float32) + dx_router).astype(jnp.bfloat16)
        grad_w_router = lax.psum(jnp.einsum('sd,se->de', x_tokens, d_logits, preferred_element_type=jnp.float32), 'ep')
        return grad_x, grad_w_in, grad_w_out, grad_w_router, aux_loss, z_loss

    return jax.shard_map(expert_layer, mesh=mesh,
                         in_specs=(P('ep', None), P(None, None), P('ep'), P('ep', None, None), P('ep', None, None), P('ep', None)),
                         out_specs=(P('ep', None), P('ep', None, None), P('ep', None, None), P(None, None), P(), P()),
                         check_vma=False)
```

```python
import functools

import jax
import jax.numpy as jnp
from jax import lax
from jax.experimental import pallas as pl
from jax.experimental.pallas import tpu as pltpu
from jax.sharding import PartitionSpec as P

AUX_WEIGHT = 0.01
Z_WEIGHT = 0.001
MESH = pl.DeviceIdType.MESH
F_CHUNK = 512
TOKEN_BLOCK = 256
UNROLL = 16


def route_slots(onehot, idx_group, capacity):
    tokens, num_experts = onehot.shape
    blocks = tokens // TOKEN_BLOCK
    chosen = onehot.reshape(blocks, TOKEN_BLOCK, num_experts)
    lower = jnp.tril(jnp.ones((TOKEN_BLOCK, TOKEN_BLOCK), jnp.bfloat16))
    within = jnp.einsum('ij,bje->bie', lower, chosen.astype(jnp.bfloat16), preferred_element_type=jnp.float32)
    totals = within[:, -1, :]
    before = (jnp.arange(blocks)[:, None] > jnp.arange(blocks)[None, :]).astype(jnp.float32)
    base = jnp.sum(before[:, :, None] * totals[None, :, :], axis=1)
    position = jnp.sum((within + base[:, None, :]) * chosen, axis=-1).reshape(tokens).astype(jnp.int32) - 1
    return jnp.where(position < capacity, idx_group * capacity + position, num_experts * capacity), base[-1] + totals[-1]


def dispatch_kernel(blocks, capacity, slot_ref, x_ref, dy_ref, gate_ref, xd_ref, gates_ref, table, stage):
    step = pl.program_id(0)
    d_model = x_ref.shape[1]
    cols = d_model // 128
    lanes = gates_ref.shape[2]
    n_local = xd_ref.shape[1]

    @pl.when(step == 0)
    def _():
        def clear(i, carry):
            table[pl.ds(pl.multiple_of(i * 512, 512), 512), :] = jnp.zeros((512, 128), jnp.float32)
            return carry
        lax.fori_loop(0, table.shape[0] // 512, clear, 0)

    @pl.when(step < blocks)
    def _():
        for c in range(cols):
            stage[pl.ds(c, TOKEN_BLOCK, stride=8), :] = x_ref[:, c * 128:(c + 1) * 128].astype(jnp.float32)
            stage[pl.ds(cols + c, TOKEN_BLOCK, stride=8), :] = dy_ref[:, c * 128:(c + 1) * 128].astype(jnp.float32)
        stage[pl.ds(2 * cols, TOKEN_BLOCK, stride=8), :] = gate_ref[...]

        def place(i, carry):
            for u in range(UNROLL):
                t = i * UNROLL + u
                slot = slot_ref[step * TOKEN_BLOCK + t]
                table[pl.ds(pl.multiple_of(slot * 8, 8), 8), :] = stage[pl.ds(pl.multiple_of(t * 8, 8), 8), :]
            return carry
        lax.fori_loop(0, TOKEN_BLOCK // UNROLL, place, 0)

    @pl.when(step >= blocks)
    def _():
        dst = step - blocks
        gates_ref[...] = jnp.zeros_like(gates_ref)
        for e in range(n_local):
            first = (dst * n_local + e) * (capacity * 8)
            for c in range(cols):
                xd_ref[0, e, 0, :, c * 128:(c + 1) * 128] = table[pl.ds(first + c, capacity, stride=8), :].astype(jnp.bfloat16)
                xd_ref[0, e, 1, :, c * 128:(c + 1) * 128] = table[pl.ds(first + cols + c, capacity, stride=8), :].astype(jnp.bfloat16)
            gate = table[pl.ds(first + 2 * cols, capacity, stride=8), :]
            row = lax.broadcasted_iota(jnp.int32, (capacity, 128), 0)
            lane = lax.broadcasted_iota(jnp.int32, (capacity, 128), 1)
            for c in range(lanes // 128):
                gates_ref[0, e:e + 1, c * 128:(c + 1) * 128] = jnp.sum(
                    jnp.where(row == lane + c * 128, gate, 0.0), axis=0, keepdims=True)


def dispatch(tok_slot, x_tokens, grad_y, gate_rows, n_dev, n_local, capacity, lanes):
    tokens, d_model = x_tokens.shape
    blocks = tokens // TOKEN_BLOCK
    n_slots = n_dev * n_local * capacity
    table_rows = -(-(n_slots + 1) * 8 // 512) * 512
    tok = lambda i: (jnp.minimum(i, blocks - 1), 0)
    dst = lambda i: jnp.maximum(i - blocks, 0)
    return pl.pallas_call(
        functools.partial(dispatch_kernel, blocks, capacity),
        grid=(blocks + n_dev,),
        out_shape=(jax.ShapeDtypeStruct((n_dev, n_local, 2, capacity, d_model), jnp.bfloat16),
                   jax.ShapeDtypeStruct((n_dev, 8, lanes), jnp.float32)),
        in_specs=[pl.BlockSpec(memory_space=pltpu.SMEM),
                  pl.BlockSpec((TOKEN_BLOCK, d_model), tok),
                  pl.BlockSpec((TOKEN_BLOCK, d_model), tok),
                  pl.BlockSpec((TOKEN_BLOCK, 128), tok)],
        out_specs=(pl.BlockSpec((1, n_local, 2, capacity, d_model), lambda i: (dst(i), 0, 0, 0, 0)),
                   pl.BlockSpec((1, 8, lanes), lambda i: (dst(i), 0, 0))),
        scratch_shapes=[pltpu.VMEM((table_rows, 128), jnp.float32),
                        pltpu.VMEM((TOKEN_BLOCK * 8, 128), jnp.float32)],
        compiler_params=pltpu.CompilerParams(dimension_semantics=('arbitrary',), vmem_limit_bytes=60 * 1024 * 1024),
        name='dispatch',
    )(tok_slot, x_tokens, grad_y, gate_rows)


def split3(v):
    hi = v.astype(jnp.bfloat16)
    rest = v - hi.astype(jnp.float32)
    mid = rest.astype(jnp.bfloat16)
    low = (rest - mid.astype(jnp.float32)).astype(jnp.bfloat16)
    return hi, mid, low


def combine_kernel(sources, capacity, slot_ref, back_ref, g_ref, x_ref, ohg_ref, p_ref, zp_ref, aux_ref, wr_t_ref, gwi_ref, gwo_t_ref,
                   gx_ref, gwr_ref, gwi_out_ref, gwo_out_ref, table, stage):
    step = pl.program_id(0)
    d_model = x_ref.shape[1]
    cols = d_model // 128
    n_local = back_ref.shape[1]
    num_experts = p_ref.shape[1]
    n_slots = sources * n_local * capacity
    gwi_out_ref[...] = gwi_ref[...]
    gwo_out_ref[0] = gwo_t_ref[0].T

    @pl.when(step == 0)
    def _():
        table[pl.ds(n_slots * 8, 8), :] = jnp.zeros((8, 128), jnp.float32)
        gwr_ref[...] = jnp.zeros_like(gwr_ref)

    @pl.when(step < sources)
    def _():
        lanes = g_ref.shape[2]
        eye = (lax.broadcasted_iota(jnp.int32, (capacity, lanes), 0)
               == lax.broadcasted_iota(jnp.int32, (capacity, lanes), 1))
        for e in range(n_local):
            first = (step * n_local + e) * (capacity * 8)
            for c in range(cols):
                table[pl.ds(first + c, capacity, stride=8), :] = back_ref[0, e, :, c * 128:(c + 1) * 128].astype(jnp.float32)
            g_col = jnp.sum(jnp.where(eye, g_ref[0, e:e + 1, :], 0.0), axis=1, keepdims=True)
            table[pl.ds(first + cols, capacity, stride=8), :] = jnp.broadcast_to(g_col, (capacity, 128))

    @pl.when(step >= sources)
    def _():
        block = step - sources

        def pick(i, carry):
            for u in range(UNROLL):
                t = i * UNROLL + u
                slot = slot_ref[block * TOKEN_BLOCK + t]
                stage[pl.ds(pl.multiple_of(t * 8, 8), 8), :] = table[pl.ds(pl.multiple_of(slot * 8, 8), 8), :]
            return carry
        lax.fori_loop(0, TOKEN_BLOCK // UNROLL, pick, 0)
        g_tok = stage[pl.ds(cols, TOKEN_BLOCK, stride=8), :][:, :num_experts]
        prob = p_ref[...]
        aux_vec = aux_ref[0:1, :]
        spread = jnp.sum(prob * aux_vec, axis=1, keepdims=True)
        d_logits = g_tok * ohg_ref[...] + prob * (aux_vec - spread) + zp_ref[...]
        hi, mid, low = split3(d_logits)
        left = jnp.concatenate([hi, mid, hi, low, mid, hi], axis=1)
        dx_router = jnp.dot(left, wr_t_ref[...], preferred_element_type=jnp.float32)
        for c in range(cols):
            part = slice(c * 128, (c + 1) * 128)
            gx_ref[:, part] = (stage[pl.ds(c, TOKEN_BLOCK, stride=8), :] + dx_router[:, part]).astype(jnp.bfloat16)
        parts = jnp.concatenate([hi, mid, low, jnp.zeros_like(hi)], axis=1)
        gwr_ref[...] += lax.dot_general(parts, x_ref[...], (((0,), (0,)), ((), ())), preferred_element_type=jnp.float32)


def combine(tok_slot, back, g_back, x_tokens, ohg, prob, zp, aux_vec, w_router, gw_in, gw_out_t):
    n_dev, n_local, capacity, d_model = back.shape
    tokens = x_tokens.shape[0]
    num_experts = prob.shape[1]
    d_ff = gw_in.shape[2]
    blocks = tokens // TOKEN_BLOCK
    steps = n_dev + blocks
    lanes = g_back.shape[2]
    n_slots = n_dev * n_local * capacity
    round_bf16 = lambda v: lax.reduce_precision(v, 8, 7)
    w_hi = round_bf16(w_router.T)
    w_mid = round_bf16(w_router.T - w_hi)
    w_low = w_router.T - w_hi - w_mid
    wr_t = jnp.concatenate([w_hi, w_hi, w_mid, w_hi, w_mid, w_low], axis=0).astype(jnp.bfloat16)
    gw_in_rows = gw_in.reshape(n_local * d_model, d_ff)
    in_rows = n_local * d_model // steps
    out_cols = d_ff // 128
    src = lambda i: jnp.minimum(i, n_dev - 1)
    tok = lambda i: (jnp.maximum(i - n_dev, 0), 0)
    flip = lambda i: jnp.minimum(i, n_local * out_cols - 1)
    gx, gwr, gw_in_out, gw_out = pl.pallas_call(
        functools.partial(combine_kernel, n_dev, capacity),
        grid=(steps,),
        out_shape=(jax.ShapeDtypeStruct((tokens, d_model), jnp.bfloat16),
                   jax.ShapeDtypeStruct((4 * num_experts, d_model), jnp.float32),
                   jax.ShapeDtypeStruct((n_local * d_model, d_ff), jnp.float32),
                   jax.ShapeDtypeStruct((n_local, d_ff, d_model), jnp.float32)),
        in_specs=[pl.BlockSpec(memory_space=pltpu.SMEM),
                  pl.BlockSpec((1, n_local, capacity, d_model), lambda i: (src(i), 0, 0, 0)),
                  pl.BlockSpec((1, 8, lanes), lambda i: (src(i), 0, 0)),
                  pl.BlockSpec((TOKEN_BLOCK, d_model), tok),
                  pl.BlockSpec((TOKEN_BLOCK, num_experts), tok),
                  pl.BlockSpec((TOKEN_BLOCK, num_experts), tok),
                  pl.BlockSpec((TOKEN_BLOCK, num_experts), tok),
                  pl.BlockSpec((8, num_experts), lambda i: (0, 0)),
                  pl.BlockSpec((6 * num_experts, d_model), lambda i: (0, 0)),
                  pl.BlockSpec((in_rows, d_ff), lambda i: (i, 0)),
                  pl.BlockSpec((1, d_model, 128), lambda i: (flip(i) // out_cols, 0, flip(i) % out_cols))],
        out_specs=(pl.BlockSpec((TOKEN_BLOCK, d_model), tok),
                   pl.BlockSpec((4 * num_experts, d_model), lambda i: (0, 0)),
                   pl.BlockSpec((in_rows, d_ff), lambda i: (i, 0)),
                   pl.BlockSpec((1, 128, d_model), lambda i: (flip(i) // out_cols, flip(i) % out_cols, 0))),
        scratch_shapes=[pltpu.VMEM(((n_slots + 1) * 8, 128), jnp.float32),
                        pltpu.VMEM((TOKEN_BLOCK * 8, 128), jnp.float32)],
        compiler_params=pltpu.CompilerParams(dimension_semantics=('arbitrary',), vmem_limit_bytes=60 * 1024 * 1024),
        name='combine',
    )(tok_slot, back, g_back, x_tokens, ohg, prob, zp, jnp.broadcast_to(aux_vec, (8, num_experts)), wr_t, gw_in_rows, gw_out_t)
    part = gwr.reshape(4, num_experts, d_model)
    return gx, (part[0] + part[1] + part[2]).T, gw_in_out.reshape(n_local, d_model, d_ff), gw_out


def flip_bits(me, k, n):
    out = 0
    bit = 1
    while bit < n:
        mine = (me // bit) % 2
        flip = (k // bit) % 2
        out = out + bit * (mine + flip - 2 * mine * flip)
        bit *= 2
    return out


def total_kernel(n, part_ref, out_ref, inbox, mine, a_send, a_recv, b_send, b_recv):
    me = lax.axis_index('ep')

    def scatter(k):
        peer = flip_bits(me, k, n)
        return pltpu.make_async_remote_copy(src_ref=part_ref.at[peer], dst_ref=inbox.at[me], send_sem=a_send.at[k],
                                            recv_sem=a_recv.at[k], device_id=(peer,), device_id_type=MESH)

    def spread(k):
        peer = flip_bits(me, k, n)
        return pltpu.make_async_remote_copy(src_ref=mine, dst_ref=out_ref.at[me], send_sem=b_send.at[k],
                                            recv_sem=b_recv.at[k], device_id=(peer,), device_id_type=MESH)

    for k in range(1, n):
        scatter(k).start()
    inbox[me] = part_ref[me]
    for k in range(1, n):
        scatter(k).wait_recv()
    total = inbox[0]
    for i in range(1, n):
        total = total + inbox[i]
    mine[...] = total
    out_ref[me] = total
    for k in range(1, n):
        spread(k).start()
    for k in range(1, n):
        scatter(k).wait_send()
        spread(k).wait()


def total(part, n_dev):
    rows, cols = part.shape
    piece = rows * cols // (n_dev * 128)
    chunks = jnp.pad(part.reshape(n_dev, piece, 128), ((0, 0), (0, -piece % 8), (0, 0)))
    dma = pltpu.SemaphoreType.DMA
    vmem_spec = pl.BlockSpec(memory_space=pltpu.VMEM)
    out = pl.pallas_call(
        functools.partial(total_kernel, n_dev),
        out_shape=jax.ShapeDtypeStruct(chunks.shape, jnp.float32),
        in_specs=[vmem_spec],
        out_specs=vmem_spec,
        scratch_shapes=[pltpu.VMEM(chunks.shape, jnp.float32), pltpu.VMEM(chunks.shape[1:], jnp.float32),
                        dma((n_dev,)), dma((n_dev,)), dma((n_dev,)), dma((n_dev,))],
        compiler_params=pltpu.CompilerParams(has_side_effects=True),
        name='total',
    )(chunks)
    return out[:, :piece].reshape(rows, cols)


def nt_dot(a, b):
    return lax.dot_general(a, b, (((1,), (1,)), ((), ())), preferred_element_type=jnp.float32)


def exchange_kernel(n, n_local, xd_ref, gate_ref, stat_ref, w_in_ref, w_out_ref,
                    gw_in_ref, gw_out_t_ref, back_ref, g_back_ref, stat_out_ref,
                    xr, gate_r, g_s, stat_r,
                    fwd_send, fwd_recv, gate_send, gate_recv,
                    ret_send, ret_recv, g_send, g_recv, stat_send, stat_recv, loc_sem):
    me = lax.axis_index('ep')
    cap, d_model = xr.shape[3], xr.shape[4]
    d_ff = w_in_ref.shape[2]

    def peer_of(k):
        return flip_bits(me, k, n)

    half = n // 2

    def rel_of(j):
        return (j % half) * 2 + j // half

    def fwd_copy(k, e, peer):
        return pltpu.make_async_remote_copy(
            src_ref=xd_ref.at[peer, e], dst_ref=xr.at[k, e],
            send_sem=fwd_send.at[k * n_local + e], recv_sem=fwd_recv.at[k * n_local + e],
            device_id=(peer,), device_id_type=MESH)

    def gate_copy(k, peer):
        return pltpu.make_async_remote_copy(
            src_ref=gate_ref.at[peer], dst_ref=gate_r.at[k],
            send_sem=gate_send.at[k], recv_sem=gate_recv.at[k],
            device_id=(peer,), device_id_type=MESH)

    def ret_copy(k, e, peer):
        return pltpu.make_async_remote_copy(
            src_ref=xr.at[k, e, 0], dst_ref=back_ref.at[me, e],
            send_sem=ret_send.at[k * n_local + e], recv_sem=ret_recv.at[k * n_local + e],
            device_id=(peer,), device_id_type=MESH)

    def g_copy(k, peer):
        return pltpu.make_async_remote_copy(
            src_ref=g_s.at[k], dst_ref=g_back_ref.at[me],
            send_sem=g_send.at[k], recv_sem=g_recv.at[k],
            device_id=(peer,), device_id_type=MESH)

    def stat_copy(k, peer):
        return pltpu.make_async_remote_copy(
            src_ref=stat_ref, dst_ref=stat_r.at[me],
            send_sem=stat_send.at[k], recv_sem=stat_recv.at[k],
            device_id=(peer,), device_id_type=MESH)

    own_in = [pltpu.make_async_copy(xd_ref.at[me, e], xr.at[0, e], loc_sem.at[e]) for e in range(n_local)]
    own_gate = pltpu.make_async_copy(gate_ref.at[me], gate_r.at[0], loc_sem.at[n_local])
    for c in own_in:
        c.start()
    own_gate.start()

    def issue(j, carry):
        k = rel_of(j)
        peer = peer_of(k)
        gate_copy(k, peer).start()
        stat_copy(k, peer).start()
        for e in range(n_local):
            fwd_copy(k, e, peer).start()
        return carry

    lax.fori_loop(1, n, issue, 0)

    gw_in_ref[...] = jnp.zeros_like(gw_in_ref)
    gw_out_t_ref[...] = jnp.zeros_like(gw_out_t_ref)
    g_s[...] = jnp.zeros_like(g_s)
    stat_r[me] = stat_ref[...]
    for c in own_in:
        c.wait()
    own_gate.wait()

    lanes = gate_r.shape[2]

    def tile(k, e):
        eye = (lax.broadcasted_iota(jnp.int32, (cap, lanes), 0)
               == lax.broadcasted_iota(jnp.int32, (cap, lanes), 1))
        rows = xr[k, e, 0]
        dy = xr[k, e, 1].astype(jnp.float32)
        gate_row = gate_r[k, pl.ds(e, 1), :]
        gate_col = jnp.sum(jnp.where(eye, gate_row, 0.0), axis=1, keepdims=True)
        grad = (gate_col * dy).astype(jnp.bfloat16)
        rows_t = rows.T
        grad_t = grad.T
        out = jnp.zeros((cap, d_model), jnp.float32)
        d_rows = jnp.zeros((cap, d_model), jnp.float32)
        for f in range(0, d_ff, F_CHUNK):
            fs = pl.ds(f, F_CHUNK)
            w_a = w_in_ref[e, :, fs]
            w_b = w_out_ref[e, fs, :]
            pre = jnp.dot(rows, w_a, preferred_element_type=jnp.float32)
            hid = jnp.maximum(pre, 0.0).astype(jnp.bfloat16)
            out = out + jnp.dot(hid, w_b, preferred_element_type=jnp.float32)
            d_hid = nt_dot(grad, w_b)
            d_pre = jnp.where(hid.astype(jnp.float32) > 0, d_hid, 0.0).astype(jnp.bfloat16)
            gw_out_t_ref[e, :, fs] += jnp.dot(grad_t, hid, preferred_element_type=jnp.float32)
            gw_in_ref[e, :, fs] += jnp.dot(rows_t, d_pre, preferred_element_type=jnp.float32)
            d_rows = d_rows + nt_dot(d_pre, w_a)
        out = out.astype(jnp.bfloat16).astype(jnp.float32)
        g_col = jnp.sum(out * dy, axis=1, keepdims=True)
        g_s[k, pl.ds(e, 1), :] = jnp.sum(jnp.where(eye, g_col, 0.0), axis=0, keepdims=True)
        xr[k, e, 0] = d_rows.astype(jnp.bfloat16)

    def step(t, carry):
        j = t // n_local
        e = t % n_local
        k = rel_of(j)
        peer = peer_of(k)

        @pl.when(j > 0)
        def _():
            @pl.when(e == 0)
            def _():
                gate_copy(k, peer).wait_recv()
            fwd_copy(k, e, peer).wait_recv()

        tile(k, e)

        @pl.when(j > 0)
        def _():
            ret_copy(k, e, peer).start()

            @pl.when(e == n_local - 1)
            def _():
                g_copy(k, peer).start()
        return carry

    lax.fori_loop(0, n * n_local, step, 0)

    own_out = [pltpu.make_async_copy(xr.at[0, e, 0], back_ref.at[me, e], loc_sem.at[e]) for e in range(n_local)]
    own_g = pltpu.make_async_copy(g_s.at[0], g_back_ref.at[me], loc_sem.at[n_local])
    for c in own_out:
        c.start()
    own_g.start()
    for c in own_out:
        c.wait()
    own_g.wait()

    def drain(j, carry):
        k = rel_of(j)
        peer = peer_of(k)
        gate_copy(k, peer).wait_send()
        stat_copy(k, peer).wait()
        g_copy(k, peer).wait()
        for e in range(n_local):
            fwd_copy(k, e, peer).wait_send()
            ret_copy(k, e, peer).wait()
        return carry

    lax.fori_loop(1, n, drain, 0)
    stat = stat_r[0]
    for i in range(1, n):
        stat = stat + stat_r[i]
    stat_out_ref[...] = stat


def exchange(xd, gates, stats, w_in, w_out, n_dev):
    n_local, d_model, d_ff = w_in.shape
    cap = xd.shape[3]
    lanes = gates.shape[2]
    any_spec = pl.BlockSpec(memory_space=pl.ANY)
    vmem_spec = pl.BlockSpec(memory_space=pltpu.VMEM)
    pairs = n_dev * n_local
    dma = pltpu.SemaphoreType.DMA
    return pl.pallas_call(
        functools.partial(exchange_kernel, n_dev, n_local),
        out_shape=(jax.ShapeDtypeStruct((n_local, d_model, d_ff), jnp.float32),
                   jax.ShapeDtypeStruct((n_local, d_model, d_ff), jnp.float32),
                   jax.ShapeDtypeStruct((n_dev, n_local, cap, d_model), jnp.bfloat16),
                   jax.ShapeDtypeStruct((n_dev, 8, lanes), jnp.float32),
                   jax.ShapeDtypeStruct(stats.shape, jnp.float32)),
        in_specs=[any_spec, any_spec, vmem_spec, vmem_spec, vmem_spec],
        out_specs=(vmem_spec, vmem_spec, any_spec, any_spec, vmem_spec),
        scratch_shapes=[
            pltpu.VMEM((n_dev, n_local, 2, cap, d_model), jnp.bfloat16),
            pltpu.VMEM((n_dev, 8, lanes), jnp.float32),
            pltpu.VMEM((n_dev, 8, lanes), jnp.float32),
            pltpu.VMEM((n_dev,) + stats.shape, jnp.float32),
            dma((pairs,)), dma((pairs,)), dma((n_dev,)), dma((n_dev,)),
            dma((pairs,)), dma((pairs,)), dma((n_dev,)), dma((n_dev,)),
            dma((n_dev,)), dma((n_dev,)), dma((n_local + 1,)),
        ],
        compiler_params=pltpu.CompilerParams(has_side_effects=True, vmem_limit_bytes=60 * 1024 * 1024),
        name='exchange',
    )(xd, gates, stats, w_in, w_out)


def solution(mesh):
    n_dev = mesh.shape['ep']

    def expert_layer(x_tokens, w_router, expert_idx, w_in, w_out, grad_y):
        tokens, d_model = x_tokens.shape
        n_local = w_in.shape[0]
        num_experts = n_local * n_dev
        capacity = (5 * tokens + 4 * num_experts - 1) // (4 * num_experts)
        total_tok = tokens * n_dev
        lanes = -(-capacity // 128) * 128
        onehot = (expert_idx[:, None] == jnp.arange(num_experts, dtype=jnp.int32)[None, :]).astype(jnp.float32)
        tok_slot, load = route_slots(onehot, expert_idx, capacity)
        logits = jnp.dot(x_tokens, w_router, preferred_element_type=jnp.float32)
        router_prob = jax.nn.softmax(logits, axis=-1)
        log_norm = jax.nn.logsumexp(logits, axis=-1, keepdims=True)
        gate_val = jnp.sum(router_prob * onehot, axis=-1, keepdims=True)
        stats = jnp.concatenate([load, jnp.sum(router_prob, axis=0), jnp.sum(log_norm * log_norm)[None]])
        stats = jnp.pad(stats[None], ((0, 7), (0, 128 - stats.shape[0])))
        xd, gates = dispatch(tok_slot, x_tokens, grad_y, jnp.broadcast_to(gate_val, (tokens, 128)), n_dev, n_local, capacity, lanes)
        gw_in, gw_out_t, back, g_back, stats = exchange(xd, gates, stats, w_in, w_out, n_dev)

        load_frac = stats[0, :num_experts] / total_tok
        mean_prob = stats[0, num_experts:2 * num_experts] / total_tok
        aux_loss = AUX_WEIGHT * num_experts * jnp.sum(load_frac * mean_prob)
        z_loss = Z_WEIGHT * stats[0, 2 * num_experts] / total_tok
        aux_vec = AUX_WEIGHT * num_experts * load_frac / total_tok
        ohg = gate_val * (onehot - router_prob)
        zp = (2.0 * Z_WEIGHT / total_tok * log_norm) * router_prob
        grad_x, part, grad_w_in, grad_w_out = combine(tok_slot, back, g_back, x_tokens, ohg, router_prob, zp, aux_vec, w_router, gw_in, gw_out_t)
        grad_w_router = total(part, n_dev)
        return grad_x, grad_w_in, grad_w_out, grad_w_router, aux_loss, z_loss

    return jax.shard_map(expert_layer, mesh=mesh,
                         in_specs=(P('ep', None), P(None, None), P('ep'), P('ep', None, None), P('ep', None, None), P('ep', None)),
                         out_specs=(P('ep', None), P('ep', None, None), P('ep', None, None), P(None, None), P(), P()),
                         check_vma=False)
```

```python
import functools

import jax
import jax.numpy as jnp
from jax import lax
from jax.experimental import pallas as pl
from jax.experimental.pallas import tpu as pltpu
from jax.sharding import PartitionSpec as P

AUX_WEIGHT = 0.01
Z_WEIGHT = 0.001
MESH = pl.DeviceIdType.MESH
F_CHUNK = 512
TOKEN_BLOCK = 256
UNROLL = 16


def route_slots(onehot, idx_group, capacity):
    tokens, num_experts = onehot.shape
    blocks = tokens // TOKEN_BLOCK
    chosen = onehot.reshape(blocks, TOKEN_BLOCK, num_experts)
    lower = jnp.tril(jnp.ones((TOKEN_BLOCK, TOKEN_BLOCK), jnp.bfloat16))
    within = jnp.einsum('ij,bje->bie', lower, chosen.astype(jnp.bfloat16), preferred_element_type=jnp.float32)
    totals = within[:, -1, :]
    before = (jnp.arange(blocks)[:, None] > jnp.arange(blocks)[None, :]).astype(jnp.float32)
    base = jnp.sum(before[:, :, None] * totals[None, :, :], axis=1)
    position = jnp.sum((within + base[:, None, :]) * chosen, axis=-1).reshape(tokens).astype(jnp.int32) - 1
    return jnp.where(position < capacity, idx_group * capacity + position, num_experts * capacity), base[-1] + totals[-1]


def dispatch_kernel(blocks, capacity, slot_ref, x_ref, dy_ref, gate_ref, xd_ref, gates_ref, table, stage):
    step = pl.program_id(0)
    d_model = x_ref.shape[1]
    cols = d_model // 128
    lanes = gates_ref.shape[2]
    n_local = xd_ref.shape[1]

    @pl.when(step == 0)
    def _():
        def clear(i, carry):
            table[pl.ds(pl.multiple_of(i * 512, 512), 512), :] = jnp.zeros((512, 128), jnp.float32)
            return carry
        lax.fori_loop(0, table.shape[0] // 512, clear, 0)

    @pl.when(step < blocks)
    def _():
        for c in range(cols):
            stage[pl.ds(c, TOKEN_BLOCK, stride=8), :] = x_ref[:, c * 128:(c + 1) * 128].astype(jnp.float32)
            stage[pl.ds(cols + c, TOKEN_BLOCK, stride=8), :] = dy_ref[:, c * 128:(c + 1) * 128].astype(jnp.float32)
        stage[pl.ds(2 * cols, TOKEN_BLOCK, stride=8), :] = gate_ref[...]

        def place(i, carry):
            for u in range(UNROLL):
                t = i * UNROLL + u
                slot = slot_ref[step * TOKEN_BLOCK + t]
                table[pl.ds(pl.multiple_of(slot * 8, 8), 8), :] = stage[pl.ds(pl.multiple_of(t * 8, 8), 8), :]
            return carry
        lax.fori_loop(0, TOKEN_BLOCK // UNROLL, place, 0)

    @pl.when(step >= blocks)
    def _():
        dst = step - blocks
        gates_ref[...] = jnp.zeros_like(gates_ref)
        for e in range(n_local):
            first = (dst * n_local + e) * (capacity * 8)
            for c in range(cols):
                xd_ref[0, e, 0, :, c * 128:(c + 1) * 128] = table[pl.ds(first + c, capacity, stride=8), :].astype(jnp.bfloat16)
                xd_ref[0, e, 1, :, c * 128:(c + 1) * 128] = table[pl.ds(first + cols + c, capacity, stride=8), :].astype(jnp.bfloat16)
            gate = table[pl.ds(first + 2 * cols, capacity, stride=8), :]
            row = lax.broadcasted_iota(jnp.int32, (capacity, 128), 0)
            lane = lax.broadcasted_iota(jnp.int32, (capacity, 128), 1)
            for c in range(lanes // 128):
                gates_ref[0, e:e + 1, c * 128:(c + 1) * 128] = jnp.sum(
                    jnp.where(row == lane + c * 128, gate, 0.0), axis=0, keepdims=True)


def dispatch(tok_slot, x_tokens, grad_y, gate_rows, n_dev, n_local, capacity, lanes):
    tokens, d_model = x_tokens.shape
    blocks = tokens // TOKEN_BLOCK
    n_slots = n_dev * n_local * capacity
    table_rows = -(-(n_slots + 1) * 8 // 512) * 512
    tok = lambda i: (jnp.minimum(i, blocks - 1), 0)
    dst = lambda i: jnp.maximum(i - blocks, 0)
    return pl.pallas_call(
        functools.partial(dispatch_kernel, blocks, capacity),
        grid=(blocks + n_dev,),
        out_shape=(jax.ShapeDtypeStruct((n_dev, n_local, 2, capacity, d_model), jnp.bfloat16),
                   jax.ShapeDtypeStruct((n_dev, 8, lanes), jnp.float32)),
        in_specs=[pl.BlockSpec(memory_space=pltpu.SMEM),
                  pl.BlockSpec((TOKEN_BLOCK, d_model), tok),
                  pl.BlockSpec((TOKEN_BLOCK, d_model), tok),
                  pl.BlockSpec((TOKEN_BLOCK, 128), tok)],
        out_specs=(pl.BlockSpec((1, n_local, 2, capacity, d_model), lambda i: (dst(i), 0, 0, 0, 0)),
                   pl.BlockSpec((1, 8, lanes), lambda i: (dst(i), 0, 0))),
        scratch_shapes=[pltpu.VMEM((table_rows, 128), jnp.float32),
                        pltpu.VMEM((TOKEN_BLOCK * 8, 128), jnp.float32)],
        compiler_params=pltpu.CompilerParams(dimension_semantics=('arbitrary',), vmem_limit_bytes=60 * 1024 * 1024),
        name='dispatch',
    )(tok_slot, x_tokens, grad_y, gate_rows)


def split3(v):
    hi = v.astype(jnp.bfloat16)
    rest = v - hi.astype(jnp.float32)
    mid = rest.astype(jnp.bfloat16)
    low = (rest - mid.astype(jnp.float32)).astype(jnp.bfloat16)
    return hi, mid, low


def combine_kernel(sources, capacity, slot_ref, back_ref, g_ref, x_ref, ohg_ref, p_ref, zp_ref, aux_ref, wr_t_ref, gwi_ref, gwo_t_ref,
                   gx_ref, gwr_ref, gwi_out_ref, gwo_out_ref, table, stage):
    step = pl.program_id(0)
    d_model = x_ref.shape[1]
    cols = d_model // 128
    n_local = back_ref.shape[1]
    num_experts = p_ref.shape[1]
    n_slots = sources * n_local * capacity
    gwi_out_ref[...] = gwi_ref[...]
    gwo_out_ref[0] = gwo_t_ref[0].T

    @pl.when(step == 0)
    def _():
        table[pl.ds(n_slots * 8, 8), :] = jnp.zeros((8, 128), jnp.float32)
        gwr_ref[...] = jnp.zeros_like(gwr_ref)

    @pl.when(step < sources)
    def _():
        lanes = g_ref.shape[2]
        eye = (lax.broadcasted_iota(jnp.int32, (capacity, lanes), 0)
               == lax.broadcasted_iota(jnp.int32, (capacity, lanes), 1))
        for e in range(n_local):
            first = (step * n_local + e) * (capacity * 8)
            for c in range(cols):
                table[pl.ds(first + c, capacity, stride=8), :] = back_ref[0, e, :, c * 128:(c + 1) * 128].astype(jnp.float32)
            g_col = jnp.sum(jnp.where(eye, g_ref[0, e:e + 1, :], 0.0), axis=1, keepdims=True)
            table[pl.ds(first + cols, capacity, stride=8), :] = jnp.broadcast_to(g_col, (capacity, 128))

    @pl.when(step >= sources)
    def _():
        block = step - sources

        def pick(i, carry):
            for u in range(UNROLL):
                t = i * UNROLL + u
                slot = slot_ref[block * TOKEN_BLOCK + t]
                stage[pl.ds(pl.multiple_of(t * 8, 8), 8), :] = table[pl.ds(pl.multiple_of(slot * 8, 8), 8), :]
            return carry
        lax.fori_loop(0, TOKEN_BLOCK // UNROLL, pick, 0)
        g_tok = stage[pl.ds(cols, TOKEN_BLOCK, stride=8), :][:, :num_experts]
        prob = p_ref[...]
        aux_vec = aux_ref[0:1, :]
        spread = jnp.sum(prob * aux_vec, axis=1, keepdims=True)
        d_logits = g_tok * ohg_ref[...] + prob * (aux_vec - spread) + zp_ref[...]
        hi, mid, low = split3(d_logits)
        left = jnp.concatenate([hi, mid, hi, low, mid, hi], axis=1)
        dx_router = jnp.dot(left, wr_t_ref[...], preferred_element_type=jnp.float32)
        for c in range(cols):
            part = slice(c * 128, (c + 1) * 128)
            gx_ref[:, part] = (stage[pl.ds(c, TOKEN_BLOCK, stride=8), :] + dx_router[:, part]).astype(jnp.bfloat16)
        parts = jnp.concatenate([hi, mid, low, jnp.zeros_like(hi)], axis=1)
        gwr_ref[...] += lax.dot_general(parts, x_ref[...], (((0,), (0,)), ((), ())), preferred_element_type=jnp.float32)


def combine(tok_slot, back, g_back, x_tokens, ohg, prob, zp, aux_vec, w_router, gw_in, gw_out_t):
    n_dev, n_local, capacity, d_model = back.shape
    tokens = x_tokens.shape[0]
    num_experts = prob.shape[1]
    d_ff = gw_in.shape[2]
    blocks = tokens // TOKEN_BLOCK
    steps = n_dev + blocks
    lanes = g_back.shape[2]
    n_slots = n_dev * n_local * capacity
    round_bf16 = lambda v: lax.reduce_precision(v, 8, 7)
    w_hi = round_bf16(w_router.T)
    w_mid = round_bf16(w_router.T - w_hi)
    w_low = w_router.T - w_hi - w_mid
    wr_t = jnp.concatenate([w_hi, w_hi, w_mid, w_hi, w_mid, w_low], axis=0).astype(jnp.bfloat16)
    gw_in_rows = gw_in.reshape(n_local * d_model, d_ff)
    in_rows = n_local * d_model // steps
    out_cols = d_ff // 128
    src = lambda i: jnp.minimum(i, n_dev - 1)
    tok = lambda i: (jnp.maximum(i - n_dev, 0), 0)
    flip = lambda i: jnp.minimum(i, n_local * out_cols - 1)
    gx, gwr, gw_in_out, gw_out = pl.pallas_call(
        functools.partial(combine_kernel, n_dev, capacity),
        grid=(steps,),
        out_shape=(jax.ShapeDtypeStruct((tokens, d_model), jnp.bfloat16),
                   jax.ShapeDtypeStruct((4 * num_experts, d_model), jnp.float32),
                   jax.ShapeDtypeStruct((n_local * d_model, d_ff), jnp.float32),
                   jax.ShapeDtypeStruct((n_local, d_ff, d_model), jnp.float32)),
        in_specs=[pl.BlockSpec(memory_space=pltpu.SMEM),
                  pl.BlockSpec((1, n_local, capacity, d_model), lambda i: (src(i), 0, 0, 0)),
                  pl.BlockSpec((1, 8, lanes), lambda i: (src(i), 0, 0)),
                  pl.BlockSpec((TOKEN_BLOCK, d_model), tok),
                  pl.BlockSpec((TOKEN_BLOCK, num_experts), tok),
                  pl.BlockSpec((TOKEN_BLOCK, num_experts), tok),
                  pl.BlockSpec((TOKEN_BLOCK, num_experts), tok),
                  pl.BlockSpec((8, num_experts), lambda i: (0, 0)),
                  pl.BlockSpec((6 * num_experts, d_model), lambda i: (0, 0)),
                  pl.BlockSpec((in_rows, d_ff), lambda i: (i, 0)),
                  pl.BlockSpec((1, d_model, 128), lambda i: (flip(i) // out_cols, 0, flip(i) % out_cols))],
        out_specs=(pl.BlockSpec((TOKEN_BLOCK, d_model), tok),
                   pl.BlockSpec((4 * num_experts, d_model), lambda i: (0, 0)),
                   pl.BlockSpec((in_rows, d_ff), lambda i: (i, 0)),
                   pl.BlockSpec((1, 128, d_model), lambda i: (flip(i) // out_cols, flip(i) % out_cols, 0))),
        scratch_shapes=[pltpu.VMEM(((n_slots + 1) * 8, 128), jnp.float32),
                        pltpu.VMEM((TOKEN_BLOCK * 8, 128), jnp.float32)],
        compiler_params=pltpu.CompilerParams(dimension_semantics=('arbitrary',), vmem_limit_bytes=60 * 1024 * 1024),
        name='combine',
    )(tok_slot, back, g_back, x_tokens, ohg, prob, zp, jnp.broadcast_to(aux_vec, (8, num_experts)), wr_t, gw_in_rows, gw_out_t)
    part = gwr.reshape(4, num_experts, d_model)
    return gx, (part[0] + part[1] + part[2]).T, gw_in_out.reshape(n_local, d_model, d_ff), gw_out


def flip_bits(me, k, n):
    out = 0
    bit = 1
    while bit < n:
        mine = (me // bit) % 2
        flip = (k // bit) % 2
        out = out + bit * (mine + flip - 2 * mine * flip)
        bit *= 2
    return out


def total_kernel(n, part_ref, out_ref, inbox, mine, a_send, a_recv, b_send, b_recv):
    me = lax.axis_index('ep')

    def scatter(k):
        peer = flip_bits(me, k, n)
        return pltpu.make_async_remote_copy(src_ref=part_ref.at[peer], dst_ref=inbox.at[me], send_sem=a_send.at[k],
                                            recv_sem=a_recv.at[k], device_id=(peer,), device_id_type=MESH)

    def spread(k):
        peer = flip_bits(me, k, n)
        return pltpu.make_async_remote_copy(src_ref=mine, dst_ref=out_ref.at[me], send_sem=b_send.at[k],
                                            recv_sem=b_recv.at[k], device_id=(peer,), device_id_type=MESH)

    for k in range(1, n):
        scatter(k).start()
    inbox[me] = part_ref[me]
    for k in range(1, n):
        scatter(k).wait_recv()
    total = inbox[0]
    for i in range(1, n):
        total = total + inbox[i]
    mine[...] = total
    out_ref[me] = total
    for k in range(1, n):
        spread(k).start()
    for k in range(1, n):
        scatter(k).wait_send()
        spread(k).wait()


def total(part, n_dev):
    rows, cols = part.shape
    piece = rows * cols // (n_dev * 128)
    chunks = jnp.pad(part.reshape(n_dev, piece, 128), ((0, 0), (0, -piece % 8), (0, 0)))
    dma = pltpu.SemaphoreType.DMA
    vmem_spec = pl.BlockSpec(memory_space=pltpu.VMEM)
    out = pl.pallas_call(
        functools.partial(total_kernel, n_dev),
        out_shape=jax.ShapeDtypeStruct(chunks.shape, jnp.float32),
        in_specs=[vmem_spec],
        out_specs=vmem_spec,
        scratch_shapes=[pltpu.VMEM(chunks.shape, jnp.float32), pltpu.VMEM(chunks.shape[1:], jnp.float32),
                        dma((n_dev,)), dma((n_dev,)), dma((n_dev,)), dma((n_dev,))],
        compiler_params=pltpu.CompilerParams(has_side_effects=True),
        name='total',
    )(chunks)
    return out[:, :piece].reshape(rows, cols)


def nt_dot(a, b):
    return lax.dot_general(a, b, (((1,), (1,)), ((), ())), preferred_element_type=jnp.float32)


def tile_at(t):
    quarter = t // 4
    edge = (7 - quarter) // 7 + quarter // 7
    turn = (t + 4) % 8
    piece = (1 - edge) * (turn // 2) + edge * (t % 4)
    stage = (t + 4) // 8
    chip = stage * (7 - stage) // 2 + stage // 4
    chip = chip + (1 - edge) * (turn % 2) * (7 - 2 * chip)
    return chip * 2 + piece // 2, piece % 2


def link_sets(n, n_local):
    assert n == 16
    pieces = []
    for chips in ((3, 4), (5, 2), (6, 1), (7,)):
        pieces.append([[(chip * 2 + c, e) for c in range(2) for e in range(n_local)] for chip in chips])
    return pieces


def exchange_kernel(n, n_local, xd_ref, gate_ref, stat_ref, w_in_ref, w_out_ref,
                    gw_in_ref, gw_out_t_ref, back_ref, g_back_ref, stat_out_ref,
                    xr, gate_r, g_s, stat_r,
                    fwd_send, fwd_recv, gate_send, gate_recv,
                    ret_send, ret_recv, g_send, g_recv, stat_send, stat_recv, loc_sem):
    me = lax.axis_index('ep')
    cap, d_model = xr.shape[3], xr.shape[4]
    d_ff = w_in_ref.shape[2]

    def peer_of(k):
        return flip_bits(me, k, n)

    def fwd_copy(k, e, part):
        sem = (k * n_local + e) * 2 + part
        peer = peer_of(k)
        return pltpu.make_async_remote_copy(
            src_ref=xd_ref.at[peer, e, part], dst_ref=xr.at[k, e, part],
            send_sem=fwd_send.at[sem], recv_sem=fwd_recv.at[sem],
            device_id=(peer,), device_id_type=MESH)

    def gate_copy(k):
        peer = peer_of(k)
        return pltpu.make_async_remote_copy(
            src_ref=gate_ref.at[peer], dst_ref=gate_r.at[k],
            send_sem=gate_send.at[k], recv_sem=gate_recv.at[k],
            device_id=(peer,), device_id_type=MESH)

    def stat_copy(k):
        return pltpu.make_async_remote_copy(
            src_ref=stat_ref, dst_ref=stat_r.at[me],
            send_sem=stat_send.at[k], recv_sem=stat_recv.at[k],
            device_id=(peer_of(k),), device_id_type=MESH)

    def ret_copy(k, e):
        sem = k * n_local + e
        return pltpu.make_async_remote_copy(
            src_ref=xr.at[k, e, 0], dst_ref=back_ref.at[me, e],
            send_sem=ret_send.at[sem], recv_sem=ret_recv.at[sem],
            device_id=(peer_of(k),), device_id_type=MESH)

    def g_copy(k):
        return pltpu.make_async_remote_copy(
            src_ref=g_s.at[k], dst_ref=g_back_ref.at[me],
            send_sem=g_send.at[k], recv_sem=g_recv.at[k],
            device_id=(peer_of(k),), device_id_type=MESH)

    sets = link_sets(n, n_local)

    def interleave(queues):
        return [queue[i] for i in range(len(queues[0])) for queue in queues]

    def send_rows(queues):
        for k, e in interleave(queues):
            if e == 0:
                gate_copy(k).start()
                stat_copy(k).start()
            for part in range(2):
                fwd_copy(k, e, part).start()

    def rows_left(queues):
        for queue in queues:
            for i, (k, e) in enumerate(queue):
                fwd_copy(k, e, 0).wait_send()
                if i < len(queue) - 1:
                    fwd_copy(k, e, 1).wait_send()

    def send_grads(queues):
        for k, e in interleave(queues):
            ret_copy(k, e).start()
            if e == n_local - 1:
                g_copy(k).start()

    def grads_left(queues):
        for queue in queues:
            for k, e in queue[:-1]:
                ret_copy(k, e).wait_send()

    near = [[(1, e) for e in range(n_local)]]
    own_in = [pltpu.make_async_copy(xd_ref.at[me, e], xr.at[0, e], loc_sem.at[e]) for e in range(n_local)]
    own_gate = pltpu.make_async_copy(gate_ref.at[me], gate_r.at[0], loc_sem.at[n_local])
    own_out = [pltpu.make_async_copy(xr.at[0, e, 0], back_ref.at[me, e], loc_sem.at[e]) for e in range(n_local)]
    own_g = pltpu.make_async_copy(g_s.at[0], g_back_ref.at[me], loc_sem.at[n_local])

    send_rows(sets[0])
    send_rows(near)
    for c in own_in:
        c.start()
    own_gate.start()
    gw_in_ref[...] = jnp.zeros_like(gw_in_ref)
    gw_out_t_ref[...] = jnp.zeros_like(gw_out_t_ref)
    g_s[...] = jnp.zeros_like(g_s)
    stat_r[me] = stat_ref[...]
    for c in own_in:
        c.wait()
    own_gate.wait()

    lanes = gate_r.shape[2]

    def tile(k, e):
        eye = (lax.broadcasted_iota(jnp.int32, (cap, lanes), 0)
               == lax.broadcasted_iota(jnp.int32, (cap, lanes), 1))
        rows = xr[k, e, 0]
        dy = xr[k, e, 1].astype(jnp.float32)
        gate_row = gate_r[k, pl.ds(e, 1), :]
        gate_col = jnp.sum(jnp.where(eye, gate_row, 0.0), axis=1, keepdims=True)
        grad = (gate_col * dy).astype(jnp.bfloat16)
        rows_t = rows.T
        grad_t = grad.T
        out = jnp.zeros((cap, d_model), jnp.float32)
        d_rows = jnp.zeros((cap, d_model), jnp.float32)
        for f in range(0, d_ff, F_CHUNK):
            fs = pl.ds(f, F_CHUNK)
            w_a = w_in_ref[e, :, fs]
            w_b = w_out_ref[e, fs, :]
            pre = jnp.dot(rows, w_a, preferred_element_type=jnp.float32)
            hid = jnp.maximum(pre, 0.0).astype(jnp.bfloat16)
            out = out + jnp.dot(hid, w_b, preferred_element_type=jnp.float32)
            d_hid = nt_dot(grad, w_b)
            d_pre = jnp.where(hid.astype(jnp.float32) > 0, d_hid, 0.0).astype(jnp.bfloat16)
            gw_out_t_ref[e, :, fs] += jnp.dot(grad_t, hid, preferred_element_type=jnp.float32)
            gw_in_ref[e, :, fs] += jnp.dot(rows_t, d_pre, preferred_element_type=jnp.float32)
            d_rows = d_rows + nt_dot(d_pre, w_a)
        out = out.astype(jnp.bfloat16).astype(jnp.float32)
        g_col = jnp.sum(out * dy, axis=1, keepdims=True)
        g_s[k, pl.ds(e, 1), :] = jnp.sum(jnp.where(eye, g_col, 0.0), axis=0, keepdims=True)
        xr[k, e, 0] = d_rows.astype(jnp.bfloat16)

    order = [(0, e) for e in range(n_local)] + near[0]
    first = []
    for queues in sets:
        first.append(len(order))
        order = order + interleave(queues)
    assert order == [tile_at(t) for t in range(len(order))]

    def own_back():
        send_grads(near)
        for c in own_out:
            c.start()
        own_g.start()

    def after_rows(done, then):
        def run():
            rows_left(sets[done])
            then()
        return run

    def after_grads(done, then):
        def run():
            grads_left(sets[done])
            then()
        return run

    events = {
        first[0]: own_back,
        first[1] - 2: after_rows(0, lambda: send_rows(sets[1])),
        first[2] - 2: after_rows(1, lambda: send_grads(sets[0])),
        first[2]: after_grads(0, lambda: send_rows(sets[2])),
        first[3] - 2: after_rows(2, lambda: send_grads(sets[1])),
        first[3]: after_grads(1, lambda: send_rows(sets[3])),
        len(order) - 1: after_rows(3, lambda: send_grads(sets[2])),
    }

    def step(t, carry):
        k, e = tile_at(t)
        for at, run in events.items():
            pl.when(t == at)(run)

        @pl.when(t >= n_local)
        def _():
            @pl.when(e == 0)
            def _():
                gate_copy(k).wait_recv()
            for part in range(2):
                fwd_copy(k, e, part).wait_recv()

        tile(k, e)
        return carry

    lax.fori_loop(0, len(order), step, 0)
    grads_left(sets[2])
    send_grads(sets[3])

    for queues in sets:
        for queue in queues:
            k, e = queue[-1]
            fwd_copy(k, e, 1).wait_send()
            if queues is not sets[3]:
                ret_copy(k, e).wait_send()
    grads_left(sets[3])
    for queue in sets[3]:
        ret_copy(*queue[-1]).wait_send()
    for k, e in near[0]:
        for part in range(2):
            fwd_copy(k, e, part).wait_send()
        ret_copy(k, e).wait_send()
    for c in own_out:
        c.wait()
    own_g.wait()

    def drain(k, carry):
        gate_copy(k).wait_send()
        stat_copy(k).wait()
        g_copy(k).wait()
        for e in range(n_local):
            ret_copy(k, e).wait_recv()
        return carry

    lax.fori_loop(1, n, drain, 0)
    stat = stat_r[0]
    for i in range(1, n):
        stat = stat + stat_r[i]
    stat_out_ref[...] = stat


def exchange(xd, gates, stats, w_in, w_out, n_dev):
    n_local, d_model, d_ff = w_in.shape
    cap = xd.shape[3]
    lanes = gates.shape[2]
    any_spec = pl.BlockSpec(memory_space=pl.ANY)
    vmem_spec = pl.BlockSpec(memory_space=pltpu.VMEM)
    pairs = n_dev * n_local
    dma = pltpu.SemaphoreType.DMA
    return pl.pallas_call(
        functools.partial(exchange_kernel, n_dev, n_local),
        out_shape=(jax.ShapeDtypeStruct((n_local, d_model, d_ff), jnp.float32),
                   jax.ShapeDtypeStruct((n_local, d_model, d_ff), jnp.float32),
                   jax.ShapeDtypeStruct((n_dev, n_local, cap, d_model), jnp.bfloat16),
                   jax.ShapeDtypeStruct((n_dev, 8, lanes), jnp.float32),
                   jax.ShapeDtypeStruct(stats.shape, jnp.float32)),
        in_specs=[any_spec, any_spec, vmem_spec, vmem_spec, vmem_spec],
        out_specs=(vmem_spec, vmem_spec, any_spec, any_spec, vmem_spec),
        scratch_shapes=[
            pltpu.VMEM((n_dev, n_local, 2, cap, d_model), jnp.bfloat16),
            pltpu.VMEM((n_dev, 8, lanes), jnp.float32),
            pltpu.VMEM((n_dev, 8, lanes), jnp.float32),
            pltpu.VMEM((n_dev,) + stats.shape, jnp.float32),
            dma((2 * pairs,)), dma((2 * pairs,)), dma((n_dev,)), dma((n_dev,)),
            dma((pairs,)), dma((pairs,)), dma((n_dev,)), dma((n_dev,)),
            dma((n_dev,)), dma((n_dev,)), dma((n_local + 1,)),
        ],
        compiler_params=pltpu.CompilerParams(has_side_effects=True, vmem_limit_bytes=60 * 1024 * 1024),
        name='exchange',
    )(xd, gates, stats, w_in, w_out)


def solution(mesh):
    n_dev = mesh.shape['ep']

    def expert_layer(x_tokens, w_router, expert_idx, w_in, w_out, grad_y):
        tokens, d_model = x_tokens.shape
        n_local = w_in.shape[0]
        num_experts = n_local * n_dev
        capacity = (5 * tokens + 4 * num_experts - 1) // (4 * num_experts)
        total_tok = tokens * n_dev
        lanes = -(-capacity // 128) * 128
        onehot = (expert_idx[:, None] == jnp.arange(num_experts, dtype=jnp.int32)[None, :]).astype(jnp.float32)
        tok_slot, load = route_slots(onehot, expert_idx, capacity)
        logits = jnp.dot(x_tokens, w_router, preferred_element_type=jnp.float32)
        router_prob = jax.nn.softmax(logits, axis=-1)
        log_norm = jax.nn.logsumexp(logits, axis=-1, keepdims=True)
        gate_val = jnp.sum(router_prob * onehot, axis=-1, keepdims=True)
        stats = jnp.concatenate([load, jnp.sum(router_prob, axis=0), jnp.sum(log_norm * log_norm)[None]])
        stats = jnp.pad(stats[None], ((0, 7), (0, 128 - stats.shape[0])))
        xd, gates = dispatch(tok_slot, x_tokens, grad_y, jnp.broadcast_to(gate_val, (tokens, 128)), n_dev, n_local, capacity, lanes)
        gw_in, gw_out_t, back, g_back, stats = exchange(xd, gates, stats, w_in, w_out, n_dev)

        load_frac = stats[0, :num_experts] / total_tok
        mean_prob = stats[0, num_experts:2 * num_experts] / total_tok
        aux_loss = AUX_WEIGHT * num_experts * jnp.sum(load_frac * mean_prob)
        z_loss = Z_WEIGHT * stats[0, 2 * num_experts] / total_tok
        aux_vec = AUX_WEIGHT * num_experts * load_frac / total_tok
        ohg = gate_val * (onehot - router_prob)
        zp = (2.0 * Z_WEIGHT / total_tok * log_norm) * router_prob
        grad_x, part, grad_w_in, grad_w_out = combine(tok_slot, back, g_back, x_tokens, ohg, router_prob, zp, aux_vec, w_router, gw_in, gw_out_t)
        grad_w_router = total(part, n_dev)
        return grad_x, grad_w_in, grad_w_out, grad_w_router, aux_loss, z_loss

    return jax.shard_map(expert_layer, mesh=mesh,
                         in_specs=(P('ep', None), P(None, None), P('ep'), P('ep', None, None), P('ep', None, None), P('ep', None)),
                         out_specs=(P('ep', None), P('ep', None, None), P('ep', None, None), P(None, None), P(), P()),
                         check_vma=False)
```

```python
import functools

import jax
import jax.numpy as jnp
from jax import lax
from jax.experimental import pallas as pl
from jax.experimental.pallas import tpu as pltpu
from jax.sharding import PartitionSpec as P

AUX_WEIGHT = 0.01
Z_WEIGHT = 0.001
MESH = pl.DeviceIdType.MESH
F_CHUNK = 512
TOKEN_BLOCK = 256
UNROLL = 16


def route_slots(onehot, idx_group, capacity):
    tokens, num_experts = onehot.shape
    blocks = tokens // TOKEN_BLOCK
    chosen = onehot.reshape(blocks, TOKEN_BLOCK, num_experts)
    lower = jnp.tril(jnp.ones((TOKEN_BLOCK, TOKEN_BLOCK), jnp.bfloat16))
    within = jnp.einsum('ij,bje->bie', lower, chosen.astype(jnp.bfloat16), preferred_element_type=jnp.float32)
    totals = within[:, -1, :]
    before = (jnp.arange(blocks)[:, None] > jnp.arange(blocks)[None, :]).astype(jnp.float32)
    base = jnp.sum(before[:, :, None] * totals[None, :, :], axis=1)
    position = jnp.sum((within + base[:, None, :]) * chosen, axis=-1).reshape(tokens).astype(jnp.int32) - 1
    return jnp.where(position < capacity, idx_group * capacity + position, num_experts * capacity), base[-1] + totals[-1]


def split3(v):
    hi = v.astype(jnp.bfloat16)
    rest = v - hi.astype(jnp.float32)
    mid = rest.astype(jnp.bfloat16)
    low = (rest - mid.astype(jnp.float32)).astype(jnp.bfloat16)
    return hi, mid, low


def combine_kernel(sources, capacity, slot_ref, back_ref, g_ref, x_ref, ohg_ref, p_ref, zp_ref, aux_ref, wr_t_ref, gwi_ref, gwo_t_ref,
                   gx_ref, gwr_ref, gwi_out_ref, gwo_out_ref, table, stage):
    step = pl.program_id(0)
    d_model = x_ref.shape[1]
    cols = d_model // 128
    n_local = back_ref.shape[1]
    num_experts = p_ref.shape[1]
    n_slots = sources * n_local * capacity
    gwi_out_ref[...] = gwi_ref[...]
    gwo_out_ref[0] = gwo_t_ref[0].T

    @pl.when(step == 0)
    def _():
        table[pl.ds(n_slots * 8, 8), :] = jnp.zeros((8, 128), jnp.float32)
        gwr_ref[...] = jnp.zeros_like(gwr_ref)

    @pl.when(step < sources)
    def _():
        lanes = g_ref.shape[2]
        eye = (lax.broadcasted_iota(jnp.int32, (capacity, lanes), 0)
               == lax.broadcasted_iota(jnp.int32, (capacity, lanes), 1))
        for e in range(n_local):
            first = (step * n_local + e) * (capacity * 8)
            for c in range(cols):
                table[pl.ds(first + c, capacity, stride=8), :] = back_ref[0, e, :, c * 128:(c + 1) * 128].astype(jnp.float32)
            g_col = jnp.sum(jnp.where(eye, g_ref[0, e:e + 1, :], 0.0), axis=1, keepdims=True)
            table[pl.ds(first + cols, capacity, stride=8), :] = jnp.broadcast_to(g_col, (capacity, 128))

    @pl.when(step >= sources)
    def _():
        block = step - sources

        def pick(i, carry):
            for u in range(UNROLL):
                t = i * UNROLL + u
                slot = slot_ref[block * TOKEN_BLOCK + t]
                stage[pl.ds(pl.multiple_of(t * 8, 8), 8), :] = table[pl.ds(pl.multiple_of(slot * 8, 8), 8), :]
            return carry
        lax.fori_loop(0, TOKEN_BLOCK // UNROLL, pick, 0)
        g_tok = stage[pl.ds(cols, TOKEN_BLOCK, stride=8), :][:, :num_experts]
        prob = p_ref[...]
        aux_vec = aux_ref[0:1, :]
        spread = jnp.sum(prob * aux_vec, axis=1, keepdims=True)
        d_logits = g_tok * ohg_ref[...] + prob * (aux_vec - spread) + zp_ref[...]
        hi, mid, low = split3(d_logits)
        left = jnp.concatenate([hi, mid, hi, low, mid, hi], axis=1)
        dx_router = jnp.dot(left, wr_t_ref[...], preferred_element_type=jnp.float32)
        for c in range(cols):
            part = slice(c * 128, (c + 1) * 128)
            gx_ref[:, part] = (stage[pl.ds(c, TOKEN_BLOCK, stride=8), :] + dx_router[:, part]).astype(jnp.bfloat16)
        parts = jnp.concatenate([hi, mid, low, jnp.zeros_like(hi)], axis=1)
        gwr_ref[...] += lax.dot_general(parts, x_ref[...], (((0,), (0,)), ((), ())), preferred_element_type=jnp.float32)


def combine(tok_slot, back, g_back, x_tokens, ohg, prob, zp, aux_vec, w_router, gw_in, gw_out_t):
    n_dev, n_local, capacity, d_model = back.shape
    tokens = x_tokens.shape[0]
    num_experts = prob.shape[1]
    d_ff = gw_in.shape[2]
    blocks = tokens // TOKEN_BLOCK
    steps = n_dev + blocks
    lanes = g_back.shape[2]
    n_slots = n_dev * n_local * capacity
    round_bf16 = lambda v: lax.reduce_precision(v, 8, 7)
    w_hi = round_bf16(w_router.T)
    w_mid = round_bf16(w_router.T - w_hi)
    w_low = w_router.T - w_hi - w_mid
    wr_t = jnp.concatenate([w_hi, w_hi, w_mid, w_hi, w_mid, w_low], axis=0).astype(jnp.bfloat16)
    gw_in_rows = gw_in.reshape(n_local * d_model, d_ff)
    in_rows = n_local * d_model // steps
    out_cols = d_ff // 128
    src = lambda i: jnp.minimum(i, n_dev - 1)
    tok = lambda i: (jnp.maximum(i - n_dev, 0), 0)
    flip = lambda i: jnp.minimum(i, n_local * out_cols - 1)
    gx, gwr, gw_in_out, gw_out = pl.pallas_call(
        functools.partial(combine_kernel, n_dev, capacity),
        grid=(steps,),
        out_shape=(jax.ShapeDtypeStruct((tokens, d_model), jnp.bfloat16),
                   jax.ShapeDtypeStruct((4 * num_experts, d_model), jnp.float32),
                   jax.ShapeDtypeStruct((n_local * d_model, d_ff), jnp.float32),
                   jax.ShapeDtypeStruct((n_local, d_ff, d_model), jnp.float32)),
        in_specs=[pl.BlockSpec(memory_space=pltpu.SMEM),
                  pl.BlockSpec((1, n_local, capacity, d_model), lambda i: (src(i), 0, 0, 0)),
                  pl.BlockSpec((1, 8, lanes), lambda i: (src(i), 0, 0)),
                  pl.BlockSpec((TOKEN_BLOCK, d_model), tok),
                  pl.BlockSpec((TOKEN_BLOCK, num_experts), tok),
                  pl.BlockSpec((TOKEN_BLOCK, num_experts), tok),
                  pl.BlockSpec((TOKEN_BLOCK, num_experts), tok),
                  pl.BlockSpec((8, num_experts), lambda i: (0, 0)),
                  pl.BlockSpec((6 * num_experts, d_model), lambda i: (0, 0)),
                  pl.BlockSpec((in_rows, d_ff), lambda i: (i, 0)),
                  pl.BlockSpec((1, d_model, 128), lambda i: (flip(i) // out_cols, 0, flip(i) % out_cols))],
        out_specs=(pl.BlockSpec((TOKEN_BLOCK, d_model), tok),
                   pl.BlockSpec((4 * num_experts, d_model), lambda i: (0, 0)),
                   pl.BlockSpec((in_rows, d_ff), lambda i: (i, 0)),
                   pl.BlockSpec((1, 128, d_model), lambda i: (flip(i) // out_cols, flip(i) % out_cols, 0))),
        scratch_shapes=[pltpu.VMEM(((n_slots + 1) * 8, 128), jnp.float32),
                        pltpu.VMEM((TOKEN_BLOCK * 8, 128), jnp.float32)],
        compiler_params=pltpu.CompilerParams(dimension_semantics=('arbitrary',), vmem_limit_bytes=60 * 1024 * 1024),
        name='combine',
    )(tok_slot, back, g_back, x_tokens, ohg, prob, zp, jnp.broadcast_to(aux_vec, (8, num_experts)), wr_t, gw_in_rows, gw_out_t)
    part = gwr.reshape(4, num_experts, d_model)
    return gx, (part[0] + part[1] + part[2]).T, gw_in_out.reshape(n_local, d_model, d_ff), gw_out


def flip_bits(me, k, n):
    out = 0
    bit = 1
    while bit < n:
        mine = (me // bit) % 2
        flip = (k // bit) % 2
        out = out + bit * (mine + flip - 2 * mine * flip)
        bit *= 2
    return out


def total_kernel(n, part_ref, out_ref, inbox, mine, a_send, a_recv, b_send, b_recv):
    me = lax.axis_index('ep')

    def scatter(k):
        peer = flip_bits(me, k, n)
        return pltpu.make_async_remote_copy(src_ref=part_ref.at[peer], dst_ref=inbox.at[me], send_sem=a_send.at[k],
                                            recv_sem=a_recv.at[k], device_id=(peer,), device_id_type=MESH)

    def spread(k):
        peer = flip_bits(me, k, n)
        return pltpu.make_async_remote_copy(src_ref=mine, dst_ref=out_ref.at[me], send_sem=b_send.at[k],
                                            recv_sem=b_recv.at[k], device_id=(peer,), device_id_type=MESH)

    for k in range(1, n):
        scatter(k).start()
    inbox[me] = part_ref[me]
    for k in range(1, n):
        scatter(k).wait_recv()
    total = inbox[0]
    for i in range(1, n):
        total = total + inbox[i]
    mine[...] = total
    out_ref[me] = total
    for k in range(1, n):
        spread(k).start()
    for k in range(1, n):
        scatter(k).wait_send()
        spread(k).wait()


def total(part, n_dev):
    rows, cols = part.shape
    piece = rows * cols // (n_dev * 128)
    chunks = jnp.pad(part.reshape(n_dev, piece, 128), ((0, 0), (0, -piece % 8), (0, 0)))
    dma = pltpu.SemaphoreType.DMA
    vmem_spec = pl.BlockSpec(memory_space=pltpu.VMEM)
    out = pl.pallas_call(
        functools.partial(total_kernel, n_dev),
        out_shape=jax.ShapeDtypeStruct(chunks.shape, jnp.float32),
        in_specs=[vmem_spec],
        out_specs=vmem_spec,
        scratch_shapes=[pltpu.VMEM(chunks.shape, jnp.float32), pltpu.VMEM(chunks.shape[1:], jnp.float32),
                        dma((n_dev,)), dma((n_dev,)), dma((n_dev,)), dma((n_dev,))],
        compiler_params=pltpu.CompilerParams(has_side_effects=True),
        name='total',
    )(chunks)
    return out[:, :piece].reshape(rows, cols)


def nt_dot(a, b):
    return lax.dot_general(a, b, (((1,), (1,)), ((), ())), preferred_element_type=jnp.float32)


def tile_at(t):
    quarter = t // 4
    edge = (7 - quarter) // 7 + quarter // 7
    turn = (t + 4) % 8
    piece = (1 - edge) * (turn // 2) + edge * (t % 4)
    stage = (t + 4) // 8
    chip = stage * (7 - stage) // 2 + stage // 4
    chip = chip + (1 - edge) * (turn % 2) * (7 - 2 * chip)
    return chip * 2 + piece // 2, piece % 2


def link_sets(n, n_local):
    assert n == 16
    pieces = []
    for chips in ((3, 4), (5, 2), (6, 1), (7,)):
        pieces.append([[(chip * 2 + c, e) for c in range(2) for e in range(n_local)] for chip in chips])
    return pieces


def exchange_kernel(n, n_local, cap, x_ref, dy_ref, slot_ref, gate_ref, stat_ref, w_in_ref, w_out_ref,
                    gw_in_ref, gw_out_t_ref, back_ref, g_back_ref, stat_out_ref,
                    table, w_a_all, w_b_all, staged, packed, gate_acc, xr, gate_s, gate_r, g_s, stat_r,
                    fwd_send, fwd_recv, gate_send, gate_recv,
                    ret_send, ret_recv, g_send, g_recv, stat_send, stat_recv, loc_sem):
    me = lax.axis_index('ep')
    d_model = x_ref.shape[1]
    d_ff = w_in_ref.shape[2]
    lanes = gate_r.shape[2]
    chunks, chunk_tok = slot_ref.shape

    def peer_of(k):
        return flip_bits(me, k, n)

    def fwd_copy(k, e, part, src):
        sem = (k * n_local + e) * 2 + part
        return pltpu.make_async_remote_copy(
            src_ref=src.at[part], dst_ref=xr.at[k, e, part],
            send_sem=fwd_send.at[sem], recv_sem=fwd_recv.at[sem],
            device_id=(peer_of(k),), device_id_type=MESH)

    def gate_copy(k):
        return pltpu.make_async_remote_copy(
            src_ref=gate_s.at[k], dst_ref=gate_r.at[k],
            send_sem=gate_send.at[k], recv_sem=gate_recv.at[k],
            device_id=(peer_of(k),), device_id_type=MESH)

    def stat_copy(k):
        return pltpu.make_async_remote_copy(
            src_ref=stat_ref, dst_ref=stat_r.at[me],
            send_sem=stat_send.at[k], recv_sem=stat_recv.at[k],
            device_id=(peer_of(k),), device_id_type=MESH)

    def ret_copy(k, e):
        sem = k * n_local + e
        return pltpu.make_async_remote_copy(
            src_ref=xr.at[k, e, 0], dst_ref=back_ref.at[me, e],
            send_sem=ret_send.at[sem], recv_sem=ret_recv.at[sem],
            device_id=(peer_of(k),), device_id_type=MESH)

    def g_copy(k):
        return pltpu.make_async_remote_copy(
            src_ref=g_s.at[k], dst_ref=g_back_ref.at[me],
            send_sem=g_send.at[k], recv_sem=g_recv.at[k],
            device_id=(peer_of(k),), device_id_type=MESH)

    sets = link_sets(n, n_local)

    def interleave(queues):
        return [queue[i] for i in range(len(queues[0])) for queue in queues]

    near = [[(1, e) for e in range(n_local)]]
    order = [(0, e) for e in range(n_local)] + near[0]
    first = []
    for queues in sets:
        first.append(len(order))
        order = order + interleave(queues)
    assert order == [tile_at(t) for t in range(len(order))]

    def rows_sent(k, e, part):
        fwd_copy(k, e, part, staged.at[0, 0]).wait_send()

    def rows_left(i):
        for queue in sets[i]:
            for j, (k, e) in enumerate(queue):
                rows_sent(k, e, 0)
                if j < len(queue) - 1:
                    rows_sent(k, e, 1)

    def rows_done(i):
        for queue in sets[i]:
            rows_sent(*queue[-1], 1)

    def send_grads(queues):
        for k, e in interleave(queues):
            ret_copy(k, e).start()
            if e == n_local - 1:
                g_copy(k).start()

    def grads_left(i):
        for queue in sets[i]:
            for k, e in queue[:-1]:
                ret_copy(k, e).wait_send()

    eye = (lax.broadcasted_iota(jnp.int32, (cap, lanes), 0)
           == lax.broadcasted_iota(jnp.int32, (cap, lanes), 1))

    def pack(k, e, dst):
        base = (peer_of(k) * n_local + e) * cap
        packed[...] = jnp.zeros_like(packed)
        gate_acc[...] = jnp.zeros_like(gate_acc)
        own_row = lax.broadcasted_iota(jnp.int32, (cap, chunk_tok), 0)

        def chunk(c, carry):
            hit = own_row == slot_ref[pl.ds(c, 1), :] - base
            start = pl.multiple_of(c * chunk_tok, chunk_tok)
            packed[...] += jnp.dot(jnp.where(hit, 1.0, 0.0).astype(jnp.bfloat16), table[pl.ds(start, chunk_tok), :],
                                   preferred_element_type=jnp.float32)
            picked = jnp.where(hit, gate_ref[pl.ds(c, 1), :], 0.0)
            for i in range(chunk_tok // 128):
                gate_acc[...] += picked[:, i * 128:(i + 1) * 128]
            return carry

        lax.fori_loop(0, chunks, chunk, 0)
        dst[0] = packed[:, :d_model].astype(jnp.bfloat16)
        dst[1] = packed[:, d_model:].astype(jnp.bfloat16)
        gate_col = jnp.sum(gate_acc[...], axis=1, keepdims=True)
        gate_s[k, pl.ds(e, 1), :] = jnp.sum(jnp.where(eye, gate_col, 0.0), axis=0, keepdims=True)

    def send_piece(k, e, src):
        for part in range(2):
            fwd_copy(k, e, part, src).start()

        @pl.when(e == n_local - 1)
        def _():
            gate_copy(k).start()
            stat_copy(k).start()

    def make_pieces(i, lo, hi, send):
        def body(j, carry):
            k, e = tile_at(first[i] + j)
            buf = staged.at[i % 2, j]
            pack(k, e, buf)
            if send:
                send_piece(k, e, buf)
            return carry
        lax.fori_loop(lo, hi, body, 0)

    def send_pieces(i, lo, hi):
        def body(j, carry):
            k, e = tile_at(first[i] + j)
            send_piece(k, e, staged.at[i % 2, j])
            return carry
        lax.fori_loop(lo, hi, body, 0)

    def tile(k, e):
        rows = xr[k, e, 0]
        dy = xr[k, e, 1].astype(jnp.float32)
        gate_row = gate_r[k, pl.ds(e, 1), :]
        gate_col = jnp.sum(jnp.where(eye, gate_row, 0.0), axis=1, keepdims=True)
        grad = (gate_col * dy).astype(jnp.bfloat16)
        rows_t = rows.T
        grad_t = grad.T
        out = jnp.zeros((cap, d_model), jnp.float32)
        d_rows = jnp.zeros((cap, d_model), jnp.float32)
        for f in range(0, d_ff, F_CHUNK):
            fs = pl.ds(f, F_CHUNK)
            w_a = w_a_all[e, :, fs]
            w_b = w_b_all[e, fs, :]
            pre = jnp.dot(rows, w_a, preferred_element_type=jnp.float32)
            hid = jnp.maximum(pre, 0.0).astype(jnp.bfloat16)
            out = out + jnp.dot(hid, w_b, preferred_element_type=jnp.float32)
            d_hid = nt_dot(grad, w_b)
            d_pre = jnp.where(hid.astype(jnp.float32) > 0, d_hid, 0.0).astype(jnp.bfloat16)
            gw_out_t_ref[e, :, fs] += jnp.dot(grad_t, hid, preferred_element_type=jnp.float32)
            gw_in_ref[e, :, fs] += jnp.dot(rows_t, d_pre, preferred_element_type=jnp.float32)
            d_rows = d_rows + nt_dot(d_pre, w_a)
        out = out.astype(jnp.bfloat16).astype(jnp.float32)
        g_col = jnp.sum(out * dy, axis=1, keepdims=True)
        g_s[k, pl.ds(e, 1), :] = jnp.sum(jnp.where(eye, g_col, 0.0), axis=0, keepdims=True)
        xr[k, e, 0] = d_rows.astype(jnp.bfloat16)

    def tiles(lo, hi, events=None):
        def body(t, carry):
            for at, run in (events or {}).items():
                pl.when(t == at)(run)
            k, e = tile_at(t)

            @pl.when(t >= n_local)
            def _():
                @pl.when(e == 0)
                def _():
                    gate_copy(k).wait_recv()
                for part in range(2):
                    fwd_copy(k, e, part, staged.at[0, 0]).wait_recv()

            tile(k, e)
            return carry
        lax.fori_loop(lo, hi, body, 0)

    load_x = pltpu.make_async_copy(x_ref, table.at[:, pl.ds(0, d_model)], loc_sem.at[0])
    load_dy = pltpu.make_async_copy(dy_ref, table.at[:, pl.ds(d_model, d_model)], loc_sem.at[1])
    load_a = pltpu.make_async_copy(w_in_ref, w_a_all, loc_sem.at[2])
    load_b = pltpu.make_async_copy(w_out_ref, w_b_all, loc_sem.at[3])
    for c in (load_x, load_dy, load_a, load_b):
        c.start()
    gate_s[...] = jnp.zeros_like(gate_s)
    g_s[...] = jnp.zeros_like(g_s)
    stat_r[me] = stat_ref[...]
    load_x.wait()
    load_dy.wait()

    make_pieces(0, 0, 8, True)
    make_pieces(1, 0, 2, False)
    rows_left(0)
    send_pieces(1, 0, 2)
    make_pieces(1, 2, 8, True)
    gw_in_ref[...] = jnp.zeros_like(gw_in_ref)
    gw_out_t_ref[...] = jnp.zeros_like(gw_out_t_ref)
    load_a.wait()
    load_b.wait()
    tiles(first[0], first[1])
    rows_left(1)
    send_grads(sets[0])
    rows_done(0)
    make_pieces(2, 0, 4, False)
    grads_left(0)
    send_pieces(2, 0, 4)
    make_pieces(2, 4, 8, True)
    tiles(first[1], first[2])
    rows_done(1)
    make_pieces(3, 0, 2, False)
    rows_left(2)
    send_grads(sets[1])
    make_pieces(3, 2, 4, False)

    def start_last():
        grads_left(1)
        send_pieces(3, 0, 4)

    tiles(first[2], first[3], {first[3] - 2: start_last})
    rows_done(2)

    def near_piece(j, carry):
        k, e = tile_at(n_local + j)
        pack(k, e, staged.at[0, j])
        send_piece(k, e, staged.at[0, j])
        return carry

    lax.fori_loop(0, n_local, near_piece, 0)

    def own_piece(j, carry):
        pack(0, j, xr.at[0, j])
        return carry

    lax.fori_loop(0, n_local, own_piece, 0)
    gate_r[0] = gate_s[0]
    tiles(0, first[0])
    own_out = [pltpu.make_async_copy(xr.at[0, e, 0], back_ref.at[me, e], loc_sem.at[e]) for e in range(n_local)]
    own_g = pltpu.make_async_copy(g_s.at[0], g_back_ref.at[me], loc_sem.at[n_local])
    send_grads(near)
    for c in own_out:
        c.start()
    own_g.start()

    def start_third():
        rows_left(3)
        send_grads(sets[2])

    tiles(first[3], len(order), {len(order) - 1: start_third})
    grads_left(2)
    send_grads(sets[3])

    rows_done(3)
    for i in range(3):
        for queue in sets[i]:
            ret_copy(*queue[-1]).wait_send()
    grads_left(3)
    for queue in sets[3]:
        ret_copy(*queue[-1]).wait_send()
    for k, e in near[0]:
        for part in range(2):
            rows_sent(k, e, part)
        ret_copy(k, e).wait_send()
    for c in own_out:
        c.wait()
    own_g.wait()

    def drain(k, carry):
        gate_copy(k).wait_send()
        stat_copy(k).wait()
        g_copy(k).wait()
        for e in range(n_local):
            ret_copy(k, e).wait_recv()
        return carry

    lax.fori_loop(1, n, drain, 0)
    stat = stat_r[0]
    for i in range(1, n):
        stat = stat + stat_r[i]
    stat_out_ref[...] = stat


def exchange(x_tokens, grad_y, tok_slot, gate_val, stats, w_in, w_out, n_dev, cap, lanes):
    n_local, d_model, d_ff = w_in.shape
    tokens = x_tokens.shape[0]
    any_spec = pl.BlockSpec(memory_space=pl.ANY)
    vmem_spec = pl.BlockSpec(memory_space=pltpu.VMEM)
    pairs = n_dev * n_local
    dma = pltpu.SemaphoreType.DMA
    small = pltpu.VMEM((n_dev, 8, lanes), jnp.float32)
    return pl.pallas_call(
        functools.partial(exchange_kernel, n_dev, n_local, cap),
        out_shape=(jax.ShapeDtypeStruct((n_local, d_model, d_ff), jnp.float32),
                   jax.ShapeDtypeStruct((n_local, d_model, d_ff), jnp.float32),
                   jax.ShapeDtypeStruct((n_dev, n_local, cap, d_model), jnp.bfloat16),
                   jax.ShapeDtypeStruct((n_dev, 8, lanes), jnp.float32),
                   jax.ShapeDtypeStruct(stats.shape, jnp.float32)),
        in_specs=[any_spec, any_spec, vmem_spec, vmem_spec, vmem_spec, any_spec, any_spec],
        out_specs=(vmem_spec, vmem_spec, any_spec, any_spec, vmem_spec),
        scratch_shapes=[
            pltpu.VMEM((tokens, 2 * d_model), jnp.bfloat16),
            pltpu.VMEM(w_in.shape, jnp.bfloat16),
            pltpu.VMEM(w_out.shape, jnp.bfloat16),
            pltpu.VMEM((2, 8, 2, cap, d_model), jnp.bfloat16),
            pltpu.VMEM((cap, 2 * d_model), jnp.float32),
            pltpu.VMEM((cap, 128), jnp.float32),
            pltpu.VMEM((n_dev, n_local, 2, cap, d_model), jnp.bfloat16),
            small, small, small,
            pltpu.VMEM((n_dev,) + stats.shape, jnp.float32),
            dma((2 * pairs,)), dma((2 * pairs,)), dma((n_dev,)), dma((n_dev,)),
            dma((pairs,)), dma((pairs,)), dma((n_dev,)), dma((n_dev,)),
            dma((n_dev,)), dma((n_dev,)), dma((4,)),
        ],
        compiler_params=pltpu.CompilerParams(has_side_effects=True, vmem_limit_bytes=63 * 1024 * 1024),
        name='exchange',
    )(x_tokens, grad_y, tok_slot.reshape(-1, 512), gate_val.reshape(-1, 512), stats, w_in, w_out)


def solution(mesh):
    n_dev = mesh.shape['ep']

    def expert_layer(x_tokens, w_router, expert_idx, w_in, w_out, grad_y):
        tokens, d_model = x_tokens.shape
        n_local = w_in.shape[0]
        num_experts = n_local * n_dev
        capacity = (5 * tokens + 4 * num_experts - 1) // (4 * num_experts)
        total_tok = tokens * n_dev
        lanes = -(-capacity // 128) * 128
        onehot = (expert_idx[:, None] == jnp.arange(num_experts, dtype=jnp.int32)[None, :]).astype(jnp.float32)
        tok_slot, load = route_slots(onehot, expert_idx, capacity)
        logits = jnp.dot(x_tokens, w_router, preferred_element_type=jnp.float32)
        router_prob = jax.nn.softmax(logits, axis=-1)
        log_norm = jax.nn.logsumexp(logits, axis=-1, keepdims=True)
        gate_val = jnp.sum(router_prob * onehot, axis=-1, keepdims=True)
        stats = jnp.concatenate([load, jnp.sum(router_prob, axis=0), jnp.sum(log_norm * log_norm)[None]])
        stats = jnp.pad(stats[None], ((0, 7), (0, 128 - stats.shape[0])))
        gw_in, gw_out_t, back, g_back, stats = exchange(x_tokens, grad_y, tok_slot, gate_val, stats, w_in, w_out, n_dev, capacity, lanes)

        load_frac = stats[0, :num_experts] / total_tok
        mean_prob = stats[0, num_experts:2 * num_experts] / total_tok
        aux_loss = AUX_WEIGHT * num_experts * jnp.sum(load_frac * mean_prob)
        z_loss = Z_WEIGHT * stats[0, 2 * num_experts] / total_tok
        aux_vec = AUX_WEIGHT * num_experts * load_frac / total_tok
        ohg = gate_val * (onehot - router_prob)
        zp = (2.0 * Z_WEIGHT / total_tok * log_norm) * router_prob
        grad_x, part, grad_w_in, grad_w_out = combine(tok_slot, back, g_back, x_tokens, ohg, router_prob, zp, aux_vec, w_router, gw_in, gw_out_t)
        grad_w_router = total(part, n_dev)
        return grad_x, grad_w_in, grad_w_out, grad_w_router, aux_loss, z_loss

    return jax.shard_map(expert_layer, mesh=mesh,
                         in_specs=(P('ep', None), P(None, None), P('ep'), P('ep', None, None), P('ep', None, None), P('ep', None)),
                         out_specs=(P('ep', None), P('ep', None, None), P('ep', None, None), P(None, None), P(), P()),
                         check_vma=False)
```

```python
import functools

import jax
import jax.numpy as jnp
from jax import lax
from jax.experimental import pallas as pl
from jax.experimental.pallas import tpu as pltpu
from jax.sharding import PartitionSpec as P

AUX_WEIGHT = 0.01
Z_WEIGHT = 0.001
MESH = pl.DeviceIdType.MESH
F_CHUNK = 512
TOKEN_BLOCK = 256
UNROLL = 16
ROW_TOKENS = 1024
GROUP = 2


def nt_dot(a, b):
    return lax.dot_general(a, b, (((1,), (1,)), ((), ())), preferred_element_type=jnp.float32)


def eye_mask(rows, cols):
    return lax.broadcasted_iota(jnp.int32, (rows, cols), 0) == lax.broadcasted_iota(jnp.int32, (rows, cols), 1)


def split3(v):
    hi = v.astype(jnp.bfloat16)
    rest = v - hi.astype(jnp.float32)
    mid = rest.astype(jnp.bfloat16)
    low = (rest - mid.astype(jnp.float32)).astype(jnp.bfloat16)
    return hi, mid, low


def split_weights(w):
    round_bf16 = lambda v: lax.reduce_precision(v, 8, 7)
    hi = round_bf16(w)
    mid = round_bf16(w - hi)
    return hi, mid, w - hi - mid


def route_kernel(capacity, x_ref, idx_ref, wr_ref, prob_ref, slot_ref, gate_ref, norm_ref, stat_ref, seen, load, prob_sum, z_sum):
    step = pl.program_id(0)
    num_experts, block = prob_ref.shape

    @pl.when(step == 0)
    def _():
        seen[...] = jnp.zeros_like(seen)
        prob_sum[...] = jnp.zeros_like(prob_sum)
        z_sum[...] = jnp.zeros_like(z_sum)

    parts = nt_dot(wr_ref[...], x_ref[...])
    logits = parts[:num_experts] + parts[num_experts:2 * num_experts] + parts[2 * num_experts:]
    top = jnp.max(logits, axis=0, keepdims=True)
    shifted = jnp.exp(logits - top)
    scale = jnp.sum(shifted, axis=0, keepdims=True)
    prob = shifted / scale
    log_norm = top + jnp.log(scale)
    idx = idx_ref[pl.ds(step, 1), :]
    chosen = jnp.where(lax.broadcasted_iota(jnp.int32, (num_experts, block), 0) == idx, 1.0, 0.0)
    prob_ref[...] = prob
    gate_ref[pl.ds(step, 1), :] = jnp.sum(prob * chosen, axis=0, keepdims=True)
    norm_ref[pl.ds(step, 1), :] = log_norm
    squares = log_norm * log_norm
    for i in range(0, block, 128):
        prob_sum[...] += prob[:, i:i + 128]
        z_sum[0:1, :] += squares[:, i:i + 128]
    upto = jnp.where(lax.broadcasted_iota(jnp.int32, (TOKEN_BLOCK, TOKEN_BLOCK), 0)
                     <= lax.broadcasted_iota(jnp.int32, (TOKEN_BLOCK, TOKEN_BLOCK), 1), 1.0, 0.0).astype(jnp.bfloat16)
    before = seen[:, 0:1]
    slots = []
    for i in range(0, block, TOKEN_BLOCK):
        part = chosen[:, i:i + TOKEN_BLOCK]
        count = jnp.dot(part.astype(jnp.bfloat16), upto, preferred_element_type=jnp.float32) + before
        position = jnp.sum(part * count, axis=0, keepdims=True).astype(jnp.int32) - 1
        slots.append(jnp.where(position < capacity, idx[:, i:i + TOKEN_BLOCK] * capacity + position, num_experts * capacity))
        before = count[:, TOKEN_BLOCK - 1:TOKEN_BLOCK]
    slot_ref[pl.ds(step, 1), :] = jnp.concatenate(slots, axis=1)
    seen[...] = jnp.broadcast_to(before, seen.shape)

    @pl.when(step == pl.num_programs(0) - 1)
    def _():
        row = lax.broadcasted_iota(jnp.int32, (num_experts, 128), 0)
        lane = lax.broadcasted_iota(jnp.int32, (num_experts, 128), 1)
        probs = jnp.sum(prob_sum[...], axis=1, keepdims=True)
        stat_ref[...] = jnp.zeros_like(stat_ref)
        total = jnp.sum(jnp.where(row == lane, seen[...], 0.0) + jnp.where(row + num_experts == lane, probs, 0.0),
                        axis=0, keepdims=True)
        squares = jnp.sum(z_sum[0:1, :], axis=1, keepdims=True)
        stat_ref[0:1, :] = total + jnp.where(lane[0:1, :] == 2 * num_experts, squares, 0.0)


def route(x_tokens, idx_rows, w_router, capacity):
    tokens, d_model = x_tokens.shape
    num_experts = w_router.shape[1]
    steps, block = idx_rows.shape
    wr = jnp.concatenate(split_weights(w_router.T), axis=0).astype(jnp.bfloat16)
    rows = lambda dtype: jax.ShapeDtypeStruct((steps, block), dtype)
    whole = pl.BlockSpec((steps, block), lambda i: (0, 0))
    return pl.pallas_call(
        functools.partial(route_kernel, capacity),
        grid=(steps,),
        out_shape=(jax.ShapeDtypeStruct((num_experts, tokens), jnp.float32), rows(jnp.int32), rows(jnp.float32), rows(jnp.float32),
                   jax.ShapeDtypeStruct((8, 128), jnp.float32)),
        in_specs=[pl.BlockSpec((block, d_model), lambda i: (i, 0)), whole,
                  pl.BlockSpec((3 * num_experts, d_model), lambda i: (0, 0))],
        out_specs=(pl.BlockSpec((num_experts, block), lambda i: (0, i)), whole, whole, whole,
                   pl.BlockSpec((8, 128), lambda i: (0, 0))),
        scratch_shapes=[pltpu.VMEM((num_experts, 128), jnp.float32), pltpu.VMEM((num_experts, 128), jnp.float32),
                        pltpu.VMEM((num_experts, 128), jnp.float32), pltpu.VMEM((8, 128), jnp.float32)],
        compiler_params=pltpu.CompilerParams(dimension_semantics=('arbitrary',)),
        name='route',
    )(x_tokens, idx_rows, wr)


def dispatch_kernel(steps, capacity, slot_ref, x_ref, dy_ref, gate_ref, xd_ref, gates_ref, table, stage):
    step = pl.program_id(0)
    block, d_model = x_ref.shape
    cols = d_model // 128
    lanes = gates_ref.shape[2]
    group, n_local = xd_ref.shape[:2]

    @pl.when(step == 0)
    def _():
        def clear(i, carry):
            table[pl.ds(pl.multiple_of(i * 512, 512), 512), :] = jnp.zeros((512, 128), jnp.float32)
            return carry
        lax.fori_loop(0, table.shape[0] // 512, clear, 0)

    @pl.when(step < steps)
    def _():
        for c in range(cols):
            stage[pl.ds(c, block, stride=8), :] = x_ref[:, c * 128:(c + 1) * 128].astype(jnp.float32)
            stage[pl.ds(cols + c, block, stride=8), :] = dy_ref[:, c * 128:(c + 1) * 128].astype(jnp.float32)
        eye = eye_mask(128, 128)
        gate_row = gate_ref[pl.ds(step, 1), :]
        for i in range(0, block, 128):
            gate = jnp.sum(jnp.where(eye, gate_row[:, i:i + 128], 0.0), axis=1, keepdims=True)
            stage[pl.ds(i * 8 + 2 * cols, 128, stride=8), :] = jnp.broadcast_to(gate, (128, 128))

        def place(i, carry):
            for u in range(UNROLL):
                t = i * UNROLL + u
                slot = slot_ref[step, t]
                table[pl.ds(pl.multiple_of(slot * 8, 8), 8), :] = stage[pl.ds(pl.multiple_of(t * 8, 8), 8), :]
            return carry
        lax.fori_loop(0, block // UNROLL, place, 0)

    @pl.when(step >= steps)
    def _():
        gates_ref[...] = jnp.zeros_like(gates_ref)
        row = lax.broadcasted_iota(jnp.int32, (capacity, 128), 0)
        lane = lax.broadcasted_iota(jnp.int32, (capacity, 128), 1)

        def unload(i, carry):
            d = i // n_local
            e = i % n_local
            first = (((step - steps) * group + d) * n_local + e) * (capacity * 8)
            for c in range(cols):
                xd_ref[d, e, 0, :, c * 128:(c + 1) * 128] = table[pl.ds(first + c, capacity, stride=8), :].astype(jnp.bfloat16)
                xd_ref[d, e, 1, :, c * 128:(c + 1) * 128] = table[pl.ds(first + cols + c, capacity, stride=8), :].astype(jnp.bfloat16)
            gate = table[pl.ds(first + 2 * cols, capacity, stride=8), :]
            gates_ref[d, pl.ds(e, 1), :] = jnp.concatenate([
                jnp.sum(jnp.where(row == lane + c * 128, gate, 0.0), axis=0, keepdims=True)
                for c in range(lanes // 128)], axis=1)
            return carry
        lax.fori_loop(0, group * n_local, unload, 0)


def dispatch(slot_rows, x_tokens, grad_y, gate_rows, n_dev, n_local, capacity, lanes):
    tokens, d_model = x_tokens.shape
    steps, block = slot_rows.shape
    n_slots = n_dev * n_local * capacity
    table_rows = -(-(n_slots + 1) * 8 // 512) * 512
    tok = lambda i: (jnp.minimum(i, steps - 1), 0)
    dst = lambda i: jnp.maximum(i - steps, 0)
    return pl.pallas_call(
        functools.partial(dispatch_kernel, steps, capacity),
        grid=(steps + n_dev // GROUP,),
        out_shape=(jax.ShapeDtypeStruct((n_dev, n_local, 2, capacity, d_model), jnp.bfloat16),
                   jax.ShapeDtypeStruct((n_dev, 8, lanes), jnp.float32)),
        in_specs=[pl.BlockSpec(memory_space=pltpu.SMEM),
                  pl.BlockSpec((block, d_model), tok),
                  pl.BlockSpec((block, d_model), tok),
                  pl.BlockSpec((steps, block), lambda i: (0, 0))],
        out_specs=(pl.BlockSpec((GROUP, n_local, 2, capacity, d_model), lambda i: (dst(i), 0, 0, 0, 0)),
                   pl.BlockSpec((GROUP, 8, lanes), lambda i: (dst(i), 0, 0))),
        scratch_shapes=[pltpu.VMEM((table_rows, 128), jnp.float32),
                        pltpu.VMEM((block * 8, 128), jnp.float32)],
        compiler_params=pltpu.CompilerParams(dimension_semantics=('arbitrary',), vmem_limit_bytes=62 * 1024 * 1024),
        name='dispatch',
    )(slot_rows, x_tokens, grad_y, gate_rows)


def combine_kernel(fills, sources, capacity, z_coef, slot_ref, back_ref, g_ref, x_ref, prob_ref, gate_ref, norm_ref, idx_ref, aux_ref,
                   wr_t_ref, gwi_ref, gwo_t_ref, gx_ref, gwr_ref, gwi_out_ref, gwo_out_ref, table, stage):
    step = pl.program_id(0)
    block, d_model = x_ref.shape
    cols = d_model // 128
    group, n_local = back_ref.shape[:2]
    num_experts = prob_ref.shape[0]
    n_slots = sources * n_local * capacity
    gwi_out_ref[...] = gwi_ref[...]
    gwo_out_ref[0] = gwo_t_ref[0].T

    @pl.when(step == 0)
    def _():
        table[pl.ds(n_slots * 8, 8), :] = jnp.zeros((8, 128), jnp.float32)
        gwr_ref[...] = jnp.zeros_like(gwr_ref)

    @pl.when(step < fills)
    def _():
        eye = eye_mask(capacity, g_ref.shape[2])

        def load(i, carry):
            d = i // n_local
            e = i % n_local
            first = ((step * group + d) * n_local + e) * (capacity * 8)
            for c in range(cols):
                table[pl.ds(first + c, capacity, stride=8), :] = back_ref[d, e, :, c * 128:(c + 1) * 128].astype(jnp.float32)
            g_col = jnp.sum(jnp.where(eye, g_ref[d, pl.ds(e, 1), :], 0.0), axis=1, keepdims=True)
            table[pl.ds(first + cols, capacity, stride=8), :] = jnp.broadcast_to(g_col, (capacity, 128))
            return carry
        lax.fori_loop(0, group * n_local, load, 0)

    @pl.when(step >= fills)
    def _():
        part = step - fills

        def pick(i, carry):
            for u in range(UNROLL):
                t = i * UNROLL + u
                slot = slot_ref[part, t]
                stage[pl.ds(pl.multiple_of(t * 8, 8), 8), :] = table[pl.ds(pl.multiple_of(slot * 8, 8), 8), :]
            return carry
        lax.fori_loop(0, block // UNROLL, pick, 0)
        eye = eye_mask(128, 128)
        g_tok = jnp.concatenate([
            jnp.sum(jnp.where(eye, stage[pl.ds(i * 8 + cols, 128, stride=8), :], 0.0), axis=0, keepdims=True)
            for i in range(0, block, 128)], axis=1)
        here = pl.ds(part, 1)
        prob = prob_ref[...]
        chosen = jnp.where(lax.broadcasted_iota(jnp.int32, (num_experts, block), 0) == idx_ref[here, :], 1.0, 0.0)
        aux_vec = aux_ref[:, 0:1]
        spread = jnp.sum(prob * aux_vec, axis=0, keepdims=True)
        d_logits = ((gate_ref[here, :] * g_tok) * (chosen - prob) + prob * (aux_vec - spread)
                    + (z_coef * norm_ref[here, :]) * prob)
        hi, mid, low = split3(d_logits)
        gwr_ref[...] += jnp.dot(jnp.concatenate([hi, mid, low], axis=0), x_ref[...], preferred_element_type=jnp.float32)
        left = jnp.concatenate([hi, mid, hi, low, mid, hi], axis=0)
        dx_router = lax.dot_general(left, wr_t_ref[...], (((0,), (0,)), ((), ())), preferred_element_type=jnp.float32)
        for c in range(cols):
            span = slice(c * 128, (c + 1) * 128)
            gx_ref[:, span] = (stage[pl.ds(c, block, stride=8), :] + dx_router[:, span]).astype(jnp.bfloat16)


def combine(slot_rows, back, g_back, x_tokens, prob, gate_rows, norm_rows, idx_rows, aux_vec, z_coef, w_router, gw_in, gw_out_t):
    n_dev, n_local, capacity, d_model = back.shape
    tokens = x_tokens.shape[0]
    num_experts = prob.shape[0]
    d_ff = gw_in.shape[2]
    blocks, block = slot_rows.shape
    fills = n_dev // GROUP
    steps = fills + blocks
    lanes = g_back.shape[2]
    n_slots = n_dev * n_local * capacity
    w_hi, w_mid, w_low = split_weights(w_router.T)
    wr_t = jnp.concatenate([w_hi, w_hi, w_mid, w_hi, w_mid, w_low], axis=0).astype(jnp.bfloat16)
    gw_in_rows = gw_in.reshape(n_local * d_model, d_ff)
    in_rows = n_local * d_model // steps
    out_cols = d_ff // 256
    src = lambda i: jnp.minimum(i, fills - 1)
    tok = lambda i: (jnp.maximum(i - fills, 0), 0)
    flip = lambda i: jnp.minimum(i, n_local * out_cols - 1)
    rows = pl.BlockSpec((blocks, block), lambda i: (0, 0))
    gx, gwr, gw_in_out, gw_out = pl.pallas_call(
        functools.partial(combine_kernel, fills, n_dev, capacity, z_coef),
        grid=(steps,),
        out_shape=(jax.ShapeDtypeStruct((tokens, d_model), jnp.bfloat16),
                   jax.ShapeDtypeStruct((3 * num_experts, d_model), jnp.float32),
                   jax.ShapeDtypeStruct((n_local * d_model, d_ff), jnp.float32),
                   jax.ShapeDtypeStruct((n_local, d_ff, d_model), jnp.float32)),
        in_specs=[pl.BlockSpec(memory_space=pltpu.SMEM),
                  pl.BlockSpec((GROUP, n_local, capacity, d_model), lambda i: (src(i), 0, 0, 0)),
                  pl.BlockSpec((GROUP, 8, lanes), lambda i: (src(i), 0, 0)),
                  pl.BlockSpec((block, d_model), tok),
                  pl.BlockSpec((num_experts, block), lambda i: (0, jnp.maximum(i - fills, 0))),
                  rows, rows, rows,
                  pl.BlockSpec((num_experts, 128), lambda i: (0, 0)),
                  pl.BlockSpec((6 * num_experts, d_model), lambda i: (0, 0)),
                  pl.BlockSpec((in_rows, d_ff), lambda i: (i, 0)),
                  pl.BlockSpec((1, d_model, 256), lambda i: (flip(i) // out_cols, 0, flip(i) % out_cols))],
        out_specs=(pl.BlockSpec((block, d_model), tok),
                   pl.BlockSpec((3 * num_experts, d_model), lambda i: (0, 0)),
                   pl.BlockSpec((in_rows, d_ff), lambda i: (i, 0)),
                   pl.BlockSpec((1, 256, d_model), lambda i: (flip(i) // out_cols, flip(i) % out_cols, 0))),
        scratch_shapes=[pltpu.VMEM(((n_slots + 1) * 8, 128), jnp.float32),
                        pltpu.VMEM((block * 8, 128), jnp.float32)],
        compiler_params=pltpu.CompilerParams(dimension_semantics=('arbitrary',), vmem_limit_bytes=63 * 1024 * 1024),
        name='combine',
    )(slot_rows, back, g_back, x_tokens, prob, gate_rows, norm_rows, idx_rows,
      jnp.broadcast_to(aux_vec[:, None], (num_experts, 128)), wr_t, gw_in_rows, gw_out_t)
    part = gwr.reshape(3, num_experts, d_model)
    return gx, (part[0] + part[1] + part[2]).T, gw_in_out.reshape(n_local, d_model, d_ff), gw_out


def flip_bits(me, k, n):
    out = 0
    bit = 1
    while bit < n:
        mine = (me // bit) % 2
        flip = (k // bit) % 2
        out = out + bit * (mine + flip - 2 * mine * flip)
        bit *= 2
    return out


def total_kernel(n, part_ref, out_ref, inbox, mine, a_send, a_recv, b_send, b_recv):
    me = lax.axis_index('ep')

    def scatter(k):
        peer = flip_bits(me, k, n)
        return pltpu.make_async_remote_copy(src_ref=part_ref.at[peer], dst_ref=inbox.at[me], send_sem=a_send.at[k],
                                            recv_sem=a_recv.at[k], device_id=(peer,), device_id_type=MESH)

    def spread(k):
        peer = flip_bits(me, k, n)
        return pltpu.make_async_remote_copy(src_ref=mine, dst_ref=out_ref.at[me], send_sem=b_send.at[k],
                                            recv_sem=b_recv.at[k], device_id=(peer,), device_id_type=MESH)

    for k in range(1, n):
        scatter(k).start()
    inbox[me] = part_ref[me]
    for k in range(1, n):
        scatter(k).wait_recv()
    total = inbox[0]
    for i in range(1, n):
        total = total + inbox[i]
    mine[...] = total
    out_ref[me] = total
    for k in range(1, n):
        spread(k).start()
    for k in range(1, n):
        scatter(k).wait_send()
        spread(k).wait()


def total(part, n_dev):
    rows, cols = part.shape
    piece = rows * cols // (n_dev * 128)
    chunks = jnp.pad(part.reshape(n_dev, piece, 128), ((0, 0), (0, -piece % 8), (0, 0)))
    dma = pltpu.SemaphoreType.DMA
    vmem_spec = pl.BlockSpec(memory_space=pltpu.VMEM)
    out = pl.pallas_call(
        functools.partial(total_kernel, n_dev),
        out_shape=jax.ShapeDtypeStruct(chunks.shape, jnp.float32),
        in_specs=[vmem_spec],
        out_specs=vmem_spec,
        scratch_shapes=[pltpu.VMEM(chunks.shape, jnp.float32), pltpu.VMEM(chunks.shape[1:], jnp.float32),
                        dma((n_dev,)), dma((n_dev,)), dma((n_dev,)), dma((n_dev,))],
        compiler_params=pltpu.CompilerParams(has_side_effects=True),
        name='total',
    )(chunks)
    return out[:, :piece].reshape(rows, cols)


def tile_at(t):
    quarter = t // 4
    edge = (7 - quarter) // 7 + quarter // 7
    turn = (t + 4) % 8
    piece = (1 - edge) * (turn // 2) + edge * (t % 4)
    stage = (t + 4) // 8
    chip = stage * (7 - stage) // 2 + stage // 4
    chip = chip + (1 - edge) * (turn % 2) * (7 - 2 * chip)
    return chip * 2 + piece // 2, piece % 2


def link_sets(n, n_local):
    assert n == 16
    pieces = []
    for chips in ((3, 4), (5, 2), (6, 1), (7,)):
        pieces.append([[(chip * 2 + c, e) for c in range(2) for e in range(n_local)] for chip in chips])
    return pieces


def exchange_kernel(n, n_local, xd_ref, gate_ref, stat_ref, w_in_ref, w_out_ref,
                    gw_in_ref, gw_out_t_ref, back_ref, g_back_ref, stat_out_ref,
                    xr, gate_r, g_s, stat_r,
                    fwd_send, fwd_recv, gate_send, gate_recv,
                    ret_send, ret_recv, g_send, g_recv, stat_send, stat_recv, loc_sem):
    me = lax.axis_index('ep')
    cap, d_model = xr.shape[3], xr.shape[4]
    d_ff = w_in_ref.shape[2]

    def peer_of(k):
        return flip_bits(me, k, n)

    def fwd_copy(k, e, part):
        sem = (k * n_local + e) * 2 + part
        peer = peer_of(k)
        return pltpu.make_async_remote_copy(
            src_ref=xd_ref.at[peer, e, part], dst_ref=xr.at[k, e, part],
            send_sem=fwd_send.at[sem], recv_sem=fwd_recv.at[sem],
            device_id=(peer,), device_id_type=MESH)

    def gate_copy(k):
        peer = peer_of(k)
        return pltpu.make_async_remote_copy(
            src_ref=gate_ref.at[peer], dst_ref=gate_r.at[k],
            send_sem=gate_send.at[k], recv_sem=gate_recv.at[k],
            device_id=(peer,), device_id_type=MESH)

    def stat_copy(k):
        return pltpu.make_async_remote_copy(
            src_ref=stat_ref, dst_ref=stat_r.at[me],
            send_sem=stat_send.at[k], recv_sem=stat_recv.at[k],
            device_id=(peer_of(k),), device_id_type=MESH)

    def ret_copy(k, e):
        sem = k * n_local + e
        return pltpu.make_async_remote_copy(
            src_ref=xr.at[k, e, 0], dst_ref=back_ref.at[me, e],
            send_sem=ret_send.at[sem], recv_sem=ret_recv.at[sem],
            device_id=(peer_of(k),), device_id_type=MESH)

    def g_copy(k):
        return pltpu.make_async_remote_copy(
            src_ref=g_s.at[k], dst_ref=g_back_ref.at[me],
            send_sem=g_send.at[k], recv_sem=g_recv.at[k],
            device_id=(peer_of(k),), device_id_type=MESH)

    sets = link_sets(n, n_local)

    def interleave(queues):
        return [queue[i] for i in range(len(queues[0])) for queue in queues]

    def send_rows(queues):
        for k, e in interleave(queues):
            if e == 0:
                gate_copy(k).start()
                stat_copy(k).start()
            for part in range(2):
                fwd_copy(k, e, part).start()

    def rows_left(queues):
        for queue in queues:
            for i, (k, e) in enumerate(queue):
                fwd_copy(k, e, 0).wait_send()
                if i < len(queue) - 1:
                    fwd_copy(k, e, 1).wait_send()

    def send_grads(queues):
        for k, e in interleave(queues):
            ret_copy(k, e).start()
            if e == n_local - 1:
                g_copy(k).start()

    def grads_left(queues):
        for queue in queues:
            for k, e in queue[:-1]:
                ret_copy(k, e).wait_send()

    near = [[(1, e) for e in range(n_local)]]
    own_in = [pltpu.make_async_copy(xd_ref.at[me, e], xr.at[0, e], loc_sem.at[e]) for e in range(n_local)]
    own_gate = pltpu.make_async_copy(gate_ref.at[me], gate_r.at[0], loc_sem.at[n_local])
    own_out = [pltpu.make_async_copy(xr.at[0, e, 0], back_ref.at[me, e], loc_sem.at[e]) for e in range(n_local)]
    own_g = pltpu.make_async_copy(g_s.at[0], g_back_ref.at[me], loc_sem.at[n_local])

    send_rows(sets[0])
    send_rows(near)
    for c in own_in:
        c.start()
    own_gate.start()
    gw_in_ref[...] = jnp.zeros_like(gw_in_ref)
    gw_out_t_ref[...] = jnp.zeros_like(gw_out_t_ref)
    g_s[...] = jnp.zeros_like(g_s)
    stat_r[me] = stat_ref[...]
    for c in own_in:
        c.wait()
    own_gate.wait()

    lanes = gate_r.shape[2]

    def tile(k, e):
        eye = (lax.broadcasted_iota(jnp.int32, (cap, lanes), 0)
               == lax.broadcasted_iota(jnp.int32, (cap, lanes), 1))
        rows = xr[k, e, 0]
        dy = xr[k, e, 1].astype(jnp.float32)
        gate_row = gate_r[k, pl.ds(e, 1), :]
        gate_col = jnp.sum(jnp.where(eye, gate_row, 0.0), axis=1, keepdims=True)
        grad = (gate_col * dy).astype(jnp.bfloat16)
        rows_t = rows.T
        grad_t = grad.T
        out = jnp.zeros((cap, d_model), jnp.float32)
        d_rows = jnp.zeros((cap, d_model), jnp.float32)
        for f in range(0, d_ff, F_CHUNK):
            fs = pl.ds(f, F_CHUNK)
            w_a = w_in_ref[e, :, fs]
            w_b = w_out_ref[e, fs, :]
            pre = jnp.dot(rows, w_a, preferred_element_type=jnp.float32)
            hid = jnp.maximum(pre, 0.0).astype(jnp.bfloat16)
            out = out + jnp.dot(hid, w_b, preferred_element_type=jnp.float32)
            d_hid = nt_dot(grad, w_b)
            d_pre = jnp.where(hid.astype(jnp.float32) > 0, d_hid, 0.0).astype(jnp.bfloat16)
            gw_out_t_ref[e, :, fs] += jnp.dot(grad_t, hid, preferred_element_type=jnp.float32)
            gw_in_ref[e, :, fs] += jnp.dot(rows_t, d_pre, preferred_element_type=jnp.float32)
            d_rows = d_rows + nt_dot(d_pre, w_a)
        out = out.astype(jnp.bfloat16).astype(jnp.float32)
        g_col = jnp.sum(out * dy, axis=1, keepdims=True)
        g_s[k, pl.ds(e, 1), :] = jnp.sum(jnp.where(eye, g_col, 0.0), axis=0, keepdims=True)
        xr[k, e, 0] = d_rows.astype(jnp.bfloat16)

    order = [(0, e) for e in range(n_local)] + near[0]
    first = []
    for queues in sets:
        first.append(len(order))
        order = order + interleave(queues)
    assert order == [tile_at(t) for t in range(len(order))]

    def own_back():
        send_grads(near)
        for c in own_out:
            c.start()
        own_g.start()

    def after_rows(done, then):
        def run():
            rows_left(sets[done])
            then()
        return run

    def after_grads(done, then):
        def run():
            grads_left(sets[done])
            then()
        return run

    events = {
        first[0]: own_back,
        first[1] - 2: after_rows(0, lambda: send_rows(sets[1])),
        first[2] - 2: after_rows(1, lambda: send_grads(sets[0])),
        first[2]: after_grads(0, lambda: send_rows(sets[2])),
        first[3] - 2: after_rows(2, lambda: send_grads(sets[1])),
        first[3]: after_grads(1, lambda: send_rows(sets[3])),
        len(order) - 1: after_rows(3, lambda: send_grads(sets[2])),
    }

    def step(t, carry):
        k, e = tile_at(t)
        for at, run in events.items():
            pl.when(t == at)(run)

        @pl.when(t >= n_local)
        def _():
            @pl.when(e == 0)
            def _():
                gate_copy(k).wait_recv()
            for part in range(2):
                fwd_copy(k, e, part).wait_recv()

        tile(k, e)
        return carry

    lax.fori_loop(0, len(order), step, 0)
    grads_left(sets[2])
    send_grads(sets[3])

    for queues in sets:
        for queue in queues:
            k, e = queue[-1]
            fwd_copy(k, e, 1).wait_send()
            if queues is not sets[3]:
                ret_copy(k, e).wait_send()
    grads_left(sets[3])
    for queue in sets[3]:
        ret_copy(*queue[-1]).wait_send()
    for k, e in near[0]:
        for part in range(2):
            fwd_copy(k, e, part).wait_send()
        ret_copy(k, e).wait_send()
    for c in own_out:
        c.wait()
    own_g.wait()

    def drain(k, carry):
        gate_copy(k).wait_send()
        stat_copy(k).wait()
        g_copy(k).wait()
        for e in range(n_local):
            ret_copy(k, e).wait_recv()
        return carry

    lax.fori_loop(1, n, drain, 0)
    stat = stat_r[0]
    for i in range(1, n):
        stat = stat + stat_r[i]
    stat_out_ref[...] = stat


def exchange(xd, gates, stats, w_in, w_out, n_dev):
    n_local, d_model, d_ff = w_in.shape
    cap = xd.shape[3]
    lanes = gates.shape[2]
    any_spec = pl.BlockSpec(memory_space=pl.ANY)
    vmem_spec = pl.BlockSpec(memory_space=pltpu.VMEM)
    pairs = n_dev * n_local
    dma = pltpu.SemaphoreType.DMA
    return pl.pallas_call(
        functools.partial(exchange_kernel, n_dev, n_local),
        out_shape=(jax.ShapeDtypeStruct((n_local, d_model, d_ff), jnp.float32),
                   jax.ShapeDtypeStruct((n_local, d_model, d_ff), jnp.float32),
                   jax.ShapeDtypeStruct((n_dev, n_local, cap, d_model), jnp.bfloat16),
                   jax.ShapeDtypeStruct((n_dev, 8, lanes), jnp.float32),
                   jax.ShapeDtypeStruct(stats.shape, jnp.float32)),
        in_specs=[any_spec, any_spec, vmem_spec, vmem_spec, vmem_spec],
        out_specs=(vmem_spec, vmem_spec, any_spec, any_spec, vmem_spec),
        scratch_shapes=[
            pltpu.VMEM((n_dev, n_local, 2, cap, d_model), jnp.bfloat16),
            pltpu.VMEM((n_dev, 8, lanes), jnp.float32),
            pltpu.VMEM((n_dev, 8, lanes), jnp.float32),
            pltpu.VMEM((n_dev,) + stats.shape, jnp.float32),
            dma((2 * pairs,)), dma((2 * pairs,)), dma((n_dev,)), dma((n_dev,)),
            dma((pairs,)), dma((pairs,)), dma((n_dev,)), dma((n_dev,)),
            dma((n_dev,)), dma((n_dev,)), dma((n_local + 1,)),
        ],
        compiler_params=pltpu.CompilerParams(has_side_effects=True, vmem_limit_bytes=60 * 1024 * 1024),
        name='exchange',
    )(xd, gates, stats, w_in, w_out)


def solution(mesh):
    n_dev = mesh.shape['ep']

    def expert_layer(x_tokens, w_router, expert_idx, w_in, w_out, grad_y):
        tokens, d_model = x_tokens.shape
        n_local = w_in.shape[0]
        num_experts = n_local * n_dev
        capacity = (5 * tokens + 4 * num_experts - 1) // (4 * num_experts)
        total_tok = tokens * n_dev
        lanes = -(-capacity // 128) * 128
        idx_rows = expert_idx.reshape(-1, ROW_TOKENS)
        prob, slot_rows, gate_rows, norm_rows, stats = route(x_tokens, idx_rows, w_router, capacity)
        xd, gates = dispatch(slot_rows, x_tokens, grad_y, gate_rows, n_dev, n_local, capacity, lanes)
        gw_in, gw_out_t, back, g_back, stats = exchange(xd, gates, stats, w_in, w_out, n_dev)

        load_frac = stats[0, :num_experts] / total_tok
        mean_prob = stats[0, num_experts:2 * num_experts] / total_tok
        aux_loss = AUX_WEIGHT * num_experts * jnp.sum(load_frac * mean_prob)
        z_loss = Z_WEIGHT * stats[0, 2 * num_experts] / total_tok
        aux_vec = AUX_WEIGHT * num_experts * load_frac / total_tok
        grad_x, part, grad_w_in, grad_w_out = combine(slot_rows, back, g_back, x_tokens, prob, gate_rows, norm_rows, idx_rows, aux_vec,
                                                      2.0 * Z_WEIGHT / total_tok, w_router, gw_in, gw_out_t)
        grad_w_router = total(part, n_dev)
        return grad_x, grad_w_in, grad_w_out, grad_w_router, aux_loss, z_loss

    return jax.shard_map(expert_layer, mesh=mesh,
                         in_specs=(P('ep', None), P(None, None), P('ep'), P('ep', None, None), P('ep', None, None), P('ep', None)),
                         out_specs=(P('ep', None), P('ep', None, None), P('ep', None, None), P(None, None), P(), P()),
                         check_vma=False)
```

```python
import functools

import jax
import jax.numpy as jnp
from jax import lax
from jax.experimental import pallas as pl
from jax.experimental.pallas import tpu as pltpu
from jax.sharding import PartitionSpec as P

AUX_WEIGHT = 0.01
Z_WEIGHT = 0.001
MESH = pl.DeviceIdType.MESH
F_CHUNK = 512
TOKEN_BLOCK = 256
UNROLL = 32
ROW_TOKENS = 1024
GROUP = 2


def nt_dot(a, b):
    return lax.dot_general(a, b, (((1,), (1,)), ((), ())), preferred_element_type=jnp.float32)


def eye_mask(rows, cols):
    return lax.broadcasted_iota(jnp.int32, (rows, cols), 0) == lax.broadcasted_iota(jnp.int32, (rows, cols), 1)


def split3(v):
    hi = v.astype(jnp.bfloat16)
    rest = v - hi.astype(jnp.float32)
    mid = rest.astype(jnp.bfloat16)
    low = (rest - mid.astype(jnp.float32)).astype(jnp.bfloat16)
    return hi, mid, low


def route_kernel(capacity, x_ref, idx_ref, wr_ref, prob_ref, slot_ref, gate_ref, norm_ref, stat_ref, seen, load, prob_sum, z_sum):
    step = pl.program_id(0)
    num_experts, block = prob_ref.shape

    @pl.when(step == 0)
    def _():
        seen[...] = jnp.zeros_like(seen)
        prob_sum[...] = jnp.zeros_like(prob_sum)
        z_sum[...] = jnp.zeros_like(z_sum)

    parts = nt_dot(jnp.concatenate(split3(wr_ref[...]), axis=0), x_ref[...])
    logits = parts[:num_experts] + parts[num_experts:2 * num_experts] + parts[2 * num_experts:]
    top = jnp.max(logits, axis=0, keepdims=True)
    shifted = jnp.exp(logits - top)
    scale = jnp.sum(shifted, axis=0, keepdims=True)
    prob = shifted / scale
    log_norm = top + jnp.log(scale)
    idx = idx_ref[pl.ds(step, 1), :]
    chosen = jnp.where(lax.broadcasted_iota(jnp.int32, (num_experts, block), 0) == idx, 1.0, 0.0)
    prob_ref[...] = prob
    gate_ref[pl.ds(step, 1), :] = jnp.sum(prob * chosen, axis=0, keepdims=True)
    norm_ref[pl.ds(step, 1), :] = log_norm
    squares = log_norm * log_norm
    for i in range(0, block, 128):
        prob_sum[...] += prob[:, i:i + 128]
        z_sum[0:1, :] += squares[:, i:i + 128]
    upto = jnp.where(lax.broadcasted_iota(jnp.int32, (TOKEN_BLOCK, TOKEN_BLOCK), 0)
                     <= lax.broadcasted_iota(jnp.int32, (TOKEN_BLOCK, TOKEN_BLOCK), 1), 1.0, 0.0).astype(jnp.bfloat16)
    before = seen[:, 0:1]
    slots = []
    for i in range(0, block, TOKEN_BLOCK):
        part = chosen[:, i:i + TOKEN_BLOCK]
        count = jnp.dot(part.astype(jnp.bfloat16), upto, preferred_element_type=jnp.float32) + before
        position = jnp.sum(part * count, axis=0, keepdims=True).astype(jnp.int32) - 1
        slots.append(8 * jnp.where(position < capacity, idx[:, i:i + TOKEN_BLOCK] * capacity + position, num_experts * capacity))
        before = count[:, TOKEN_BLOCK - 1:TOKEN_BLOCK]
    slot_ref[pl.ds(step, 1), :] = jnp.concatenate(slots, axis=1)
    seen[...] = jnp.broadcast_to(before, seen.shape)

    @pl.when(step == pl.num_programs(0) - 1)
    def _():
        row = lax.broadcasted_iota(jnp.int32, (num_experts, 128), 0)
        lane = lax.broadcasted_iota(jnp.int32, (num_experts, 128), 1)
        probs = jnp.sum(prob_sum[...], axis=1, keepdims=True)
        stat_ref[...] = jnp.zeros_like(stat_ref)
        total = jnp.sum(jnp.where(row == lane, seen[...], 0.0) + jnp.where(row + num_experts == lane, probs, 0.0),
                        axis=0, keepdims=True)
        squares = jnp.sum(z_sum[0:1, :], axis=1, keepdims=True)
        stat_ref[0:1, :] = total + jnp.where(lane[0:1, :] == 2 * num_experts, squares, 0.0)


def route(x_tokens, idx_rows, w_router, capacity):
    tokens, d_model = x_tokens.shape
    num_experts = w_router.shape[1]
    steps, block = idx_rows.shape
    rows = lambda dtype: jax.ShapeDtypeStruct((steps, block), dtype)
    whole = pl.BlockSpec((steps, block), lambda i: (0, 0))
    return pl.pallas_call(
        functools.partial(route_kernel, capacity),
        grid=(steps,),
        out_shape=(jax.ShapeDtypeStruct((num_experts, tokens), jnp.float32), rows(jnp.int32), rows(jnp.float32), rows(jnp.float32),
                   jax.ShapeDtypeStruct((8, 128), jnp.float32)),
        in_specs=[pl.BlockSpec((block, d_model), lambda i: (i, 0)), whole,
                  pl.BlockSpec((num_experts, d_model), lambda i: (0, 0))],
        out_specs=(pl.BlockSpec((num_experts, block), lambda i: (0, i)), whole, whole, whole,
                   pl.BlockSpec((8, 128), lambda i: (0, 0))),
        scratch_shapes=[pltpu.VMEM((num_experts, 128), jnp.float32), pltpu.VMEM((num_experts, 128), jnp.float32),
                        pltpu.VMEM((num_experts, 128), jnp.float32), pltpu.VMEM((8, 128), jnp.float32)],
        compiler_params=pltpu.CompilerParams(dimension_semantics=('arbitrary',)),
        name='route',
    )(x_tokens, idx_rows, w_router.T)


def dispatch_kernel(steps, capacity, slot_ref, x_ref, dy_ref, gate_ref, xd_ref, gates_ref, table, stage):
    step = pl.program_id(0)
    block, d_model = x_ref.shape
    cols = d_model // 128
    lanes = gates_ref.shape[2]
    group, n_local = xd_ref.shape[:2]

    @pl.when(step == 0)
    def _():
        def clear(i, carry):
            table[pl.ds(pl.multiple_of(i * 512, 512), 512), :] = jnp.zeros((512, 128), jnp.float32)
            return carry
        lax.fori_loop(0, table.shape[0] // 512, clear, 0)

    @pl.when(step < steps)
    def _():
        for c in range(cols):
            stage[pl.ds(c, block, stride=8), :] = x_ref[:, c * 128:(c + 1) * 128].astype(jnp.float32)
            stage[pl.ds(cols + c, block, stride=8), :] = dy_ref[:, c * 128:(c + 1) * 128].astype(jnp.float32)
        eye = eye_mask(128, 128)
        gate_row = gate_ref[pl.ds(step, 1), :]
        for i in range(0, block, 128):
            gate = jnp.sum(jnp.where(eye, gate_row[:, i:i + 128], 0.0), axis=1, keepdims=True)
            stage[pl.ds(i * 8 + 2 * cols, 128, stride=8), :] = jnp.broadcast_to(gate, (128, 128))

        def place(i, carry):
            for u in range(UNROLL):
                t = i * UNROLL + u
                slot = slot_ref[step * block + t]
                table[pl.ds(pl.multiple_of(slot, 8), 8), :] = stage[pl.ds(pl.multiple_of(t * 8, 8), 8), :]
            return carry
        lax.fori_loop(0, block // UNROLL, place, 0)

    @pl.when(step >= steps)
    def _():
        gates_ref[...] = jnp.zeros_like(gates_ref)
        row = lax.broadcasted_iota(jnp.int32, (capacity, 128), 0)
        lane = lax.broadcasted_iota(jnp.int32, (capacity, 128), 1)

        def unload(i, carry):
            d = i // n_local
            e = i % n_local
            first = (((step - steps) * group + d) * n_local + e) * (capacity * 8)
            for c in range(cols):
                xd_ref[d, e, 0, :, c * 128:(c + 1) * 128] = table[pl.ds(first + c, capacity, stride=8), :].astype(jnp.bfloat16)
                xd_ref[d, e, 1, :, c * 128:(c + 1) * 128] = table[pl.ds(first + cols + c, capacity, stride=8), :].astype(jnp.bfloat16)
            gate = table[pl.ds(first + 2 * cols, capacity, stride=8), :]
            gates_ref[d, pl.ds(e, 1), :] = jnp.concatenate([
                jnp.sum(jnp.where(row == lane + c * 128, gate, 0.0), axis=0, keepdims=True)
                for c in range(lanes // 128)], axis=1)
            return carry
        lax.fori_loop(0, group * n_local, unload, 0)


def dispatch(slot_rows, x_tokens, grad_y, gate_rows, n_dev, n_local, capacity, lanes):
    tokens, d_model = x_tokens.shape
    steps, block = gate_rows.shape
    n_slots = n_dev * n_local * capacity
    table_rows = -(-(n_slots + 1) * 8 // 512) * 512
    tok = lambda i: (jnp.minimum(i, steps - 1), 0)
    dst = lambda i: jnp.maximum(i - steps, 0)
    return pl.pallas_call(
        functools.partial(dispatch_kernel, steps, capacity),
        grid=(steps + n_dev // GROUP,),
        out_shape=(jax.ShapeDtypeStruct((n_dev, n_local, 2, capacity, d_model), jnp.bfloat16),
                   jax.ShapeDtypeStruct((n_dev, 8, lanes), jnp.float32)),
        in_specs=[pl.BlockSpec(memory_space=pltpu.SMEM),
                  pl.BlockSpec((block, d_model), tok),
                  pl.BlockSpec((block, d_model), tok),
                  pl.BlockSpec((steps, block), lambda i: (0, 0))],
        out_specs=(pl.BlockSpec((GROUP, n_local, 2, capacity, d_model), lambda i: (dst(i), 0, 0, 0, 0)),
                   pl.BlockSpec((GROUP, 8, lanes), lambda i: (dst(i), 0, 0))),
        scratch_shapes=[pltpu.VMEM((table_rows, 128), jnp.float32),
                        pltpu.VMEM((block * 8, 128), jnp.float32)],
        compiler_params=pltpu.CompilerParams(dimension_semantics=('arbitrary',), vmem_limit_bytes=62 * 1024 * 1024),
        name='dispatch',
    )(slot_rows, x_tokens, grad_y, gate_rows)


def combine_kernel(fills, sources, capacity, z_coef, slot_ref, back_ref, g_ref, x_ref, prob_ref, gate_ref, norm_ref, idx_ref, aux_ref,
                   wr_t_ref, gwi_ref, gwo_t_ref, gx_ref, gwr_ref, gwi_out_ref, gwo_out_ref, table, stage):
    step = pl.program_id(0)
    block, d_model = x_ref.shape
    cols = d_model // 128
    group, n_local = back_ref.shape[:2]
    num_experts = prob_ref.shape[0]
    n_slots = sources * n_local * capacity
    gwi_out_ref[...] = gwi_ref[...]
    gwo_out_ref[0] = gwo_t_ref[0].T

    @pl.when(step == 0)
    def _():
        table[pl.ds(n_slots * 8, 8), :] = jnp.zeros((8, 128), jnp.float32)
        gwr_ref[...] = jnp.zeros_like(gwr_ref)

    @pl.when(step < fills)
    def _():
        eye = eye_mask(capacity, g_ref.shape[2])

        def load(i, carry):
            d = i // n_local
            e = i % n_local
            first = ((step * group + d) * n_local + e) * (capacity * 8)
            for c in range(cols):
                table[pl.ds(first + c, capacity, stride=8), :] = back_ref[d, e, :, c * 128:(c + 1) * 128].astype(jnp.float32)
            g_col = jnp.sum(jnp.where(eye, g_ref[d, pl.ds(e, 1), :], 0.0), axis=1, keepdims=True)
            table[pl.ds(first + cols, capacity, stride=8), :] = jnp.broadcast_to(g_col, (capacity, 128))
            return carry
        lax.fori_loop(0, group * n_local, load, 0)

    @pl.when(step >= fills)
    def _():
        part = step - fills

        def pick(i, carry):
            for u in range(UNROLL):
                t = i * UNROLL + u
                slot = slot_ref[part * block + t]
                stage[pl.ds(pl.multiple_of(t * 8, 8), 8), :] = table[pl.ds(pl.multiple_of(slot, 8), 8), :]
            return carry
        lax.fori_loop(0, block // UNROLL, pick, 0)
        eye = eye_mask(128, 128)
        g_tok = jnp.concatenate([
            jnp.sum(jnp.where(eye, stage[pl.ds(i * 8 + cols, 128, stride=8), :], 0.0), axis=0, keepdims=True)
            for i in range(0, block, 128)], axis=1)
        here = pl.ds(part, 1)
        prob = prob_ref[...]
        chosen = jnp.where(lax.broadcasted_iota(jnp.int32, (num_experts, block), 0) == idx_ref[here, :], 1.0, 0.0)
        aux_vec = aux_ref[:, 0:1]
        spread = jnp.sum(prob * aux_vec, axis=0, keepdims=True)
        d_logits = ((gate_ref[here, :] * g_tok) * (chosen - prob) + prob * (aux_vec - spread)
                    + (z_coef * norm_ref[here, :]) * prob)
        hi, mid, low = split3(d_logits)
        gwr_ref[...] += jnp.dot(jnp.concatenate([hi, mid, low], axis=0), x_ref[...], preferred_element_type=jnp.float32)
        left = jnp.concatenate([hi, mid, hi, low, mid, hi], axis=0)
        w_hi, w_mid, w_low = split3(wr_t_ref[...])
        right = jnp.concatenate([w_hi, w_hi, w_mid, w_hi, w_mid, w_low], axis=0)
        dx_router = lax.dot_general(left, right, (((0,), (0,)), ((), ())), preferred_element_type=jnp.float32)
        for c in range(cols):
            span = slice(c * 128, (c + 1) * 128)
            gx_ref[:, span] = (stage[pl.ds(c, block, stride=8), :] + dx_router[:, span]).astype(jnp.bfloat16)


def combine(slot_rows, back, g_back, x_tokens, prob, gate_rows, norm_rows, idx_rows, aux_vec, z_coef, w_router, gw_in, gw_out_t):
    n_dev, n_local, capacity, d_model = back.shape
    tokens = x_tokens.shape[0]
    num_experts = prob.shape[0]
    d_ff = gw_in.shape[2]
    blocks, block = gate_rows.shape
    fills = n_dev // GROUP
    steps = fills + blocks
    lanes = g_back.shape[2]
    n_slots = n_dev * n_local * capacity
    gw_in_rows = gw_in.reshape(n_local * d_model, d_ff)
    in_rows = n_local * d_model // steps
    out_cols = d_ff // 256
    src = lambda i: jnp.minimum(i, fills - 1)
    tok = lambda i: (jnp.maximum(i - fills, 0), 0)
    flip = lambda i: jnp.minimum(i, n_local * out_cols - 1)
    rows = pl.BlockSpec((blocks, block), lambda i: (0, 0))
    gx, gwr, gw_in_out, gw_out = pl.pallas_call(
        functools.partial(combine_kernel, fills, n_dev, capacity, z_coef),
        grid=(steps,),
        out_shape=(jax.ShapeDtypeStruct((tokens, d_model), jnp.bfloat16),
                   jax.ShapeDtypeStruct((3 * num_experts, d_model), jnp.float32),
                   jax.ShapeDtypeStruct((n_local * d_model, d_ff), jnp.float32),
                   jax.ShapeDtypeStruct((n_local, d_ff, d_model), jnp.float32)),
        in_specs=[pl.BlockSpec(memory_space=pltpu.SMEM),
                  pl.BlockSpec((GROUP, n_local, capacity, d_model), lambda i: (src(i), 0, 0, 0)),
                  pl.BlockSpec((GROUP, 8, lanes), lambda i: (src(i), 0, 0)),
                  pl.BlockSpec((block, d_model), tok),
                  pl.BlockSpec((num_experts, block), lambda i: (0, jnp.maximum(i - fills, 0))),
                  rows, rows, rows,
                  pl.BlockSpec((num_experts, 128), lambda i: (0, 0)),
                  pl.BlockSpec((num_experts, d_model), lambda i: (0, 0)),
                  pl.BlockSpec((in_rows, d_ff), lambda i: (i, 0)),
                  pl.BlockSpec((1, d_model, 256), lambda i: (flip(i) // out_cols, 0, flip(i) % out_cols))],
        out_specs=(pl.BlockSpec((block, d_model), tok),
                   pl.BlockSpec((3 * num_experts, d_model), lambda i: (0, 0)),
                   pl.BlockSpec((in_rows, d_ff), lambda i: (i, 0)),
                   pl.BlockSpec((1, 256, d_model), lambda i: (flip(i) // out_cols, flip(i) % out_cols, 0))),
        scratch_shapes=[pltpu.VMEM(((n_slots + 1) * 8, 128), jnp.float32),
                        pltpu.VMEM((block * 8, 128), jnp.float32)],
        compiler_params=pltpu.CompilerParams(dimension_semantics=('arbitrary',), vmem_limit_bytes=63 * 1024 * 1024),
        name='combine',
    )(slot_rows, back, g_back, x_tokens, prob, gate_rows, norm_rows, idx_rows,
      jnp.broadcast_to(aux_vec[:, None], (num_experts, 128)), w_router.T, gw_in_rows, gw_out_t)
    part = gwr.reshape(3, num_experts, d_model)
    return gx, (part[0] + part[1] + part[2]).T, gw_in_out.reshape(n_local, d_model, d_ff), gw_out


def flip_bits(me, k, n):
    out = 0
    bit = 1
    while bit < n:
        mine = (me // bit) % 2
        flip = (k // bit) % 2
        out = out + bit * (mine + flip - 2 * mine * flip)
        bit *= 2
    return out


def total_kernel(n, part_ref, out_ref, inbox, mine, a_send, a_recv, b_send, b_recv):
    me = lax.axis_index('ep')

    def scatter(k):
        peer = flip_bits(me, k, n)
        return pltpu.make_async_remote_copy(src_ref=part_ref.at[peer], dst_ref=inbox.at[me], send_sem=a_send.at[k],
                                            recv_sem=a_recv.at[k], device_id=(peer,), device_id_type=MESH)

    def spread(k):
        peer = flip_bits(me, k, n)
        return pltpu.make_async_remote_copy(src_ref=mine, dst_ref=out_ref.at[me], send_sem=b_send.at[k],
                                            recv_sem=b_recv.at[k], device_id=(peer,), device_id_type=MESH)

    for k in range(1, n):
        scatter(k).start()
    inbox[me] = part_ref[me]
    for k in range(1, n):
        scatter(k).wait_recv()
    total = inbox[0]
    for i in range(1, n):
        total = total + inbox[i]
    mine[...] = total
    out_ref[me] = total
    for k in range(1, n):
        spread(k).start()
    for k in range(1, n):
        scatter(k).wait_send()
        spread(k).wait()


def total(part, n_dev):
    rows, cols = part.shape
    piece = rows * cols // (n_dev * 128)
    chunks = jnp.pad(part.reshape(n_dev, piece, 128), ((0, 0), (0, -piece % 8), (0, 0)))
    dma = pltpu.SemaphoreType.DMA
    vmem_spec = pl.BlockSpec(memory_space=pltpu.VMEM)
    out = pl.pallas_call(
        functools.partial(total_kernel, n_dev),
        out_shape=jax.ShapeDtypeStruct(chunks.shape, jnp.float32),
        in_specs=[vmem_spec],
        out_specs=vmem_spec,
        scratch_shapes=[pltpu.VMEM(chunks.shape, jnp.float32), pltpu.VMEM(chunks.shape[1:], jnp.float32),
                        dma((n_dev,)), dma((n_dev,)), dma((n_dev,)), dma((n_dev,))],
        compiler_params=pltpu.CompilerParams(has_side_effects=True),
        name='total',
    )(chunks)
    return out[:, :piece].reshape(rows, cols)


def tile_at(t):
    quarter = t // 4
    edge = (7 - quarter) // 7 + quarter // 7
    turn = (t + 4) % 8
    piece = (1 - edge) * (turn // 2) + edge * (t % 4)
    stage = (t + 4) // 8
    chip = stage * (7 - stage) // 2 + stage // 4
    chip = chip + (1 - edge) * (turn % 2) * (7 - 2 * chip)
    return chip * 2 + piece // 2, piece % 2


def link_sets(n, n_local):
    assert n == 16
    pieces = []
    for chips in ((3, 4), (5, 2), (6, 1), (7,)):
        pieces.append([[(chip * 2 + c, e) for c in range(2) for e in range(n_local)] for chip in chips])
    return pieces


def exchange_kernel(n, n_local, xd_ref, gate_ref, stat_ref, w_in_hbm, w_out_hbm,
                    gw_in_hbm, gw_out_t_hbm, back_ref, g_back_ref, stat_out_ref,
                    w_in_ref, w_out_ref, gw_in_ref, gw_out_t_ref, xr, gate_r, g_s, stat_r,
                    fwd_send, fwd_recv, gate_send, gate_recv,
                    ret_send, ret_recv, g_send, g_recv, stat_send, stat_recv, loc_sem):
    me = lax.axis_index('ep')
    cap, d_model = xr.shape[3], xr.shape[4]
    d_ff = w_in_ref.shape[2]

    def peer_of(k):
        return flip_bits(me, k, n)

    def fwd_copy(k, e, part):
        sem = (k * n_local + e) * 2 + part
        peer = peer_of(k)
        return pltpu.make_async_remote_copy(
            src_ref=xd_ref.at[peer, e, part], dst_ref=xr.at[k, e, part],
            send_sem=fwd_send.at[sem], recv_sem=fwd_recv.at[sem],
            device_id=(peer,), device_id_type=MESH)

    def gate_copy(k):
        peer = peer_of(k)
        return pltpu.make_async_remote_copy(
            src_ref=gate_ref.at[peer], dst_ref=gate_r.at[k],
            send_sem=gate_send.at[k], recv_sem=gate_recv.at[k],
            device_id=(peer,), device_id_type=MESH)

    def stat_copy(k):
        return pltpu.make_async_remote_copy(
            src_ref=stat_ref, dst_ref=stat_r.at[me],
            send_sem=stat_send.at[k], recv_sem=stat_recv.at[k],
            device_id=(peer_of(k),), device_id_type=MESH)

    def ret_copy(k, e):
        sem = k * n_local + e
        return pltpu.make_async_remote_copy(
            src_ref=xr.at[k, e, 0], dst_ref=back_ref.at[me, e],
            send_sem=ret_send.at[sem], recv_sem=ret_recv.at[sem],
            device_id=(peer_of(k),), device_id_type=MESH)

    def g_copy(k):
        return pltpu.make_async_remote_copy(
            src_ref=g_s.at[k], dst_ref=g_back_ref.at[me],
            send_sem=g_send.at[k], recv_sem=g_recv.at[k],
            device_id=(peer_of(k),), device_id_type=MESH)

    sets = link_sets(n, n_local)

    def interleave(queues):
        return [queue[i] for i in range(len(queues[0])) for queue in queues]

    def send_rows(queues):
        for k, e in interleave(queues):
            if e == 0:
                gate_copy(k).start()
                stat_copy(k).start()
            for part in range(2):
                fwd_copy(k, e, part).start()

    def rows_left(queues):
        for queue in queues:
            for i, (k, e) in enumerate(queue):
                fwd_copy(k, e, 0).wait_send()
                if i < len(queue) - 1:
                    fwd_copy(k, e, 1).wait_send()

    def send_grads(queues):
        for k, e in interleave(queues):
            ret_copy(k, e).start()
            if e == n_local - 1:
                g_copy(k).start()

    def grads_left(queues):
        for queue in queues:
            for k, e in queue[:-1]:
                ret_copy(k, e).wait_send()

    near = [[(1, e) for e in range(n_local)]]
    own_in = [pltpu.make_async_copy(xd_ref.at[me, e], xr.at[0, e], loc_sem.at[e]) for e in range(n_local)]
    own_gate = pltpu.make_async_copy(gate_ref.at[me], gate_r.at[0], loc_sem.at[n_local])
    own_out = [pltpu.make_async_copy(xr.at[0, e, 0], back_ref.at[me, e], loc_sem.at[e]) for e in range(n_local)]
    own_g = pltpu.make_async_copy(g_s.at[0], g_back_ref.at[me], loc_sem.at[n_local])

    send_rows(sets[0])
    send_rows(near)
    for c in own_in:
        c.start()
    own_gate.start()
    weights = [pltpu.make_async_copy(w_in_hbm, w_in_ref, loc_sem.at[n_local + 1]),
               pltpu.make_async_copy(w_out_hbm, w_out_ref, loc_sem.at[n_local + 2])]
    for c in weights:
        c.start()
    gw_in_ref[...] = jnp.zeros_like(gw_in_ref)
    gw_out_t_ref[...] = jnp.zeros_like(gw_out_t_ref)
    g_s[...] = jnp.zeros_like(g_s)
    stat_r[me] = stat_ref[...]
    for c in own_in:
        c.wait()
    own_gate.wait()
    for c in weights:
        c.wait()

    lanes = gate_r.shape[2]

    def tile(k, e):
        eye = (lax.broadcasted_iota(jnp.int32, (cap, lanes), 0)
               == lax.broadcasted_iota(jnp.int32, (cap, lanes), 1))
        rows = xr[k, e, 0]
        dy = xr[k, e, 1].astype(jnp.float32)
        gate_row = gate_r[k, pl.ds(e, 1), :]
        gate_col = jnp.sum(jnp.where(eye, gate_row, 0.0), axis=1, keepdims=True)
        grad = (gate_col * dy).astype(jnp.bfloat16)
        rows_t = rows.T
        grad_t = grad.T
        out = jnp.zeros((cap, d_model), jnp.float32)
        d_rows = jnp.zeros((cap, d_model), jnp.float32)
        for f in range(0, d_ff, F_CHUNK):
            fs = pl.ds(f, F_CHUNK)
            w_a = w_in_ref[e, :, fs]
            w_b = w_out_ref[e, fs, :]
            pre = jnp.dot(rows, w_a, preferred_element_type=jnp.float32)
            hid = jnp.maximum(pre, 0.0).astype(jnp.bfloat16)
            out = out + jnp.dot(hid, w_b, preferred_element_type=jnp.float32)
            d_hid = nt_dot(grad, w_b)
            d_pre = jnp.where(hid.astype(jnp.float32) > 0, d_hid, 0.0).astype(jnp.bfloat16)
            gw_out_t_ref[e, :, fs] += jnp.dot(grad_t, hid, preferred_element_type=jnp.float32)
            gw_in_ref[e, :, fs] += jnp.dot(rows_t, d_pre, preferred_element_type=jnp.float32)
            d_rows = d_rows + nt_dot(d_pre, w_a)
        out = out.astype(jnp.bfloat16).astype(jnp.float32)
        g_col = jnp.sum(out * dy, axis=1, keepdims=True)
        g_s[k, pl.ds(e, 1), :] = jnp.sum(jnp.where(eye, g_col, 0.0), axis=0, keepdims=True)
        xr[k, e, 0] = d_rows.astype(jnp.bfloat16)

    order = [(0, e) for e in range(n_local)] + near[0]
    first = []
    for queues in sets:
        first.append(len(order))
        order = order + interleave(queues)
    assert order == [tile_at(t) for t in range(len(order))]

    def own_back():
        send_grads(near)
        for c in own_out:
            c.start()
        own_g.start()

    def after_rows(done, then):
        def run():
            rows_left(sets[done])
            then()
        return run

    def after_grads(done, then):
        def run():
            grads_left(sets[done])
            then()
        return run

    events = {
        first[0]: own_back,
        first[1] - 2: after_rows(0, lambda: send_rows(sets[1])),
        first[2] - 2: after_rows(1, lambda: send_grads(sets[0])),
        first[2]: after_grads(0, lambda: send_rows(sets[2])),
        first[3] - 2: after_rows(2, lambda: send_grads(sets[1])),
        first[3]: after_grads(1, lambda: send_rows(sets[3])),
        len(order) - 1: after_rows(3, lambda: send_grads(sets[2])),
    }

    def step(t, carry):
        k, e = tile_at(t)
        for at, run in events.items():
            pl.when(t == at)(run)

        @pl.when(t >= n_local)
        def _():
            @pl.when(e == 0)
            def _():
                gate_copy(k).wait_recv()
            for part in range(2):
                fwd_copy(k, e, part).wait_recv()

        tile(k, e)
        return carry

    lax.fori_loop(0, len(order), step, 0)
    totals = [pltpu.make_async_copy(gw_in_ref, gw_in_hbm, loc_sem.at[n_local + 1]),
              pltpu.make_async_copy(gw_out_t_ref, gw_out_t_hbm, loc_sem.at[n_local + 2])]
    for c in totals:
        c.start()
    grads_left(sets[2])
    send_grads(sets[3])

    for queues in sets:
        for queue in queues:
            k, e = queue[-1]
            fwd_copy(k, e, 1).wait_send()
            if queues is not sets[3]:
                ret_copy(k, e).wait_send()
    grads_left(sets[3])
    for queue in sets[3]:
        ret_copy(*queue[-1]).wait_send()
    for k, e in near[0]:
        for part in range(2):
            fwd_copy(k, e, part).wait_send()
        ret_copy(k, e).wait_send()
    for c in own_out:
        c.wait()
    own_g.wait()
    for c in totals:
        c.wait()

    def drain(k, carry):
        gate_copy(k).wait_send()
        stat_copy(k).wait()
        g_copy(k).wait()
        for e in range(n_local):
            ret_copy(k, e).wait_recv()
        return carry

    lax.fori_loop(1, n, drain, 0)
    stat = stat_r[0]
    for i in range(1, n):
        stat = stat + stat_r[i]
    stat_out_ref[...] = stat


def exchange(xd, gates, stats, w_in, w_out, n_dev):
    n_local, d_model, d_ff = w_in.shape
    cap = xd.shape[3]
    lanes = gates.shape[2]
    any_spec = pl.BlockSpec(memory_space=pl.ANY)
    vmem_spec = pl.BlockSpec(memory_space=pltpu.VMEM)
    pairs = n_dev * n_local
    dma = pltpu.SemaphoreType.DMA
    return pl.pallas_call(
        functools.partial(exchange_kernel, n_dev, n_local),
        out_shape=(jax.ShapeDtypeStruct((n_local, d_model, d_ff), jnp.float32),
                   jax.ShapeDtypeStruct((n_local, d_model, d_ff), jnp.float32),
                   jax.ShapeDtypeStruct((n_dev, n_local, cap, d_model), jnp.bfloat16),
                   jax.ShapeDtypeStruct((n_dev, 8, lanes), jnp.float32),
                   jax.ShapeDtypeStruct(stats.shape, jnp.float32)),
        in_specs=[any_spec, any_spec, vmem_spec, any_spec, any_spec],
        out_specs=(any_spec, any_spec, any_spec, any_spec, vmem_spec),
        scratch_shapes=[
            pltpu.VMEM(w_in.shape, jnp.bfloat16),
            pltpu.VMEM(w_out.shape, jnp.bfloat16),
            pltpu.VMEM(w_in.shape, jnp.float32),
            pltpu.VMEM(w_in.shape, jnp.float32),
            pltpu.VMEM((n_dev, n_local, 2, cap, d_model), jnp.bfloat16),
            pltpu.VMEM((n_dev, 8, lanes), jnp.float32),
            pltpu.VMEM((n_dev, 8, lanes), jnp.float32),
            pltpu.VMEM((n_dev,) + stats.shape, jnp.float32),
            dma((2 * pairs,)), dma((2 * pairs,)), dma((n_dev,)), dma((n_dev,)),
            dma((pairs,)), dma((pairs,)), dma((n_dev,)), dma((n_dev,)),
            dma((n_dev,)), dma((n_dev,)), dma((n_local + 3,)),
        ],
        compiler_params=pltpu.CompilerParams(has_side_effects=True, vmem_limit_bytes=60 * 1024 * 1024),
        name='exchange',
    )(xd, gates, stats, w_in, w_out)


def solution(mesh):
    n_dev = mesh.shape['ep']

    def expert_layer(x_tokens, w_router, expert_idx, w_in, w_out, grad_y):
        tokens, d_model = x_tokens.shape
        n_local = w_in.shape[0]
        num_experts = n_local * n_dev
        capacity = (5 * tokens + 4 * num_experts - 1) // (4 * num_experts)
        total_tok = tokens * n_dev
        lanes = -(-capacity // 128) * 128
        idx_rows = expert_idx.reshape(-1, ROW_TOKENS)
        prob, slot_rows, gate_rows, norm_rows, stats = route(x_tokens, idx_rows, w_router, capacity)
        slot_rows = slot_rows.reshape(tokens)
        xd, gates = dispatch(slot_rows, x_tokens, grad_y, gate_rows, n_dev, n_local, capacity, lanes)
        gw_in, gw_out_t, back, g_back, stats = exchange(xd, gates, stats, w_in, w_out, n_dev)

        load_frac = stats[0, :num_experts] / total_tok
        mean_prob = stats[0, num_experts:2 * num_experts] / total_tok
        aux_loss = AUX_WEIGHT * num_experts * jnp.sum(load_frac * mean_prob)
        z_loss = Z_WEIGHT * stats[0, 2 * num_experts] / total_tok
        aux_vec = AUX_WEIGHT * num_experts * load_frac / total_tok
        grad_x, part, grad_w_in, grad_w_out = combine(slot_rows, back, g_back, x_tokens, prob, gate_rows, norm_rows, idx_rows, aux_vec,
                                                      2.0 * Z_WEIGHT / total_tok, w_router, gw_in, gw_out_t)
        grad_w_router = total(part, n_dev)
        return grad_x, grad_w_in, grad_w_out, grad_w_router, aux_loss, z_loss

    return jax.shard_map(expert_layer, mesh=mesh,
                         in_specs=(P('ep', None), P(None, None), P('ep'), P('ep', None, None), P('ep', None, None), P('ep', None)),
                         out_specs=(P('ep', None), P('ep', None, None), P('ep', None, None), P(None, None), P(), P()),
                         check_vma=False)
```

```python
import functools

import jax
import jax.numpy as jnp
from jax import lax
from jax.experimental import pallas as pl
from jax.experimental.pallas import tpu as pltpu
from jax.sharding import PartitionSpec as P

AUX_WEIGHT = 0.01
Z_WEIGHT = 0.001
MESH = pl.DeviceIdType.MESH
F_CHUNK = 512
TOKEN_BLOCK = 256
UNROLL = 32
ROW_TOKENS = 1024
GROUP = 2


def nt_dot(a, b):
    return lax.dot_general(a, b, (((1,), (1,)), ((), ())), preferred_element_type=jnp.float32)


def eye_mask(rows, cols):
    return lax.broadcasted_iota(jnp.int32, (rows, cols), 0) == lax.broadcasted_iota(jnp.int32, (rows, cols), 1)


def split3(v):
    hi = v.astype(jnp.bfloat16)
    rest = v - hi.astype(jnp.float32)
    mid = rest.astype(jnp.bfloat16)
    low = (rest - mid.astype(jnp.float32)).astype(jnp.bfloat16)
    return hi, mid, low


def route_kernel(capacity, x_ref, idx_ref, wr_ref, prob_ref, slot_ref, pos_ref, gate_ref, norm_ref, stat_ref, seen, prob_sum, z_sum):
    step = pl.program_id(0)
    num_experts, block = prob_ref.shape

    @pl.when(step == 0)
    def _():
        seen[...] = jnp.zeros_like(seen)
        prob_sum[...] = jnp.zeros_like(prob_sum)
        z_sum[...] = jnp.zeros_like(z_sum)

    parts = nt_dot(jnp.concatenate(split3(wr_ref[...]), axis=0), x_ref[...])
    logits = parts[:num_experts] + parts[num_experts:2 * num_experts] + parts[2 * num_experts:]
    top = jnp.max(logits, axis=0, keepdims=True)
    shifted = jnp.exp(logits - top)
    scale = jnp.sum(shifted, axis=0, keepdims=True)
    prob = shifted / scale
    log_norm = top + jnp.log(scale)
    idx = idx_ref[pl.ds(step, 1), :]
    chosen = jnp.where(lax.broadcasted_iota(jnp.int32, (num_experts, block), 0) == idx, 1.0, 0.0)
    prob_ref[...] = prob
    gate_ref[pl.ds(step, 1), :] = jnp.sum(prob * chosen, axis=0, keepdims=True)
    norm_ref[pl.ds(step, 1), :] = log_norm
    squares = log_norm * log_norm
    for i in range(0, block, 128):
        prob_sum[...] += prob[:, i:i + 128]
        z_sum[0:1, :] += squares[:, i:i + 128]
    upto = jnp.where(lax.broadcasted_iota(jnp.int32, (TOKEN_BLOCK, TOKEN_BLOCK), 0)
                     <= lax.broadcasted_iota(jnp.int32, (TOKEN_BLOCK, TOKEN_BLOCK), 1), 1.0, 0.0).astype(jnp.bfloat16)
    before = seen[:, 0:1]
    slots = []
    places = []
    for i in range(0, block, TOKEN_BLOCK):
        part = chosen[:, i:i + TOKEN_BLOCK]
        count = jnp.dot(part.astype(jnp.bfloat16), upto, preferred_element_type=jnp.float32) + before
        position = jnp.sum(part * count, axis=0, keepdims=True).astype(jnp.int32) - 1
        places.append(position)
        slots.append(8 * jnp.where(position < capacity, idx[:, i:i + TOKEN_BLOCK] * capacity + position, num_experts * capacity))
        before = count[:, TOKEN_BLOCK - 1:TOKEN_BLOCK]
    slot_ref[pl.ds(step, 1), :] = jnp.concatenate(slots, axis=1)
    pos_ref[pl.ds(step, 1), :] = jnp.concatenate(places, axis=1)
    seen[...] = jnp.broadcast_to(before, seen.shape)

    @pl.when(step == pl.num_programs(0) - 1)
    def _():
        row = lax.broadcasted_iota(jnp.int32, (num_experts, 128), 0)
        lane = lax.broadcasted_iota(jnp.int32, (num_experts, 128), 1)
        probs = jnp.sum(prob_sum[...], axis=1, keepdims=True)
        stat_ref[...] = jnp.zeros_like(stat_ref)
        total = jnp.sum(jnp.where(row == lane, seen[...], 0.0) + jnp.where(row + num_experts == lane, probs, 0.0),
                        axis=0, keepdims=True)
        squares = jnp.sum(z_sum[0:1, :], axis=1, keepdims=True)
        stat_ref[0:1, :] = total + jnp.where(lane[0:1, :] == 2 * num_experts, squares, 0.0)


def route(x_tokens, idx_rows, w_router, capacity):
    tokens, d_model = x_tokens.shape
    num_experts = w_router.shape[1]
    steps, block = idx_rows.shape
    rows = lambda dtype: jax.ShapeDtypeStruct((steps, block), dtype)
    whole = pl.BlockSpec((steps, block), lambda i: (0, 0))
    return pl.pallas_call(
        functools.partial(route_kernel, capacity),
        grid=(steps,),
        out_shape=(jax.ShapeDtypeStruct((num_experts, tokens), jnp.float32), rows(jnp.int32), rows(jnp.int32), rows(jnp.float32), rows(jnp.float32),
                   jax.ShapeDtypeStruct((8, 128), jnp.float32)),
        in_specs=[pl.BlockSpec((block, d_model), lambda i: (i, 0)), whole,
                  pl.BlockSpec((num_experts, d_model), lambda i: (0, 0))],
        out_specs=(pl.BlockSpec((num_experts, block), lambda i: (0, i)), whole, whole, whole, whole,
                   pl.BlockSpec((8, 128), lambda i: (0, 0))),
        scratch_shapes=[pltpu.VMEM((num_experts, 128), jnp.float32), pltpu.VMEM((num_experts, 128), jnp.float32), pltpu.VMEM((8, 128), jnp.float32)],
        compiler_params=pltpu.CompilerParams(dimension_semantics=('arbitrary',)),
        name='route',
    )(x_tokens, idx_rows, w_router.T)


def dispatch_kernel(steps, capacity, slot_ref, x_ref, dy_ref, gate_ref, xd_ref, gates_ref, table, stage):
    step = pl.program_id(0)
    block, d_model = x_ref.shape
    cols = d_model // 128
    lanes = gates_ref.shape[2]
    group, n_local = xd_ref.shape[:2]

    @pl.when(step == 0)
    def _():
        def clear(i, carry):
            table[pl.ds(pl.multiple_of(i * 512, 512), 512), :] = jnp.zeros((512, 128), jnp.float32)
            return carry
        lax.fori_loop(0, table.shape[0] // 512, clear, 0)

    @pl.when(step < steps)
    def _():
        for c in range(cols):
            stage[pl.ds(c, block, stride=8), :] = x_ref[:, c * 128:(c + 1) * 128].astype(jnp.float32)
            stage[pl.ds(cols + c, block, stride=8), :] = dy_ref[:, c * 128:(c + 1) * 128].astype(jnp.float32)
        eye = eye_mask(128, 128)
        gate_row = gate_ref[pl.ds(step, 1), :]
        for i in range(0, block, 128):
            gate = jnp.sum(jnp.where(eye, gate_row[:, i:i + 128], 0.0), axis=1, keepdims=True)
            stage[pl.ds(i * 8 + 2 * cols, 128, stride=8), :] = jnp.broadcast_to(gate, (128, 128))

        def place(i, carry):
            for u in range(UNROLL):
                t = i * UNROLL + u
                slot = slot_ref[step * block + t]
                table[pl.ds(pl.multiple_of(slot, 8), 8), :] = stage[pl.ds(pl.multiple_of(t * 8, 8), 8), :]
            return carry
        lax.fori_loop(0, block // UNROLL, place, 0)

    @pl.when(step >= steps)
    def _():
        gates_ref[...] = jnp.zeros_like(gates_ref)
        row = lax.broadcasted_iota(jnp.int32, (capacity, 128), 0)
        lane = lax.broadcasted_iota(jnp.int32, (capacity, 128), 1)

        def unload(i, carry):
            d = i // n_local
            e = i % n_local
            first = (((step - steps) * group + d) * n_local + e) * (capacity * 8)
            for c in range(cols):
                xd_ref[d, e, 0, :, c * 128:(c + 1) * 128] = table[pl.ds(first + c, capacity, stride=8), :].astype(jnp.bfloat16)
                xd_ref[d, e, 1, :, c * 128:(c + 1) * 128] = table[pl.ds(first + cols + c, capacity, stride=8), :].astype(jnp.bfloat16)
            gate = table[pl.ds(first + 2 * cols, capacity, stride=8), :]
            gates_ref[d, pl.ds(e, 1), :] = jnp.concatenate([
                jnp.sum(jnp.where(row == lane + c * 128, gate, 0.0), axis=0, keepdims=True)
                for c in range(lanes // 128)], axis=1)
            return carry
        lax.fori_loop(0, group * n_local, unload, 0)


def dispatch(slot_rows, x_tokens, grad_y, gate_rows, n_dev, n_local, capacity, lanes):
    tokens, d_model = x_tokens.shape
    steps, block = gate_rows.shape
    n_slots = n_dev * n_local * capacity
    table_rows = -(-(n_slots + 1) * 8 // 512) * 512
    tok = lambda i: (jnp.minimum(i, steps - 1), 0)
    dst = lambda i: jnp.maximum(i - steps, 0)
    return pl.pallas_call(
        functools.partial(dispatch_kernel, steps, capacity),
        grid=(steps + n_dev // GROUP,),
        out_shape=(jax.ShapeDtypeStruct((n_dev, n_local, 2, capacity, d_model), jnp.bfloat16),
                   jax.ShapeDtypeStruct((n_dev, 8, lanes), jnp.float32)),
        in_specs=[pl.BlockSpec(memory_space=pltpu.SMEM),
                  pl.BlockSpec((block, d_model), tok),
                  pl.BlockSpec((block, d_model), tok),
                  pl.BlockSpec((steps, block), lambda i: (0, 0))],
        out_specs=(pl.BlockSpec((GROUP, n_local, 2, capacity, d_model), lambda i: (dst(i), 0, 0, 0, 0)),
                   pl.BlockSpec((GROUP, 8, lanes), lambda i: (dst(i), 0, 0))),
        scratch_shapes=[pltpu.VMEM((table_rows, 128), jnp.float32),
                        pltpu.VMEM((block * 8, 128), jnp.float32)],
        compiler_params=pltpu.CompilerParams(dimension_semantics=('arbitrary',), vmem_limit_bytes=62 * 1024 * 1024),
        name='dispatch',
    )(slot_rows, x_tokens, grad_y, gate_rows)


def combine_kernel(fills, sources, capacity, slot_ref, back_ref, dl_ref, wr_t_ref, gwi_ref, gwo_t_ref,
                   gx_ref, gwi_out_ref, gwo_out_ref, table, stage):
    step = pl.program_id(0)
    block, d_model = gx_ref.shape
    cols = d_model // 128
    group, n_local = back_ref.shape[:2]
    n_slots = sources * n_local * capacity
    gwi_out_ref[...] = gwi_ref[...]
    gwo_out_ref[0] = gwo_t_ref[0].T

    @pl.when(step == 0)
    def _():
        table[pl.ds(n_slots * 8, 8), :] = jnp.zeros((8, 128), jnp.float32)

    @pl.when(step < fills)
    def _():
        def load(i, carry):
            d = i // n_local
            e = i % n_local
            first = ((step * group + d) * n_local + e) * (capacity * 8)
            for c in range(cols):
                table[pl.ds(first + c, capacity, stride=8), :] = back_ref[d, e, :, c * 128:(c + 1) * 128].astype(jnp.float32)
            return carry
        lax.fori_loop(0, group * n_local, load, 0)

    @pl.when(step >= fills)
    def _():
        part = step - fills

        def pick(i, carry):
            for u in range(UNROLL):
                t = i * UNROLL + u
                slot = slot_ref[part * block + t]
                stage[pl.ds(pl.multiple_of(t * 8, 8), 8), :] = table[pl.ds(pl.multiple_of(slot, 8), 8), :]
            return carry
        lax.fori_loop(0, block // UNROLL, pick, 0)
        hi, mid, low = split3(dl_ref[...])
        left = jnp.concatenate([hi, mid, hi, low, mid, hi], axis=0)
        w_hi, w_mid, w_low = split3(wr_t_ref[...])
        right = jnp.concatenate([w_hi, w_hi, w_mid, w_hi, w_mid, w_low], axis=0)
        dx_router = lax.dot_general(left, right, (((0,), (0,)), ((), ())), preferred_element_type=jnp.float32)
        for c in range(cols):
            span = slice(c * 128, (c + 1) * 128)
            gx_ref[:, span] = (stage[pl.ds(c, block, stride=8), :] + dx_router[:, span]).astype(jnp.bfloat16)


def combine(slot_rows, back, d_logits, w_router, gw_in, gw_out_t):
    n_dev, n_local, capacity, d_model = back.shape
    num_experts, tokens = d_logits.shape
    d_ff = gw_in.shape[2]
    block = ROW_TOKENS
    blocks = tokens // block
    fills = n_dev // GROUP
    steps = fills + blocks
    n_slots = n_dev * n_local * capacity
    gw_in_rows = gw_in.reshape(n_local * d_model, d_ff)
    in_rows = n_local * d_model // steps
    out_cols = d_ff // 256
    src = lambda i: jnp.minimum(i, fills - 1)
    tok = lambda i: (jnp.maximum(i - fills, 0), 0)
    flip = lambda i: jnp.minimum(i, n_local * out_cols - 1)
    gx, gw_in_out, gw_out = pl.pallas_call(
        functools.partial(combine_kernel, fills, n_dev, capacity),
        grid=(steps,),
        out_shape=(jax.ShapeDtypeStruct((tokens, d_model), jnp.bfloat16),
                   jax.ShapeDtypeStruct((n_local * d_model, d_ff), jnp.float32),
                   jax.ShapeDtypeStruct((n_local, d_ff, d_model), jnp.float32)),
        in_specs=[pl.BlockSpec(memory_space=pltpu.SMEM),
                  pl.BlockSpec((GROUP, n_local, capacity, d_model), lambda i: (src(i), 0, 0, 0)),
                  pl.BlockSpec((num_experts, block), lambda i: (0, jnp.maximum(i - fills, 0))),
                  pl.BlockSpec((num_experts, d_model), lambda i: (0, 0)),
                  pl.BlockSpec((in_rows, d_ff), lambda i: (i, 0)),
                  pl.BlockSpec((1, d_model, 256), lambda i: (flip(i) // out_cols, 0, flip(i) % out_cols))],
        out_specs=(pl.BlockSpec((block, d_model), tok),
                   pl.BlockSpec((in_rows, d_ff), lambda i: (i, 0)),
                   pl.BlockSpec((1, 256, d_model), lambda i: (flip(i) // out_cols, flip(i) % out_cols, 0))),
        scratch_shapes=[pltpu.VMEM(((n_slots + 1) * 8, 128), jnp.float32),
                        pltpu.VMEM((block * 8, 128), jnp.float32)],
        compiler_params=pltpu.CompilerParams(dimension_semantics=('arbitrary',), vmem_limit_bytes=63 * 1024 * 1024),
        name='combine',
    )(slot_rows, back, d_logits, w_router.T, gw_in_rows, gw_out_t)
    return gx, gw_in_out.reshape(n_local, d_model, d_ff), gw_out


def flip_bits(me, k, n):
    out = 0
    bit = 1
    while bit < n:
        mine = (me // bit) % 2
        flip = (k // bit) % 2
        out = out + bit * (mine + flip - 2 * mine * flip)
        bit *= 2
    return out


def tile_at(t):
    quarter = t // 4
    edge = (7 - quarter) // 7 + quarter // 7
    turn = (t + 4) % 8
    piece = (1 - edge) * (turn // 2) + edge * (t % 4)
    stage = (t + 4) // 8
    chip = stage * (7 - stage) // 2 + stage // 4
    chip = chip + (1 - edge) * (turn % 2) * (7 - 2 * chip)
    return chip * 2 + piece // 2, piece % 2


def link_sets(n, n_local):
    assert n == 16
    pieces = []
    for chips in ((3, 4), (5, 2), (6, 1), (7,)):
        pieces.append([[(chip * 2 + c, e) for c in range(2) for e in range(n_local)] for chip in chips])
    return pieces


def exchange_kernel(n, n_local, total_tok, xd_ref, gate_ref, stat_ref, w_in_hbm, w_out_hbm,
                    x_hbm, prob_ref, pos_ref, idx_ref, gate_rows_ref, norm_ref,
                    gw_in_hbm, gw_out_t_hbm, back_ref, dl_ref, gwr_ref, stat_out_ref,
                    w_in_ref, w_out_ref, gw_in_ref, gw_out_t_ref, x_ref, gwr_acc, gwr_s, gwr_r, gwr_mine,
                    xr, gate_r, g_s, g_r, stat_r,
                    fwd_send, fwd_recv, gate_send, gate_recv,
                    ret_send, ret_recv, g_send, g_recv, stat_send, stat_recv, a_send, a_recv, b_send, b_recv, loc_sem):
    me = lax.axis_index('ep')
    cap, d_model = xr.shape[3], xr.shape[4]
    d_ff = w_in_ref.shape[2]

    def peer_of(k):
        return flip_bits(me, k, n)

    def fwd_copy(k, e, part):
        sem = (k * n_local + e) * 2 + part
        peer = peer_of(k)
        return pltpu.make_async_remote_copy(
            src_ref=xd_ref.at[peer, e, part], dst_ref=xr.at[k, e, part],
            send_sem=fwd_send.at[sem], recv_sem=fwd_recv.at[sem],
            device_id=(peer,), device_id_type=MESH)

    def gate_copy(k):
        peer = peer_of(k)
        return pltpu.make_async_remote_copy(
            src_ref=gate_ref.at[peer], dst_ref=gate_r.at[k],
            send_sem=gate_send.at[k], recv_sem=gate_recv.at[k],
            device_id=(peer,), device_id_type=MESH)

    def stat_copy(k):
        return pltpu.make_async_remote_copy(
            src_ref=stat_ref, dst_ref=stat_r.at[me],
            send_sem=stat_send.at[k], recv_sem=stat_recv.at[k],
            device_id=(peer_of(k),), device_id_type=MESH)

    def ret_copy(k, e):
        sem = k * n_local + e
        return pltpu.make_async_remote_copy(
            src_ref=xr.at[k, e, 0], dst_ref=back_ref.at[me, e],
            send_sem=ret_send.at[sem], recv_sem=ret_recv.at[sem],
            device_id=(peer_of(k),), device_id_type=MESH)

    def g_copy(k):
        return pltpu.make_async_remote_copy(
            src_ref=g_s.at[k], dst_ref=g_r.at[me],
            send_sem=g_send.at[k], recv_sem=g_recv.at[k],
            device_id=(peer_of(k),), device_id_type=MESH)

    def scatter_copy(k):
        peer = peer_of(k)
        return pltpu.make_async_remote_copy(
            src_ref=gwr_s.at[peer], dst_ref=gwr_r.at[me], send_sem=a_send.at[k], recv_sem=a_recv.at[k],
            device_id=(peer,), device_id_type=MESH)

    def spread_copy(k):
        return pltpu.make_async_remote_copy(
            src_ref=gwr_mine, dst_ref=gwr_ref.at[me], send_sem=b_send.at[k], recv_sem=b_recv.at[k],
            device_id=(peer_of(k),), device_id_type=MESH)

    sets = link_sets(n, n_local)

    def interleave(queues):
        return [queue[i] for i in range(len(queues[0])) for queue in queues]

    def send_rows(queues):
        for k, e in interleave(queues):
            if e == 0:
                gate_copy(k).start()
                stat_copy(k).start()
            for part in range(2):
                fwd_copy(k, e, part).start()

    def rows_left(queues):
        for queue in queues:
            for i, (k, e) in enumerate(queue):
                fwd_copy(k, e, 0).wait_send()
                if i < len(queue) - 1:
                    fwd_copy(k, e, 1).wait_send()

    def send_grads(queues, lo=0, hi=None):
        for k, e in interleave(queues)[lo:hi]:
            ret_copy(k, e).start()

    def grads_left(queues):
        for queue in queues:
            for k, e in queue[:-1]:
                ret_copy(k, e).wait_send()

    near = [[(1, e) for e in range(n_local)]]
    own_in = [pltpu.make_async_copy(xd_ref.at[me, e], xr.at[0, e], loc_sem.at[e]) for e in range(n_local)]
    own_gate = pltpu.make_async_copy(gate_ref.at[me], gate_r.at[0], loc_sem.at[n_local])
    own_out = [pltpu.make_async_copy(xr.at[0, e, 0], back_ref.at[me, e], loc_sem.at[e]) for e in range(n_local)]
    load_x = pltpu.make_async_copy(x_hbm, x_ref, loc_sem.at[n_local + 3])

    send_rows(sets[0])
    send_rows(near)
    for c in own_in:
        c.start()
    own_gate.start()
    weights = [pltpu.make_async_copy(w_in_hbm, w_in_ref, loc_sem.at[n_local + 1]),
               pltpu.make_async_copy(w_out_hbm, w_out_ref, loc_sem.at[n_local + 2])]
    for c in weights:
        c.start()
    load_x.start()
    gwr_s[...] = jnp.zeros_like(gwr_s)
    gw_in_ref[...] = jnp.zeros_like(gw_in_ref)
    gw_out_t_ref[...] = jnp.zeros_like(gw_out_t_ref)
    g_s[...] = jnp.zeros_like(g_s)
    stat_r[me] = stat_ref[...]
    for c in own_in:
        c.wait()
    own_gate.wait()
    for c in weights:
        c.wait()

    lanes = gate_r.shape[2]

    def tile(k, e):
        eye = (lax.broadcasted_iota(jnp.int32, (cap, lanes), 0)
               == lax.broadcasted_iota(jnp.int32, (cap, lanes), 1))
        rows = xr[k, e, 0]
        dy = xr[k, e, 1].astype(jnp.float32)
        gate_row = gate_r[k, pl.ds(e, 1), :]
        gate_col = jnp.sum(jnp.where(eye, gate_row, 0.0), axis=1, keepdims=True)
        grad = (gate_col * dy).astype(jnp.bfloat16)
        rows_t = rows.T
        grad_t = grad.T
        out = jnp.zeros((cap, d_model), jnp.float32)
        d_rows = jnp.zeros((cap, d_model), jnp.float32)
        for f in range(0, d_ff, F_CHUNK):
            fs = pl.ds(f, F_CHUNK)
            w_a = w_in_ref[e, :, fs]
            w_b = w_out_ref[e, fs, :]
            pre = jnp.dot(rows, w_a, preferred_element_type=jnp.float32)
            hid = jnp.maximum(pre, 0.0).astype(jnp.bfloat16)
            out = out + jnp.dot(hid, w_b, preferred_element_type=jnp.float32)
            d_hid = nt_dot(grad, w_b)
            d_pre = jnp.where(hid.astype(jnp.float32) > 0, d_hid, 0.0).astype(jnp.bfloat16)
            gw_out_t_ref[e, :, fs] += jnp.dot(grad_t, hid, preferred_element_type=jnp.float32)
            gw_in_ref[e, :, fs] += jnp.dot(rows_t, d_pre, preferred_element_type=jnp.float32)
            d_rows = d_rows + nt_dot(d_pre, w_a)
        out = out.astype(jnp.bfloat16).astype(jnp.float32)
        g_col = jnp.sum(out * dy, axis=1, keepdims=True)
        g_s[k, pl.ds(e, 1), :] = jnp.sum(jnp.where(eye, g_col, 0.0), axis=0, keepdims=True)
        xr[k, e, 0] = d_rows.astype(jnp.bfloat16)

    order = [(0, e) for e in range(n_local)] + near[0]
    first = []
    for queues in sets:
        first.append(len(order))
        order = order + interleave(queues)
    assert order == [tile_at(t) for t in range(len(order))]

    def own_back():
        send_grads(near)
        for c in own_out:
            c.start()

    def after_rows(done, then):
        def run():
            rows_left(sets[done])
            then()
        return run

    def after_grads(done, then):
        def run():
            grads_left(sets[done])
            then()
        return run

    events = {
        first[0]: own_back,
        first[1] - 2: after_rows(0, lambda: send_rows(sets[1])),
        first[2] - 2: after_rows(1, lambda: send_grads(sets[0])),
        first[2]: after_grads(0, lambda: send_rows(sets[2])),
        first[3] - 2: after_rows(2, lambda: send_grads(sets[1])),
        first[3]: after_grads(1, lambda: send_rows(sets[3])),
        len(order) - 1: after_rows(3, lambda: send_grads(sets[2], 0, 4)),
    }

    def step(t, carry):
        k, e = tile_at(t)
        for at, run in events.items():
            pl.when(t == at)(run)

        @pl.when(t >= n_local)
        def _():
            @pl.when(e == 0)
            def _():
                gate_copy(k).wait_recv()
            for part in range(2):
                fwd_copy(k, e, part).wait_recv()

        tile(k, e)

        @pl.when(t >= n_local)
        def _():
            @pl.when(e == n_local - 1)
            def _():
                g_copy(k).start()
        return carry

    lax.fori_loop(0, len(order), step, 0)
    send_grads(sets[2], 4)
    totals = [pltpu.make_async_copy(gw_in_ref, gw_in_hbm, loc_sem.at[n_local + 1]),
              pltpu.make_async_copy(gw_out_t_ref, gw_out_t_hbm, loc_sem.at[n_local + 2])]
    for c in totals:
        c.start()
    load_x.wait()
    g_r[me] = g_s[0]
    grads_left(sets[2])
    send_grads(sets[3], 0, 2)

    def arrive(k, carry):
        stat_copy(k).wait()
        g_copy(k).wait()
        return carry

    lax.fori_loop(1, n, arrive, 0)
    stat = stat_r[0]
    for i in range(1, n):
        stat = stat + stat_r[i]
    stat_out_ref[...] = stat
    num_experts = n * n_local
    load = jnp.sum(jnp.where(eye_mask(num_experts, 128), stat[0:1, :], 0.0), axis=1, keepdims=True)
    aux_vec = (AUX_WEIGHT * num_experts / total_tok) * (load / total_tok)
    g_all = jnp.concatenate([g_r[d, 0:n_local, :] for d in range(n)], axis=0)
    g_parts = jnp.concatenate(split3(g_all), axis=0)
    span = pos_ref.shape[1]
    gwr_acc[...] = jnp.zeros_like(gwr_acc)

    def router(c, carry):
        here = pl.ds(c, 1)
        cols = pl.ds(pl.multiple_of(c * span, span), span)
        place = jnp.where(lax.broadcasted_iota(jnp.int32, (lanes, span), 0) == pos_ref[here, :], 1.0, 0.0)
        found = jnp.dot(g_parts, place.astype(jnp.bfloat16), preferred_element_type=jnp.float32)
        found = found[:num_experts] + found[num_experts:2 * num_experts] + found[2 * num_experts:]
        chosen = jnp.where(lax.broadcasted_iota(jnp.int32, (num_experts, span), 0) == idx_ref[here, :], 1.0, 0.0)
        g_tok = jnp.sum(found * chosen, axis=0, keepdims=True)
        prob = prob_ref[:, cols]
        spread = jnp.sum(prob * aux_vec, axis=0, keepdims=True)
        d_logits = ((gate_rows_ref[here, :] * g_tok) * (chosen - prob) + prob * (aux_vec - spread)
                    + ((2.0 * Z_WEIGHT / total_tok) * norm_ref[here, :]) * prob)
        dl_ref[:, cols] = d_logits
        gwr_acc[...] += jnp.dot(jnp.concatenate(split3(d_logits), axis=0), x_ref[cols, :], preferred_element_type=jnp.float32)
        return carry

    lax.fori_loop(0, pos_ref.shape[0], router, 0)
    part = gwr_acc[0:num_experts, :] + gwr_acc[num_experts:2 * num_experts, :] + gwr_acc[2 * num_experts:, :]
    for d in range(n):
        gwr_s[d, 0:n_local, :] = part[d * n_local:(d + 1) * n_local]
    gwr_r[me] = gwr_s[me]

    def scatter(k, carry):
        scatter_copy(k).start()
        return carry

    lax.fori_loop(1, n, scatter, 0)
    send_grads(sets[3], 2)

    def gathered(k, carry):
        scatter_copy(k).wait()
        return carry

    lax.fori_loop(1, n, gathered, 0)
    mine = gwr_r[0]
    for i in range(1, n):
        mine = mine + gwr_r[i]
    gwr_mine[...] = mine
    gwr_ref[me] = mine

    def spread_all(k, carry):
        spread_copy(k).start()
        return carry

    lax.fori_loop(1, n, spread_all, 0)

    for queues in sets:
        for queue in queues:
            k, e = queue[-1]
            fwd_copy(k, e, 1).wait_send()
            if queues is not sets[3]:
                ret_copy(k, e).wait_send()
    grads_left(sets[3])
    for queue in sets[3]:
        ret_copy(*queue[-1]).wait_send()
    for k, e in near[0]:
        for part in range(2):
            fwd_copy(k, e, part).wait_send()
        ret_copy(k, e).wait_send()
    for c in own_out:
        c.wait()
    for c in totals:
        c.wait()

    def drain(k, carry):
        gate_copy(k).wait_send()
        spread_copy(k).wait()
        for e in range(n_local):
            ret_copy(k, e).wait_recv()
        return carry

    lax.fori_loop(1, n, drain, 0)


def exchange(xd, gates, stats, w_in, w_out, x_tokens, prob, pos_rows, idx_rows, gate_rows, norm_rows, n_dev):
    n_local, d_model, d_ff = w_in.shape
    cap = xd.shape[3]
    lanes = gates.shape[2]
    any_spec = pl.BlockSpec(memory_space=pl.ANY)
    vmem_spec = pl.BlockSpec(memory_space=pltpu.VMEM)
    pairs = n_dev * n_local
    dma = pltpu.SemaphoreType.DMA
    return pl.pallas_call(
        functools.partial(exchange_kernel, n_dev, n_local, x_tokens.shape[0] * n_dev),
        out_shape=(jax.ShapeDtypeStruct((n_local, d_model, d_ff), jnp.float32),
                   jax.ShapeDtypeStruct((n_local, d_model, d_ff), jnp.float32),
                   jax.ShapeDtypeStruct((n_dev, n_local, cap, d_model), jnp.bfloat16),
                   jax.ShapeDtypeStruct(prob.shape, jnp.float32),
                   jax.ShapeDtypeStruct((n_dev, 8, d_model), jnp.float32),
                   jax.ShapeDtypeStruct(stats.shape, jnp.float32)),
        in_specs=[any_spec, any_spec, vmem_spec, any_spec, any_spec, any_spec] + [vmem_spec] * 5,
        out_specs=(any_spec, any_spec, any_spec, vmem_spec, vmem_spec, vmem_spec),
        scratch_shapes=[
            pltpu.VMEM(w_in.shape, jnp.bfloat16),
            pltpu.VMEM(w_out.shape, jnp.bfloat16),
            pltpu.VMEM(w_in.shape, jnp.float32),
            pltpu.VMEM(w_in.shape, jnp.float32),
            pltpu.VMEM(x_tokens.shape, jnp.bfloat16),
            pltpu.VMEM((3 * pairs, d_model), jnp.float32),
            pltpu.VMEM((n_dev, 8, d_model), jnp.float32),
            pltpu.VMEM((n_dev, 8, d_model), jnp.float32),
            pltpu.VMEM((8, d_model), jnp.float32),
            pltpu.VMEM((n_dev, n_local, 2, cap, d_model), jnp.bfloat16),
            pltpu.VMEM((n_dev, 8, lanes), jnp.float32),
            pltpu.VMEM((n_dev, 8, lanes), jnp.float32),
            pltpu.VMEM((n_dev, 8, lanes), jnp.float32),
            pltpu.VMEM((n_dev,) + stats.shape, jnp.float32),
            dma((2 * pairs,)), dma((2 * pairs,)), dma((n_dev,)), dma((n_dev,)),
            dma((pairs,)), dma((pairs,)), dma((n_dev,)), dma((n_dev,)),
            dma((n_dev,)), dma((n_dev,)), dma((n_dev,)), dma((n_dev,)), dma((n_dev,)), dma((n_dev,)),
            dma((n_local + 4,)),
        ],
        compiler_params=pltpu.CompilerParams(has_side_effects=True, vmem_limit_bytes=60 * 1024 * 1024),
        name='exchange',
    )(xd, gates, stats, w_in, w_out, x_tokens, prob, pos_rows, idx_rows, gate_rows, norm_rows)


def solution(mesh):
    n_dev = mesh.shape['ep']

    def expert_layer(x_tokens, w_router, expert_idx, w_in, w_out, grad_y):
        tokens, d_model = x_tokens.shape
        n_local = w_in.shape[0]
        num_experts = n_local * n_dev
        capacity = (5 * tokens + 4 * num_experts - 1) // (4 * num_experts)
        total_tok = tokens * n_dev
        lanes = -(-capacity // 128) * 128
        idx_rows = expert_idx.reshape(-1, ROW_TOKENS)
        prob, slot_rows, pos_rows, gate_rows, norm_rows, stats = route(x_tokens, idx_rows, w_router, capacity)
        slot_rows = slot_rows.reshape(tokens)
        xd, gates = dispatch(slot_rows, x_tokens, grad_y, gate_rows, n_dev, n_local, capacity, lanes)
        gw_in, gw_out_t, back, d_logits, gwr, stats = exchange(xd, gates, stats, w_in, w_out, x_tokens, prob, pos_rows, idx_rows,
                                                               gate_rows, norm_rows, n_dev)
        grad_x, grad_w_in, grad_w_out = combine(slot_rows, back, d_logits, w_router, gw_in, gw_out_t)
        grad_w_router = gwr[:, :n_local].reshape(num_experts, d_model).T

        load_frac = stats[0, :num_experts] / total_tok
        mean_prob = stats[0, num_experts:2 * num_experts] / total_tok
        aux_loss = AUX_WEIGHT * num_experts * jnp.sum(load_frac * mean_prob)
        z_loss = Z_WEIGHT * stats[0, 2 * num_experts] / total_tok
        return grad_x, grad_w_in, grad_w_out, grad_w_router, aux_loss, z_loss

    return jax.shard_map(expert_layer, mesh=mesh,
                         in_specs=(P('ep', None), P(None, None), P('ep'), P('ep', None, None), P('ep', None, None), P('ep', None)),
                         out_specs=(P('ep', None), P('ep', None, None), P('ep', None, None), P(None, None), P(), P()),
                         check_vma=False)
```

```python
import functools

import jax
import jax.numpy as jnp
from jax import lax
from jax.experimental import pallas as pl
from jax.experimental.pallas import tpu as pltpu
from jax.sharding import PartitionSpec as P

AUX_WEIGHT = 0.01
Z_WEIGHT = 0.001
MESH = pl.DeviceIdType.MESH
F_CHUNK = 512
TOKEN_BLOCK = 256
UNROLL = 32
ROW_GROUP = 32
ROW_TOKENS = 1024
GROUP = 2


def nt_dot(a, b):
    return lax.dot_general(a, b, (((1,), (1,)), ((), ())), preferred_element_type=jnp.float32)


def eye_mask(rows, cols):
    return lax.broadcasted_iota(jnp.int32, (rows, cols), 0) == lax.broadcasted_iota(jnp.int32, (rows, cols), 1)


def split3(v):
    hi = v.astype(jnp.bfloat16)
    rest = v - hi.astype(jnp.float32)
    mid = rest.astype(jnp.bfloat16)
    low = (rest - mid.astype(jnp.float32)).astype(jnp.bfloat16)
    return hi, mid, low


def route_kernel(capacity, x_ref, idx_ref, wr_ref, prob_ref, slot_ref, pos_ref, gate_ref, norm_ref, stat_ref, seen, prob_sum, z_sum):
    step = pl.program_id(0)
    num_experts, block = prob_ref.shape

    @pl.when(step == 0)
    def _():
        seen[...] = jnp.zeros_like(seen)
        prob_sum[...] = jnp.zeros_like(prob_sum)
        z_sum[...] = jnp.zeros_like(z_sum)

    parts = nt_dot(jnp.concatenate(split3(wr_ref[...]), axis=0), x_ref[...])
    logits = parts[:num_experts] + parts[num_experts:2 * num_experts] + parts[2 * num_experts:]
    top = jnp.max(logits, axis=0, keepdims=True)
    shifted = jnp.exp(logits - top)
    scale = jnp.sum(shifted, axis=0, keepdims=True)
    prob = shifted / scale
    log_norm = top + jnp.log(scale)
    idx = idx_ref[pl.ds(step, 1), :]
    chosen = jnp.where(lax.broadcasted_iota(jnp.int32, (num_experts, block), 0) == idx, 1.0, 0.0)
    prob_ref[...] = prob
    gate_ref[pl.ds(step, 1), :] = jnp.sum(prob * chosen, axis=0, keepdims=True)
    norm_ref[pl.ds(step, 1), :] = log_norm
    squares = log_norm * log_norm
    for i in range(0, block, 128):
        prob_sum[...] += prob[:, i:i + 128]
        z_sum[0:1, :] += squares[:, i:i + 128]
    upto = jnp.where(lax.broadcasted_iota(jnp.int32, (TOKEN_BLOCK, TOKEN_BLOCK), 0)
                     <= lax.broadcasted_iota(jnp.int32, (TOKEN_BLOCK, TOKEN_BLOCK), 1), 1.0, 0.0).astype(jnp.bfloat16)
    before = seen[:, 0:1]
    slots = []
    places = []
    for i in range(0, block, TOKEN_BLOCK):
        part = chosen[:, i:i + TOKEN_BLOCK]
        count = jnp.dot(part.astype(jnp.bfloat16), upto, preferred_element_type=jnp.float32) + before
        position = jnp.sum(part * count, axis=0, keepdims=True).astype(jnp.int32) - 1
        places.append(position)
        slots.append(8 * jnp.where(position < capacity, idx[:, i:i + TOKEN_BLOCK] * capacity + position, num_experts * capacity))
        before = count[:, TOKEN_BLOCK - 1:TOKEN_BLOCK]
    slot_ref[pl.ds(step, 1), :] = jnp.concatenate(slots, axis=1)
    pos_ref[pl.ds(step, 1), :] = jnp.concatenate(places, axis=1)
    seen[...] = jnp.broadcast_to(before, seen.shape)

    @pl.when(step == pl.num_programs(0) - 1)
    def _():
        row = lax.broadcasted_iota(jnp.int32, (num_experts, 128), 0)
        lane = lax.broadcasted_iota(jnp.int32, (num_experts, 128), 1)
        probs = jnp.sum(prob_sum[...], axis=1, keepdims=True)
        stat_ref[...] = jnp.zeros_like(stat_ref)
        total = jnp.sum(jnp.where(row == lane, seen[...], 0.0) + jnp.where(row + num_experts == lane, probs, 0.0),
                        axis=0, keepdims=True)
        squares = jnp.sum(z_sum[0:1, :], axis=1, keepdims=True)
        stat_ref[0:1, :] = total + jnp.where(lane[0:1, :] == 2 * num_experts, squares, 0.0)


def route(x_tokens, idx_rows, w_router, capacity):
    tokens, d_model = x_tokens.shape
    num_experts = w_router.shape[1]
    steps, block = idx_rows.shape
    rows = lambda dtype: jax.ShapeDtypeStruct((steps, block), dtype)
    whole = pl.BlockSpec((steps, block), lambda i: (0, 0))
    return pl.pallas_call(
        functools.partial(route_kernel, capacity),
        grid=(steps,),
        out_shape=(jax.ShapeDtypeStruct((num_experts, tokens), jnp.float32), rows(jnp.int32), rows(jnp.int32), rows(jnp.float32), rows(jnp.float32),
                   jax.ShapeDtypeStruct((8, 128), jnp.float32)),
        in_specs=[pl.BlockSpec((block, d_model), lambda i: (i, 0)), whole,
                  pl.BlockSpec((num_experts, d_model), lambda i: (0, 0))],
        out_specs=(pl.BlockSpec((num_experts, block), lambda i: (0, i)), whole, whole, whole, whole,
                   pl.BlockSpec((8, 128), lambda i: (0, 0))),
        scratch_shapes=[pltpu.VMEM((num_experts, 128), jnp.float32), pltpu.VMEM((num_experts, 128), jnp.float32), pltpu.VMEM((8, 128), jnp.float32)],
        compiler_params=pltpu.CompilerParams(dimension_semantics=('arbitrary',)),
        name='route',
    )(x_tokens, idx_rows, w_router.T)


def dispatch_kernel(steps, capacity, slot_ref, x_ref, dy_ref, gate_ref, xd_ref, gates_ref, table, stage):
    step = pl.program_id(0)
    block, d_model = x_ref.shape
    cols = d_model // 128
    lanes = gates_ref.shape[2]
    group, n_local = xd_ref.shape[:2]

    @pl.when(step == 0)
    def _():
        def clear(i, carry):
            table[pl.ds(pl.multiple_of(i * 512, 512), 512), :] = jnp.zeros((512, 128), jnp.float32)
            return carry
        lax.fori_loop(0, table.shape[0] // 512, clear, 0)

    @pl.when(step < steps)
    def _():
        for r in range(0, block, ROW_GROUP):
            for c in range(2 * cols):
                rows_ref = x_ref if c < cols else dy_ref
                span = slice(c % cols * 128, (c % cols + 1) * 128)
                stage[pl.ds(r * 8 + c, ROW_GROUP, stride=8), :] = rows_ref[r:r + ROW_GROUP, span].astype(jnp.float32)
        eye = eye_mask(128, 128)
        gate_row = gate_ref[pl.ds(step, 1), :]
        for i in range(0, block, 128):
            gate = jnp.sum(jnp.where(eye, gate_row[:, i:i + 128], 0.0), axis=1, keepdims=True)
            stage[pl.ds(i * 8 + 2 * cols, 128, stride=8), :] = jnp.broadcast_to(gate, (128, 128))

        def place(i, carry):
            for u in range(UNROLL):
                t = i * UNROLL + u
                slot = slot_ref[step * block + t]
                table[pl.ds(pl.multiple_of(slot, 8), 8), :] = stage[pl.ds(pl.multiple_of(t * 8, 8), 8), :]
            return carry
        lax.fori_loop(0, block // UNROLL, place, 0)

    @pl.when(step >= steps)
    def _():
        gates_ref[...] = jnp.zeros_like(gates_ref)
        row = lax.broadcasted_iota(jnp.int32, (capacity, 128), 0)
        lane = lax.broadcasted_iota(jnp.int32, (capacity, 128), 1)

        def unload(i, carry):
            d = i // n_local
            e = i % n_local
            first = (((step - steps) * group + d) * n_local + e) * (capacity * 8)
            for r in range(0, capacity, ROW_GROUP):
                for c in range(2 * cols):
                    span = slice(c % cols * 128, (c % cols + 1) * 128)
                    xd_ref[d, e, c // cols, r:r + ROW_GROUP, span] = table[
                        pl.ds(first + r * 8 + c, ROW_GROUP, stride=8), :].astype(jnp.bfloat16)
            gate = table[pl.ds(first + 2 * cols, capacity, stride=8), :]
            gates_ref[d, pl.ds(e, 1), :] = jnp.concatenate([
                jnp.sum(jnp.where(row == lane + c * 128, gate, 0.0), axis=0, keepdims=True)
                for c in range(lanes // 128)], axis=1)
            return carry
        lax.fori_loop(0, group * n_local, unload, 0)


def dispatch(slot_rows, x_tokens, grad_y, gate_rows, n_dev, n_local, capacity, lanes):
    tokens, d_model = x_tokens.shape
    steps, block = gate_rows.shape
    n_slots = n_dev * n_local * capacity
    table_rows = -(-(n_slots + 1) * 8 // 512) * 512
    tok = lambda i: (jnp.minimum(i, steps - 1), 0)
    dst = lambda i: jnp.maximum(i - steps, 0)
    return pl.pallas_call(
        functools.partial(dispatch_kernel, steps, capacity),
        grid=(steps + n_dev // GROUP,),
        out_shape=(jax.ShapeDtypeStruct((n_dev, n_local, 2, capacity, d_model), jnp.bfloat16),
                   jax.ShapeDtypeStruct((n_dev, 8, lanes), jnp.float32)),
        in_specs=[pl.BlockSpec(memory_space=pltpu.SMEM),
                  pl.BlockSpec((block, d_model), tok),
                  pl.BlockSpec((block, d_model), tok),
                  pl.BlockSpec((steps, block), lambda i: (0, 0))],
        out_specs=(pl.BlockSpec((GROUP, n_local, 2, capacity, d_model), lambda i: (dst(i), 0, 0, 0, 0)),
                   pl.BlockSpec((GROUP, 8, lanes), lambda i: (dst(i), 0, 0))),
        scratch_shapes=[pltpu.VMEM((table_rows, 128), jnp.float32),
                        pltpu.VMEM((block * 8, 128), jnp.float32)],
        compiler_params=pltpu.CompilerParams(dimension_semantics=('arbitrary',), vmem_limit_bytes=62 * 1024 * 1024),
        name='dispatch',
    )(slot_rows, x_tokens, grad_y, gate_rows)


def combine_kernel(fills, sources, capacity, slot_ref, back_ref, dl_ref, wr_t_ref, gwi_ref, gwo_t_ref,
                   gx_ref, gwi_out_ref, gwo_out_ref, table, stage):
    step = pl.program_id(0)
    block, d_model = gx_ref.shape
    cols = d_model // 128
    group, n_local = back_ref.shape[:2]
    n_slots = sources * n_local * capacity
    gwi_out_ref[...] = gwi_ref[...]
    gwo_out_ref[0] = gwo_t_ref[0].T

    @pl.when(step == 0)
    def _():
        table[pl.ds(n_slots * 8, 8), :] = jnp.zeros((8, 128), jnp.float32)

    @pl.when(step < fills)
    def _():
        def load(i, carry):
            d = i // n_local
            e = i % n_local
            first = ((step * group + d) * n_local + e) * (capacity * 8)
            for r in range(0, capacity, ROW_GROUP):
                for c in range(cols):
                    table[pl.ds(first + r * 8 + c, ROW_GROUP, stride=8), :] = back_ref[
                        d, e, r:r + ROW_GROUP, c * 128:(c + 1) * 128].astype(jnp.float32)
            return carry
        lax.fori_loop(0, group * n_local, load, 0)

    @pl.when(step >= fills)
    def _():
        part = step - fills

        def pick(i, carry):
            for u in range(UNROLL):
                t = i * UNROLL + u
                slot = slot_ref[part * block + t]
                stage[pl.ds(pl.multiple_of(t * 8, 8), 8), :] = table[pl.ds(pl.multiple_of(slot, 8), 8), :]
            return carry
        lax.fori_loop(0, block // UNROLL, pick, 0)
        hi, mid, low = split3(dl_ref[...])
        left = jnp.concatenate([hi, mid, hi, low, mid, hi], axis=0)
        w_hi, w_mid, w_low = split3(wr_t_ref[...])
        right = jnp.concatenate([w_hi, w_hi, w_mid, w_hi, w_mid, w_low], axis=0)
        dx_router = lax.dot_general(left, right, (((0,), (0,)), ((), ())), preferred_element_type=jnp.float32)
        for r in range(0, block, ROW_GROUP):
            for c in range(cols):
                span = slice(c * 128, (c + 1) * 128)
                gx_ref[r:r + ROW_GROUP, span] = (stage[pl.ds(r * 8 + c, ROW_GROUP, stride=8), :]
                                                 + dx_router[r:r + ROW_GROUP, span]).astype(jnp.bfloat16)


def combine(slot_rows, back, d_logits, w_router, gw_in, gw_out_t):
    n_dev, n_local, capacity, d_model = back.shape
    num_experts, tokens = d_logits.shape
    d_ff = gw_in.shape[2]
    block = ROW_TOKENS
    blocks = tokens // block
    fills = n_dev // GROUP
    steps = fills + blocks
    n_slots = n_dev * n_local * capacity
    gw_in_rows = gw_in.reshape(n_local * d_model, d_ff)
    in_rows = n_local * d_model // steps
    out_cols = d_ff // 256
    src = lambda i: jnp.minimum(i, fills - 1)
    tok = lambda i: (jnp.maximum(i - fills, 0), 0)
    flip = lambda i: jnp.minimum(i, n_local * out_cols - 1)
    gx, gw_in_out, gw_out = pl.pallas_call(
        functools.partial(combine_kernel, fills, n_dev, capacity),
        grid=(steps,),
        out_shape=(jax.ShapeDtypeStruct((tokens, d_model), jnp.bfloat16),
                   jax.ShapeDtypeStruct((n_local * d_model, d_ff), jnp.float32),
                   jax.ShapeDtypeStruct((n_local, d_ff, d_model), jnp.float32)),
        in_specs=[pl.BlockSpec(memory_space=pltpu.SMEM),
                  pl.BlockSpec((GROUP, n_local, capacity, d_model), lambda i: (src(i), 0, 0, 0)),
                  pl.BlockSpec((num_experts, block), lambda i: (0, jnp.maximum(i - fills, 0))),
                  pl.BlockSpec((num_experts, d_model), lambda i: (0, 0)),
                  pl.BlockSpec((in_rows, d_ff), lambda i: (i, 0)),
                  pl.BlockSpec((1, d_model, 256), lambda i: (flip(i) // out_cols, 0, flip(i) % out_cols))],
        out_specs=(pl.BlockSpec((block, d_model), tok),
                   pl.BlockSpec((in_rows, d_ff), lambda i: (i, 0)),
                   pl.BlockSpec((1, 256, d_model), lambda i: (flip(i) // out_cols, flip(i) % out_cols, 0))),
        scratch_shapes=[pltpu.VMEM(((n_slots + 1) * 8, 128), jnp.float32),
                        pltpu.VMEM((block * 8, 128), jnp.float32)],
        compiler_params=pltpu.CompilerParams(dimension_semantics=('arbitrary',), vmem_limit_bytes=63 * 1024 * 1024),
        name='combine',
    )(slot_rows, back, d_logits, w_router.T, gw_in_rows, gw_out_t)
    return gx, gw_in_out.reshape(n_local, d_model, d_ff), gw_out


def flip_bits(me, k, n):
    out = 0
    bit = 1
    while bit < n:
        mine = (me // bit) % 2
        flip = (k // bit) % 2
        out = out + bit * (mine + flip - 2 * mine * flip)
        bit *= 2
    return out


def tile_at(t):
    quarter = t // 4
    edge = (7 - quarter) // 7 + quarter // 7
    turn = (t + 4) % 8
    piece = (1 - edge) * (turn // 2) + edge * (t % 4)
    stage = (t + 4) // 8
    chip = stage * (7 - stage) // 2 + stage // 4
    chip = chip + (1 - edge) * (turn % 2) * (7 - 2 * chip)
    return chip * 2 + piece // 2, piece % 2


def link_sets(n, n_local):
    assert n == 16
    pieces = []
    for chips in ((3, 4), (5, 2), (6, 1), (7,)):
        pieces.append([[(chip * 2 + c, e) for c in range(2) for e in range(n_local)] for chip in chips])
    return pieces


def exchange_kernel(n, n_local, total_tok, xd_ref, gate_ref, stat_ref, w_in_hbm, w_out_hbm,
                    x_hbm, prob_ref, pos_ref, idx_ref, gate_rows_ref, norm_ref,
                    gw_in_hbm, gw_out_t_hbm, back_ref, dl_ref, gwr_ref, stat_out_ref,
                    w_in_ref, w_out_ref, gw_in_ref, gw_out_t_ref, x_ref, gwr_acc, gwr_s, gwr_r, gwr_mine,
                    xr, gate_r, g_s, g_r, stat_r,
                    fwd_send, fwd_recv, gate_send, gate_recv,
                    ret_send, ret_recv, g_send, g_recv, stat_send, stat_recv, a_send, a_recv, b_send, b_recv, loc_sem):
    me = lax.axis_index('ep')
    cap, d_model = xr.shape[3], xr.shape[4]
    d_ff = w_in_ref.shape[2]

    def peer_of(k):
        return flip_bits(me, k, n)

    def fwd_copy(k, e, part):
        sem = (k * n_local + e) * 2 + part
        peer = peer_of(k)
        return pltpu.make_async_remote_copy(
            src_ref=xd_ref.at[peer, e, part], dst_ref=xr.at[k, e, part],
            send_sem=fwd_send.at[sem], recv_sem=fwd_recv.at[sem],
            device_id=(peer,), device_id_type=MESH)

    def gate_copy(k):
        peer = peer_of(k)
        return pltpu.make_async_remote_copy(
            src_ref=gate_ref.at[peer], dst_ref=gate_r.at[k],
            send_sem=gate_send.at[k], recv_sem=gate_recv.at[k],
            device_id=(peer,), device_id_type=MESH)

    def stat_copy(k):
        return pltpu.make_async_remote_copy(
            src_ref=stat_ref, dst_ref=stat_r.at[me],
            send_sem=stat_send.at[k], recv_sem=stat_recv.at[k],
            device_id=(peer_of(k),), device_id_type=MESH)

    def ret_copy(k, e):
        sem = k * n_local + e
        return pltpu.make_async_remote_copy(
            src_ref=xr.at[k, e, 0], dst_ref=back_ref.at[me, e],
            send_sem=ret_send.at[sem], recv_sem=ret_recv.at[sem],
            device_id=(peer_of(k),), device_id_type=MESH)

    def g_copy(k):
        return pltpu.make_async_remote_copy(
            src_ref=g_s.at[k], dst_ref=g_r.at[me],
            send_sem=g_send.at[k], recv_sem=g_recv.at[k],
            device_id=(peer_of(k),), device_id_type=MESH)

    def scatter_copy(k):
        peer = peer_of(k)
        return pltpu.make_async_remote_copy(
            src_ref=gwr_s.at[peer], dst_ref=gwr_r.at[me], send_sem=a_send.at[k], recv_sem=a_recv.at[k],
            device_id=(peer,), device_id_type=MESH)

    def spread_copy(k):
        return pltpu.make_async_remote_copy(
            src_ref=gwr_mine, dst_ref=gwr_ref.at[me], send_sem=b_send.at[k], recv_sem=b_recv.at[k],
            device_id=(peer_of(k),), device_id_type=MESH)

    sets = link_sets(n, n_local)

    def interleave(queues):
        return [queue[i] for i in range(len(queues[0])) for queue in queues]

    def send_rows(queues):
        for k, e in interleave(queues):
            if e == 0:
                gate_copy(k).start()
                stat_copy(k).start()
            for part in range(2):
                fwd_copy(k, e, part).start()

    def rows_left(queues):
        for queue in queues:
            for i, (k, e) in enumerate(queue):
                fwd_copy(k, e, 0).wait_send()
                if i < len(queue) - 1:
                    fwd_copy(k, e, 1).wait_send()

    def send_grads(queues, lo=0, hi=None):
        for k, e in interleave(queues)[lo:hi]:
            ret_copy(k, e).start()

    def grads_left(queues):
        for queue in queues:
            for k, e in queue[:-1]:
                ret_copy(k, e).wait_send()

    near = [[(1, e) for e in range(n_local)]]
    own_in = [pltpu.make_async_copy(xd_ref.at[me, e], xr.at[0, e], loc_sem.at[e]) for e in range(n_local)]
    own_gate = pltpu.make_async_copy(gate_ref.at[me], gate_r.at[0], loc_sem.at[n_local])
    own_out = [pltpu.make_async_copy(xr.at[0, e, 0], back_ref.at[me, e], loc_sem.at[e]) for e in range(n_local)]
    load_x = pltpu.make_async_copy(x_hbm, x_ref, loc_sem.at[n_local + 3])

    send_rows(sets[0])
    send_rows(near)
    for c in own_in:
        c.start()
    own_gate.start()
    weights = [pltpu.make_async_copy(w_in_hbm, w_in_ref, loc_sem.at[n_local + 1]),
               pltpu.make_async_copy(w_out_hbm, w_out_ref, loc_sem.at[n_local + 2])]
    for c in weights:
        c.start()
    load_x.start()
    gwr_s[...] = jnp.zeros_like(gwr_s)
    gw_in_ref[...] = jnp.zeros_like(gw_in_ref)
    gw_out_t_ref[...] = jnp.zeros_like(gw_out_t_ref)
    g_s[...] = jnp.zeros_like(g_s)
    stat_r[me] = stat_ref[...]
    for c in own_in:
        c.wait()
    own_gate.wait()
    for c in weights:
        c.wait()

    lanes = gate_r.shape[2]

    def tile(k, e):
        eye = (lax.broadcasted_iota(jnp.int32, (cap, lanes), 0)
               == lax.broadcasted_iota(jnp.int32, (cap, lanes), 1))
        rows = xr[k, e, 0]
        dy = xr[k, e, 1].astype(jnp.float32)
        gate_row = gate_r[k, pl.ds(e, 1), :]
        gate_col = jnp.sum(jnp.where(eye, gate_row, 0.0), axis=1, keepdims=True)
        grad = (gate_col * dy).astype(jnp.bfloat16)
        rows_t = rows.T
        grad_t = grad.T
        out = jnp.zeros((cap, d_model), jnp.float32)
        d_rows = jnp.zeros((cap, d_model), jnp.float32)
        for f in range(0, d_ff, F_CHUNK):
            fs = pl.ds(f, F_CHUNK)
            w_a = w_in_ref[e, :, fs]
            w_b = w_out_ref[e, fs, :]
            pre = jnp.dot(rows, w_a, preferred_element_type=jnp.float32)
            hid = jnp.maximum(pre, 0.0).astype(jnp.bfloat16)
            out = out + jnp.dot(hid, w_b, preferred_element_type=jnp.float32)
            d_hid = nt_dot(grad, w_b)
            d_pre = jnp.where(hid.astype(jnp.float32) > 0, d_hid, 0.0).astype(jnp.bfloat16)
            gw_out_t_ref[e, :, fs] += jnp.dot(grad_t, hid, preferred_element_type=jnp.float32)
            gw_in_ref[e, :, fs] += jnp.dot(rows_t, d_pre, preferred_element_type=jnp.float32)
            d_rows = d_rows + nt_dot(d_pre, w_a)
        out = out.astype(jnp.bfloat16).astype(jnp.float32)
        g_col = jnp.sum(out * dy, axis=1, keepdims=True)
        g_s[k, pl.ds(e, 1), :] = jnp.sum(jnp.where(eye, g_col, 0.0), axis=0, keepdims=True)
        xr[k, e, 0] = d_rows.astype(jnp.bfloat16)

    order = [(0, e) for e in range(n_local)] + near[0]
    first = []
    for queues in sets:
        first.append(len(order))
        order = order + interleave(queues)
    assert order == [tile_at(t) for t in range(len(order))]

    def own_back():
        send_grads(near)
        for c in own_out:
            c.start()

    def after_rows(done, then):
        def run():
            rows_left(sets[done])
            then()
        return run

    def after_grads(done, then):
        def run():
            grads_left(sets[done])
            then()
        return run

    events = {
        first[0]: own_back,
        first[1] - 2: after_rows(0, lambda: send_rows(sets[1])),
        first[2] - 2: after_rows(1, lambda: send_grads(sets[0])),
        first[2]: after_grads(0, lambda: send_rows(sets[2])),
        first[3] - 2: after_rows(2, lambda: send_grads(sets[1])),
        first[3]: after_grads(1, lambda: send_rows(sets[3])),
        len(order) - 1: after_rows(3, lambda: send_grads(sets[2], 0, 4)),
    }

    def step(t, carry):
        k, e = tile_at(t)
        for at, run in events.items():
            pl.when(t == at)(run)

        @pl.when(t >= n_local)
        def _():
            @pl.when(e == 0)
            def _():
                gate_copy(k).wait_recv()
            for part in range(2):
                fwd_copy(k, e, part).wait_recv()

        tile(k, e)

        @pl.when(t >= n_local)
        def _():
            @pl.when(e == n_local - 1)
            def _():
                g_copy(k).start()
        return carry

    lax.fori_loop(0, len(order), step, 0)
    send_grads(sets[2], 4)
    totals = [pltpu.make_async_copy(gw_in_ref, gw_in_hbm, loc_sem.at[n_local + 1]),
              pltpu.make_async_copy(gw_out_t_ref, gw_out_t_hbm, loc_sem.at[n_local + 2])]
    for c in totals:
        c.start()
    load_x.wait()
    g_r[me] = g_s[0]
    grads_left(sets[2])
    send_grads(sets[3], 0, 2)

    def arrive(k, carry):
        stat_copy(k).wait()
        g_copy(k).wait()
        return carry

    lax.fori_loop(1, n, arrive, 0)
    stat = stat_r[0]
    for i in range(1, n):
        stat = stat + stat_r[i]
    stat_out_ref[...] = stat
    num_experts = n * n_local
    load = jnp.sum(jnp.where(eye_mask(num_experts, 128), stat[0:1, :], 0.0), axis=1, keepdims=True)
    aux_vec = (AUX_WEIGHT * num_experts / total_tok) * (load / total_tok)
    g_all = jnp.concatenate([g_r[d, 0:n_local, :] for d in range(n)], axis=0)
    g_parts = jnp.concatenate(split3(g_all), axis=0)
    span = pos_ref.shape[1]
    gwr_acc[...] = jnp.zeros_like(gwr_acc)

    def router(c, carry):
        here = pl.ds(c, 1)
        cols = pl.ds(pl.multiple_of(c * span, span), span)
        place = jnp.where(lax.broadcasted_iota(jnp.int32, (lanes, span), 0) == pos_ref[here, :], 1.0, 0.0)
        found = jnp.dot(g_parts, place.astype(jnp.bfloat16), preferred_element_type=jnp.float32)
        found = found[:num_experts] + found[num_experts:2 * num_experts] + found[2 * num_experts:]
        chosen = jnp.where(lax.broadcasted_iota(jnp.int32, (num_experts, span), 0) == idx_ref[here, :], 1.0, 0.0)
        g_tok = jnp.sum(found * chosen, axis=0, keepdims=True)
        prob = prob_ref[:, cols]
        spread = jnp.sum(prob * aux_vec, axis=0, keepdims=True)
        d_logits = ((gate_rows_ref[here, :] * g_tok) * (chosen - prob) + prob * (aux_vec - spread)
                    + ((2.0 * Z_WEIGHT / total_tok) * norm_ref[here, :]) * prob)
        dl_ref[:, cols] = d_logits
        gwr_acc[...] += jnp.dot(jnp.concatenate(split3(d_logits), axis=0), x_ref[cols, :], preferred_element_type=jnp.float32)
        return carry

    lax.fori_loop(0, pos_ref.shape[0], router, 0)
    part = gwr_acc[0:num_experts, :] + gwr_acc[num_experts:2 * num_experts, :] + gwr_acc[2 * num_experts:, :]
    for d in range(n):
        gwr_s[d, 0:n_local, :] = part[d * n_local:(d + 1) * n_local]
    gwr_r[me] = gwr_s[me]

    def scatter(k, carry):
        scatter_copy(k).start()
        return carry

    lax.fori_loop(1, n, scatter, 0)
    send_grads(sets[3], 2, 3)

    def gathered(k, carry):
        scatter_copy(k).wait()
        return carry

    lax.fori_loop(1, n, gathered, 0)
    mine = gwr_r[0]
    for i in range(1, n):
        mine = mine + gwr_r[i]
    gwr_mine[...] = mine
    gwr_ref[me] = mine

    def spread_all(k, carry):
        spread_copy(k).start()
        return carry

    lax.fori_loop(1, n, spread_all, 0)
    send_grads(sets[3], 3)

    for queues in sets:
        for queue in queues:
            k, e = queue[-1]
            fwd_copy(k, e, 1).wait_send()
            if queues is not sets[3]:
                ret_copy(k, e).wait_send()
    grads_left(sets[3])
    for queue in sets[3]:
        ret_copy(*queue[-1]).wait_send()
    for k, e in near[0]:
        for part in range(2):
            fwd_copy(k, e, part).wait_send()
        ret_copy(k, e).wait_send()
    for c in own_out:
        c.wait()
    for c in totals:
        c.wait()

    def drain(k, carry):
        gate_copy(k).wait_send()
        spread_copy(k).wait()
        for e in range(n_local):
            ret_copy(k, e).wait_recv()
        return carry

    lax.fori_loop(1, n, drain, 0)


def exchange(xd, gates, stats, w_in, w_out, x_tokens, prob, pos_rows, idx_rows, gate_rows, norm_rows, n_dev):
    n_local, d_model, d_ff = w_in.shape
    cap = xd.shape[3]
    lanes = gates.shape[2]
    any_spec = pl.BlockSpec(memory_space=pl.ANY)
    vmem_spec = pl.BlockSpec(memory_space=pltpu.VMEM)
    pairs = n_dev * n_local
    dma = pltpu.SemaphoreType.DMA
    return pl.pallas_call(
        functools.partial(exchange_kernel, n_dev, n_local, x_tokens.shape[0] * n_dev),
        out_shape=(jax.ShapeDtypeStruct((n_local, d_model, d_ff), jnp.float32),
                   jax.ShapeDtypeStruct((n_local, d_model, d_ff), jnp.float32),
                   jax.ShapeDtypeStruct((n_dev, n_local, cap, d_model), jnp.bfloat16),
                   jax.ShapeDtypeStruct(prob.shape, jnp.float32),
                   jax.ShapeDtypeStruct((n_dev, 8, d_model), jnp.float32),
                   jax.ShapeDtypeStruct(stats.shape, jnp.float32)),
        in_specs=[any_spec, any_spec, vmem_spec, any_spec, any_spec, any_spec] + [vmem_spec] * 5,
        out_specs=(any_spec, any_spec, any_spec, vmem_spec, vmem_spec, vmem_spec),
        scratch_shapes=[
            pltpu.VMEM(w_in.shape, jnp.bfloat16),
            pltpu.VMEM(w_out.shape, jnp.bfloat16),
            pltpu.VMEM(w_in.shape, jnp.float32),
            pltpu.VMEM(w_in.shape, jnp.float32),
            pltpu.VMEM(x_tokens.shape, jnp.bfloat16),
            pltpu.VMEM((3 * pairs, d_model), jnp.float32),
            pltpu.VMEM((n_dev, 8, d_model), jnp.float32),
            pltpu.VMEM((n_dev, 8, d_model), jnp.float32),
            pltpu.VMEM((8, d_model), jnp.float32),
            pltpu.VMEM((n_dev, n_local, 2, cap, d_model), jnp.bfloat16),
            pltpu.VMEM((n_dev, 8, lanes), jnp.float32),
            pltpu.VMEM((n_dev, 8, lanes), jnp.float32),
            pltpu.VMEM((n_dev, 8, lanes), jnp.float32),
            pltpu.VMEM((n_dev,) + stats.shape, jnp.float32),
            dma((2 * pairs,)), dma((2 * pairs,)), dma((n_dev,)), dma((n_dev,)),
            dma((pairs,)), dma((pairs,)), dma((n_dev,)), dma((n_dev,)),
            dma((n_dev,)), dma((n_dev,)), dma((n_dev,)), dma((n_dev,)), dma((n_dev,)), dma((n_dev,)),
            dma((n_local + 4,)),
        ],
        compiler_params=pltpu.CompilerParams(has_side_effects=True, vmem_limit_bytes=60 * 1024 * 1024),
        name='exchange',
    )(xd, gates, stats, w_in, w_out, x_tokens, prob, pos_rows, idx_rows, gate_rows, norm_rows)


def solution(mesh):
    n_dev = mesh.shape['ep']

    def expert_layer(x_tokens, w_router, expert_idx, w_in, w_out, grad_y):
        tokens, d_model = x_tokens.shape
        n_local = w_in.shape[0]
        num_experts = n_local * n_dev
        capacity = (5 * tokens + 4 * num_experts - 1) // (4 * num_experts)
        total_tok = tokens * n_dev
        lanes = -(-capacity // 128) * 128
        idx_rows = expert_idx.reshape(-1, ROW_TOKENS)
        prob, slot_rows, pos_rows, gate_rows, norm_rows, stats = route(x_tokens, idx_rows, w_router, capacity)
        slot_rows = slot_rows.reshape(tokens)
        xd, gates = dispatch(slot_rows, x_tokens, grad_y, gate_rows, n_dev, n_local, capacity, lanes)
        gw_in, gw_out_t, back, d_logits, gwr, stats = exchange(xd, gates, stats, w_in, w_out, x_tokens, prob, pos_rows, idx_rows,
                                                               gate_rows, norm_rows, n_dev)
        grad_x, grad_w_in, grad_w_out = combine(slot_rows, back, d_logits, w_router, gw_in, gw_out_t)
        grad_w_router = gwr[:, :n_local].reshape(num_experts, d_model).T

        load_frac = stats[0, :num_experts] / total_tok
        mean_prob = stats[0, num_experts:2 * num_experts] / total_tok
        aux_loss = AUX_WEIGHT * num_experts * jnp.sum(load_frac * mean_prob)
        z_loss = Z_WEIGHT * stats[0, 2 * num_experts] / total_tok
        return grad_x, grad_w_in, grad_w_out, grad_w_router, aux_loss, z_loss

    return jax.shard_map(expert_layer, mesh=mesh,
                         in_specs=(P('ep', None), P(None, None), P('ep'), P('ep', None, None), P('ep', None, None), P('ep', None)),
                         out_specs=(P('ep', None), P('ep', None, None), P('ep', None, None), P(None, None), P(), P()),
                         check_vma=False)
```

```python
import functools

import jax
import jax.numpy as jnp
from jax import lax
from jax.experimental import pallas as pl
from jax.experimental.pallas import tpu as pltpu
from jax.sharding import PartitionSpec as P

AUX_WEIGHT = 0.01
Z_WEIGHT = 0.001
MESH = pl.DeviceIdType.MESH
F_CHUNK = 512
TOKEN_BLOCK = 256
UNROLL = 32
ROW_GROUP = 32
ROW_TOKENS = 1024
GROUP = 2


def nt_dot(a, b):
    return lax.dot_general(a, b, (((1,), (1,)), ((), ())), preferred_element_type=jnp.float32)


def eye_mask(rows, cols):
    return lax.broadcasted_iota(jnp.int32, (rows, cols), 0) == lax.broadcasted_iota(jnp.int32, (rows, cols), 1)


def split3(v):
    hi = v.astype(jnp.bfloat16)
    rest = v - hi.astype(jnp.float32)
    mid = rest.astype(jnp.bfloat16)
    low = (rest - mid.astype(jnp.float32)).astype(jnp.bfloat16)
    return hi, mid, low


def route_kernel(capacity, x_ref, idx_ref, wr_ref, prob_ref, slot_ref, pos_ref, gate_ref, norm_ref, stat_ref, seen, prob_sum, z_sum):
    step = pl.program_id(0)
    num_experts, block = prob_ref.shape

    @pl.when(step == 0)
    def _():
        seen[...] = jnp.zeros_like(seen)
        prob_sum[...] = jnp.zeros_like(prob_sum)
        z_sum[...] = jnp.zeros_like(z_sum)

    parts = nt_dot(jnp.concatenate(split3(wr_ref[...]), axis=0), x_ref[...])
    logits = parts[:num_experts] + parts[num_experts:2 * num_experts] + parts[2 * num_experts:]
    top = jnp.max(logits, axis=0, keepdims=True)
    shifted = jnp.exp(logits - top)
    scale = jnp.sum(shifted, axis=0, keepdims=True)
    prob = shifted / scale
    log_norm = top + jnp.log(scale)
    idx = idx_ref[pl.ds(step, 1), :]
    chosen = jnp.where(lax.broadcasted_iota(jnp.int32, (num_experts, block), 0) == idx, 1.0, 0.0)
    prob_ref[...] = prob
    gate_ref[pl.ds(step, 1), :] = jnp.sum(prob * chosen, axis=0, keepdims=True)
    norm_ref[pl.ds(step, 1), :] = log_norm
    squares = log_norm * log_norm
    for i in range(0, block, 128):
        prob_sum[...] += prob[:, i:i + 128]
        z_sum[0:1, :] += squares[:, i:i + 128]
    upto = jnp.where(lax.broadcasted_iota(jnp.int32, (TOKEN_BLOCK, TOKEN_BLOCK), 0)
                     <= lax.broadcasted_iota(jnp.int32, (TOKEN_BLOCK, TOKEN_BLOCK), 1), 1.0, 0.0).astype(jnp.bfloat16)
    before = seen[:, 0:1]
    slots = []
    places = []
    for i in range(0, block, TOKEN_BLOCK):
        part = chosen[:, i:i + TOKEN_BLOCK]
        count = jnp.dot(part.astype(jnp.bfloat16), upto, preferred_element_type=jnp.float32) + before
        position = jnp.sum(part * count, axis=0, keepdims=True).astype(jnp.int32) - 1
        places.append(position)
        slots.append(8 * jnp.where(position < capacity, idx[:, i:i + TOKEN_BLOCK] * capacity + position, num_experts * capacity))
        before = count[:, TOKEN_BLOCK - 1:TOKEN_BLOCK]
    slot_ref[pl.ds(step, 1), :] = jnp.concatenate(slots, axis=1)
    pos_ref[pl.ds(step, 1), :] = jnp.concatenate(places, axis=1)
    seen[...] = jnp.broadcast_to(before, seen.shape)

    @pl.when(step == pl.num_programs(0) - 1)
    def _():
        row = lax.broadcasted_iota(jnp.int32, (num_experts, 128), 0)
        lane = lax.broadcasted_iota(jnp.int32, (num_experts, 128), 1)
        probs = jnp.sum(prob_sum[...], axis=1, keepdims=True)
        stat_ref[...] = jnp.zeros_like(stat_ref)
        total = jnp.sum(jnp.where(row == lane, seen[...], 0.0) + jnp.where(row + num_experts == lane, probs, 0.0),
                        axis=0, keepdims=True)
        squares = jnp.sum(z_sum[0:1, :], axis=1, keepdims=True)
        stat_ref[0:1, :] = total + jnp.where(lane[0:1, :] == 2 * num_experts, squares, 0.0)


def route(x_tokens, idx_rows, w_router, capacity):
    tokens, d_model = x_tokens.shape
    num_experts = w_router.shape[1]
    steps, block = idx_rows.shape
    rows = lambda dtype: jax.ShapeDtypeStruct((steps, block), dtype)
    whole = pl.BlockSpec((steps, block), lambda i: (0, 0))
    return pl.pallas_call(
        functools.partial(route_kernel, capacity),
        grid=(steps,),
        out_shape=(jax.ShapeDtypeStruct((num_experts, tokens), jnp.float32), rows(jnp.int32), rows(jnp.int32), rows(jnp.float32), rows(jnp.float32),
                   jax.ShapeDtypeStruct((8, 128), jnp.float32)),
        in_specs=[pl.BlockSpec((block, d_model), lambda i: (i, 0)), whole,
                  pl.BlockSpec((num_experts, d_model), lambda i: (0, 0))],
        out_specs=(pl.BlockSpec((num_experts, block), lambda i: (0, i)), whole, whole, whole, whole,
                   pl.BlockSpec((8, 128), lambda i: (0, 0))),
        scratch_shapes=[pltpu.VMEM((num_experts, 128), jnp.float32), pltpu.VMEM((num_experts, 128), jnp.float32), pltpu.VMEM((8, 128), jnp.float32)],
        compiler_params=pltpu.CompilerParams(dimension_semantics=('arbitrary',)),
        name='route',
    )(x_tokens, idx_rows, w_router.T)


def dispatch_kernel(steps, capacity, lane_cols, slot_ref, x_ref, dy_ref, gate_ref, xd_ref, gates_ref, table, stage):
    step = pl.program_id(0)
    block, d_model = x_ref.shape
    cols = d_model // 128
    group, n_local = xd_ref.shape[:2]

    @pl.when(step == 0)
    def _():
        def clear(i, carry):
            table[pl.ds(pl.multiple_of(i * 512, 512), 512), :] = jnp.zeros((512, 128), jnp.float32)
            return carry
        lax.fori_loop(0, table.shape[0] // 512, clear, 0)

    @pl.when(step < steps)
    def _():
        for r in range(0, block, ROW_GROUP):
            for c in range(2 * cols):
                rows_ref = x_ref if c < cols else dy_ref
                span = slice(c % cols * 128, (c % cols + 1) * 128)
                stage[pl.ds(r * 8 + c, ROW_GROUP, stride=8), :] = rows_ref[r:r + ROW_GROUP, span].astype(jnp.float32)
        eye = eye_mask(128, 128)
        gate_row = gate_ref[pl.ds(step, 1), :]
        for i in range(0, block, 128):
            gate = jnp.sum(jnp.where(eye, gate_row[:, i:i + 128], 0.0), axis=1, keepdims=True)
            stage[pl.ds(i * 8 + 2 * cols, 128, stride=8), :] = jnp.broadcast_to(gate, (128, 128))

        def place(i, carry):
            for u in range(UNROLL):
                t = i * UNROLL + u
                slot = slot_ref[step * block + t]
                table[pl.ds(pl.multiple_of(slot, 8), 8), :] = stage[pl.ds(pl.multiple_of(t * 8, 8), 8), :]
            return carry
        lax.fori_loop(0, block // UNROLL, place, 0)

    @pl.when(step >= steps)
    def _():
        gates_ref[...] = jnp.zeros_like(gates_ref)
        row = lax.broadcasted_iota(jnp.int32, (capacity, 128), 0)
        lane = lax.broadcasted_iota(jnp.int32, (capacity, 128), 1)

        def unload(i, carry):
            d = i // n_local
            e = i % n_local
            first = (((step - steps) * group + d) * n_local + e) * (capacity * 8)
            for r in range(0, capacity, ROW_GROUP):
                for c in range(2 * cols):
                    span = slice(c % cols * 128, (c % cols + 1) * 128)
                    xd_ref[d, e, c // cols, r:r + ROW_GROUP, span] = table[
                        pl.ds(first + r * 8 + c, ROW_GROUP, stride=8), :].astype(jnp.bfloat16)
            gate = table[pl.ds(first + 2 * cols, capacity, stride=8), :]
            for c in range(lane_cols):
                gates_ref[d, pl.ds(e * lane_cols + c, 1), :] = jnp.sum(
                    jnp.where(row == lane + c * 128, gate, 0.0), axis=0, keepdims=True)
            return carry
        lax.fori_loop(0, group * n_local, unload, 0)


def dispatch(slot_rows, x_tokens, grad_y, gate_rows, n_dev, n_local, capacity, lanes):
    tokens, d_model = x_tokens.shape
    steps, block = gate_rows.shape
    n_slots = n_dev * n_local * capacity
    table_rows = -(-(n_slots + 1) * 8 // 512) * 512
    tok = lambda i: (jnp.minimum(i, steps - 1), 0)
    dst = lambda i: jnp.maximum(i - steps, 0)
    return pl.pallas_call(
        functools.partial(dispatch_kernel, steps, capacity, lanes // 128),
        grid=(steps + n_dev // GROUP,),
        out_shape=(jax.ShapeDtypeStruct((n_dev, n_local, 2, capacity, d_model), jnp.bfloat16),
                   jax.ShapeDtypeStruct((n_dev, 8, 128), jnp.float32)),
        in_specs=[pl.BlockSpec(memory_space=pltpu.SMEM),
                  pl.BlockSpec((block, d_model), tok),
                  pl.BlockSpec((block, d_model), tok),
                  pl.BlockSpec((steps, block), lambda i: (0, 0))],
        out_specs=(pl.BlockSpec((GROUP, n_local, 2, capacity, d_model), lambda i: (dst(i), 0, 0, 0, 0)),
                   pl.BlockSpec((GROUP, 8, 128), lambda i: (dst(i), 0, 0))),
        scratch_shapes=[pltpu.VMEM((table_rows, 128), jnp.float32),
                        pltpu.VMEM((block * 8, 128), jnp.float32)],
        compiler_params=pltpu.CompilerParams(dimension_semantics=('arbitrary',), vmem_limit_bytes=62 * 1024 * 1024),
        name='dispatch',
    )(slot_rows, x_tokens, grad_y, gate_rows)


def combine_kernel(fills, sources, capacity, slot_ref, back_ref, dl_ref, wr_t_ref, gwi_ref, gwo_t_ref,
                   gx_ref, gwi_out_ref, gwo_out_ref, table, stage):
    step = pl.program_id(0)
    block, d_model = gx_ref.shape
    cols = d_model // 128
    group, n_local = back_ref.shape[:2]
    n_slots = sources * n_local * capacity
    gwi_out_ref[...] = gwi_ref[...]
    gwo_out_ref[0] = gwo_t_ref[0].T

    @pl.when(step == 0)
    def _():
        table[pl.ds(n_slots * 8, 8), :] = jnp.zeros((8, 128), jnp.float32)

    @pl.when(step < fills)
    def _():
        def load(i, carry):
            d = i // n_local
            e = i % n_local
            first = ((step * group + d) * n_local + e) * (capacity * 8)
            for r in range(0, capacity, ROW_GROUP):
                for c in range(cols):
                    table[pl.ds(first + r * 8 + c, ROW_GROUP, stride=8), :] = back_ref[
                        d, e, r:r + ROW_GROUP, c * 128:(c + 1) * 128].astype(jnp.float32)
            return carry
        lax.fori_loop(0, group * n_local, load, 0)

    @pl.when(step >= fills)
    def _():
        part = step - fills

        def pick(i, carry):
            for u in range(UNROLL):
                t = i * UNROLL + u
                slot = slot_ref[part * block + t]
                stage[pl.ds(pl.multiple_of(t * 8, 8), 8), :] = table[pl.ds(pl.multiple_of(slot, 8), 8), :]
            return carry
        lax.fori_loop(0, block // UNROLL, pick, 0)
        hi, mid, low = split3(dl_ref[...])
        left = jnp.concatenate([hi, mid, hi, low, mid, hi], axis=0)
        w_hi, w_mid, w_low = split3(wr_t_ref[...])
        right = jnp.concatenate([w_hi, w_hi, w_mid, w_hi, w_mid, w_low], axis=0)
        dx_router = lax.dot_general(left, right, (((0,), (0,)), ((), ())), preferred_element_type=jnp.float32)
        for r in range(0, block, ROW_GROUP):
            for c in range(cols):
                span = slice(c * 128, (c + 1) * 128)
                gx_ref[r:r + ROW_GROUP, span] = (stage[pl.ds(r * 8 + c, ROW_GROUP, stride=8), :]
                                                 + dx_router[r:r + ROW_GROUP, span]).astype(jnp.bfloat16)


def combine(slot_rows, back, d_logits, w_router, gw_in, gw_out_t):
    n_dev, n_local, capacity, d_model = back.shape
    num_experts, tokens = d_logits.shape
    d_ff = gw_in.shape[2]
    block = ROW_TOKENS
    blocks = tokens // block
    fills = n_dev // GROUP
    steps = fills + blocks
    n_slots = n_dev * n_local * capacity
    gw_in_rows = gw_in.reshape(n_local * d_model, d_ff)
    in_rows = n_local * d_model // steps
    out_cols = d_ff // 256
    src = lambda i: jnp.minimum(i, fills - 1)
    tok = lambda i: (jnp.maximum(i - fills, 0), 0)
    flip = lambda i: jnp.minimum(i, n_local * out_cols - 1)
    gx, gw_in_out, gw_out = pl.pallas_call(
        functools.partial(combine_kernel, fills, n_dev, capacity),
        grid=(steps,),
        out_shape=(jax.ShapeDtypeStruct((tokens, d_model), jnp.bfloat16),
                   jax.ShapeDtypeStruct((n_local * d_model, d_ff), jnp.float32),
                   jax.ShapeDtypeStruct((n_local, d_ff, d_model), jnp.float32)),
        in_specs=[pl.BlockSpec(memory_space=pltpu.SMEM),
                  pl.BlockSpec((GROUP, n_local, capacity, d_model), lambda i: (src(i), 0, 0, 0)),
                  pl.BlockSpec((num_experts, block), lambda i: (0, jnp.maximum(i - fills, 0))),
                  pl.BlockSpec((num_experts, d_model), lambda i: (0, 0)),
                  pl.BlockSpec((in_rows, d_ff), lambda i: (i, 0)),
                  pl.BlockSpec((1, d_model, 256), lambda i: (flip(i) // out_cols, 0, flip(i) % out_cols))],
        out_specs=(pl.BlockSpec((block, d_model), tok),
                   pl.BlockSpec((in_rows, d_ff), lambda i: (i, 0)),
                   pl.BlockSpec((1, 256, d_model), lambda i: (flip(i) // out_cols, flip(i) % out_cols, 0))),
        scratch_shapes=[pltpu.VMEM(((n_slots + 1) * 8, 128), jnp.float32),
                        pltpu.VMEM((block * 8, 128), jnp.float32)],
        compiler_params=pltpu.CompilerParams(dimension_semantics=('arbitrary',), vmem_limit_bytes=63 * 1024 * 1024),
        name='combine',
    )(slot_rows, back, d_logits, w_router.T, gw_in_rows, gw_out_t)
    return gx, gw_in_out.reshape(n_local, d_model, d_ff), gw_out


def flip_bits(me, k, n):
    out = 0
    bit = 1
    while bit < n:
        mine = (me // bit) % 2
        flip = (k // bit) % 2
        out = out + bit * (mine + flip - 2 * mine * flip)
        bit *= 2
    return out


def tile_at(t):
    quarter = t // 4
    edge = (7 - quarter) // 7 + quarter // 7
    turn = (t + 4) % 8
    piece = (1 - edge) * (turn // 2) + edge * (t % 4)
    stage = (t + 4) // 8
    chip = stage * (7 - stage) // 2 + stage // 4
    chip = chip + (1 - edge) * (turn % 2) * (7 - 2 * chip)
    return chip * 2 + piece // 2, piece % 2


def link_sets(n, n_local):
    assert n == 16
    pieces = []
    for chips in ((3, 4), (5, 2), (6, 1), (7,)):
        pieces.append([[(chip * 2 + c, e) for c in range(2) for e in range(n_local)] for chip in chips])
    return pieces


def exchange_kernel(n, n_local, total_tok, xd_ref, gate_ref, stat_ref, w_in_hbm, w_out_hbm,
                    x_hbm, prob_ref, pos_ref, idx_ref, gate_rows_ref, norm_ref,
                    gw_in_hbm, gw_out_t_hbm, back_ref, dl_ref, gwr_ref, stat_out_ref,
                    w_in_ref, w_out_ref, gw_in_ref, gw_out_t_ref, x_ref, gwr_acc, gwr_s, gwr_r, gwr_mine,
                    xr, gate_r, g_s, g_r, stat_r,
                    fwd_send, fwd_recv, gate_send, gate_recv,
                    ret_send, ret_recv, g_send, g_recv, stat_send, stat_recv, a_send, a_recv, b_send, b_recv, loc_sem):
    me = lax.axis_index('ep')
    cap, d_model = xr.shape[3], xr.shape[4]
    d_ff = w_in_ref.shape[2]

    def peer_of(k):
        return flip_bits(me, k, n)

    def fwd_copy(k, e, part):
        sem = (k * n_local + e) * 2 + part
        peer = peer_of(k)
        return pltpu.make_async_remote_copy(
            src_ref=xd_ref.at[peer, e, part], dst_ref=xr.at[k, e, part],
            send_sem=fwd_send.at[sem], recv_sem=fwd_recv.at[sem],
            device_id=(peer,), device_id_type=MESH)

    def gate_copy(k):
        peer = peer_of(k)
        return pltpu.make_async_remote_copy(
            src_ref=gate_ref.at[peer], dst_ref=gate_r.at[k],
            send_sem=gate_send.at[k], recv_sem=gate_recv.at[k],
            device_id=(peer,), device_id_type=MESH)

    def stat_copy(k):
        return pltpu.make_async_remote_copy(
            src_ref=stat_ref, dst_ref=stat_r.at[me],
            send_sem=stat_send.at[k], recv_sem=stat_recv.at[k],
            device_id=(peer_of(k),), device_id_type=MESH)

    def ret_copy(k, e):
        sem = k * n_local + e
        return pltpu.make_async_remote_copy(
            src_ref=xr.at[k, e, 0], dst_ref=back_ref.at[me, e],
            send_sem=ret_send.at[sem], recv_sem=ret_recv.at[sem],
            device_id=(peer_of(k),), device_id_type=MESH)

    def g_copy(k):
        return pltpu.make_async_remote_copy(
            src_ref=g_s.at[k], dst_ref=g_r.at[me],
            send_sem=g_send.at[k], recv_sem=g_recv.at[k],
            device_id=(peer_of(k),), device_id_type=MESH)

    def scatter_copy(k):
        peer = peer_of(k)
        return pltpu.make_async_remote_copy(
            src_ref=gwr_s.at[peer], dst_ref=gwr_r.at[me], send_sem=a_send.at[k], recv_sem=a_recv.at[k],
            device_id=(peer,), device_id_type=MESH)

    def spread_copy(k):
        return pltpu.make_async_remote_copy(
            src_ref=gwr_mine, dst_ref=gwr_ref.at[me], send_sem=b_send.at[k], recv_sem=b_recv.at[k],
            device_id=(peer_of(k),), device_id_type=MESH)

    sets = link_sets(n, n_local)

    def interleave(queues):
        return [queue[i] for i in range(len(queues[0])) for queue in queues]

    def send_rows(queues):
        for k, e in interleave(queues):
            if e == 0:
                gate_copy(k).start()
                stat_copy(k).start()
            for part in range(2):
                fwd_copy(k, e, part).start()

    def rows_left(queues):
        for queue in queues:
            for i, (k, e) in enumerate(queue):
                fwd_copy(k, e, 0).wait_send()
                if i < len(queue) - 1:
                    fwd_copy(k, e, 1).wait_send()

    def send_grads(queues, lo=0, hi=None):
        for k, e in interleave(queues)[lo:hi]:
            ret_copy(k, e).start()

    def grads_left(queues):
        for queue in queues:
            for k, e in queue[:-1]:
                ret_copy(k, e).wait_send()

    near = [[(1, e) for e in range(n_local)]]
    own_in = [pltpu.make_async_copy(xd_ref.at[me, e], xr.at[0, e], loc_sem.at[e]) for e in range(n_local)]
    own_gate = pltpu.make_async_copy(gate_ref.at[me], gate_r.at[0], loc_sem.at[n_local])
    own_out = [pltpu.make_async_copy(xr.at[0, e, 0], back_ref.at[me, e], loc_sem.at[e]) for e in range(n_local)]
    load_x = pltpu.make_async_copy(x_hbm, x_ref, loc_sem.at[n_local + 3])

    send_rows(sets[0])
    send_rows(near)
    for c in own_in:
        c.start()
    own_gate.start()
    weights = [pltpu.make_async_copy(w_in_hbm, w_in_ref, loc_sem.at[n_local + 1]),
               pltpu.make_async_copy(w_out_hbm, w_out_ref, loc_sem.at[n_local + 2])]
    for c in weights:
        c.start()
    load_x.start()
    gwr_s[...] = jnp.zeros_like(gwr_s)
    gw_in_ref[...] = jnp.zeros_like(gw_in_ref)
    gw_out_t_ref[...] = jnp.zeros_like(gw_out_t_ref)
    g_s[...] = jnp.zeros_like(g_s)
    stat_r[me] = stat_ref[...]
    for c in own_in:
        c.wait()
    own_gate.wait()
    for c in weights:
        c.wait()

    lane_cols = -(-cap // 128)
    lanes = lane_cols * 128

    def tile(k, e):
        eye = (lax.broadcasted_iota(jnp.int32, (cap, lanes), 0)
               == lax.broadcasted_iota(jnp.int32, (cap, lanes), 1))
        rows = xr[k, e, 0]
        dy = xr[k, e, 1].astype(jnp.float32)
        gate_row = jnp.concatenate([gate_r[k, pl.ds(e * lane_cols + c, 1), :] for c in range(lane_cols)], axis=1)
        gate_col = jnp.sum(jnp.where(eye, gate_row, 0.0), axis=1, keepdims=True)
        grad = (gate_col * dy).astype(jnp.bfloat16)
        rows_t = rows.T
        grad_t = grad.T
        out = jnp.zeros((cap, d_model), jnp.float32)
        d_rows = jnp.zeros((cap, d_model), jnp.float32)
        for f in range(0, d_ff, F_CHUNK):
            fs = pl.ds(f, F_CHUNK)
            w_a = w_in_ref[e, :, fs]
            w_b = w_out_ref[e, fs, :]
            pre = jnp.dot(rows, w_a, preferred_element_type=jnp.float32)
            hid = jnp.maximum(pre, 0.0).astype(jnp.bfloat16)
            out = out + jnp.dot(hid, w_b, preferred_element_type=jnp.float32)
            d_hid = nt_dot(grad, w_b)
            d_pre = jnp.where(hid.astype(jnp.float32) > 0, d_hid, 0.0).astype(jnp.bfloat16)
            gw_out_t_ref[e, :, fs] += jnp.dot(grad_t, hid, preferred_element_type=jnp.float32)
            gw_in_ref[e, :, fs] += jnp.dot(rows_t, d_pre, preferred_element_type=jnp.float32)
            d_rows = d_rows + nt_dot(d_pre, w_a)
        out = out.astype(jnp.bfloat16).astype(jnp.float32)
        g_col = jnp.sum(out * dy, axis=1, keepdims=True)
        g_row = jnp.sum(jnp.where(eye, g_col, 0.0), axis=0, keepdims=True)
        for c in range(lane_cols):
            g_s[k, pl.ds(e * lane_cols + c, 1), :] = g_row[:, c * 128:(c + 1) * 128]
        xr[k, e, 0] = d_rows.astype(jnp.bfloat16)

    order = [(0, e) for e in range(n_local)] + near[0]
    first = []
    for queues in sets:
        first.append(len(order))
        order = order + interleave(queues)
    assert order == [tile_at(t) for t in range(len(order))]

    def own_back():
        send_grads(near)
        for c in own_out:
            c.start()

    def after_rows(done, then):
        def run():
            rows_left(sets[done])
            then()
        return run

    def after_grads(done, then):
        def run():
            grads_left(sets[done])
            then()
        return run

    events = {
        first[0]: own_back,
        first[1] - 2: after_rows(0, lambda: send_rows(sets[1])),
        first[2] - 2: after_rows(1, lambda: send_grads(sets[0])),
        first[2]: after_grads(0, lambda: send_rows(sets[2])),
        first[3] - 2: after_rows(2, lambda: send_grads(sets[1])),
        first[3]: after_grads(1, lambda: send_rows(sets[3])),
        len(order) - 1: after_rows(3, lambda: send_grads(sets[2], 0, 4)),
    }

    def step(t, carry):
        k, e = tile_at(t)
        for at, run in events.items():
            pl.when(t == at)(run)

        @pl.when(t >= n_local)
        def _():
            @pl.when(e == 0)
            def _():
                gate_copy(k).wait_recv()
            for part in range(2):
                fwd_copy(k, e, part).wait_recv()

        tile(k, e)

        @pl.when(t >= n_local)
        def _():
            @pl.when(e == n_local - 1)
            def _():
                g_copy(k).start()
        return carry

    lax.fori_loop(0, len(order), step, 0)
    send_grads(sets[2], 4)
    totals = [pltpu.make_async_copy(gw_in_ref, gw_in_hbm, loc_sem.at[n_local + 1]),
              pltpu.make_async_copy(gw_out_t_ref, gw_out_t_hbm, loc_sem.at[n_local + 2])]
    for c in totals:
        c.start()
    load_x.wait()
    g_r[me] = g_s[0]
    grads_left(sets[2])
    send_grads(sets[3], 0, 2)

    def arrive(k, carry):
        stat_copy(k).wait()
        g_copy(k).wait()
        return carry

    lax.fori_loop(1, n, arrive, 0)
    stat = stat_r[0]
    for i in range(1, n):
        stat = stat + stat_r[i]
    stat_out_ref[...] = stat
    num_experts = n * n_local
    load = jnp.sum(jnp.where(eye_mask(num_experts, 128), stat[0:1, :], 0.0), axis=1, keepdims=True)
    aux_vec = (AUX_WEIGHT * num_experts / total_tok) * (load / total_tok)
    g_all = jnp.concatenate([
        jnp.concatenate([g_r[:, e * lane_cols + c, :] for c in range(lane_cols)], axis=1) for e in range(n_local)], axis=0)
    g_parts = jnp.concatenate(split3(g_all), axis=0)
    span = pos_ref.shape[1]
    gwr_acc[...] = jnp.zeros_like(gwr_acc)

    def router(c, carry):
        here = pl.ds(c, 1)
        cols = pl.ds(pl.multiple_of(c * span, span), span)
        place = jnp.where(lax.broadcasted_iota(jnp.int32, (lanes, span), 0) == pos_ref[here, :], 1.0, 0.0)
        found = jnp.dot(g_parts, place.astype(jnp.bfloat16), preferred_element_type=jnp.float32)
        found = found[:num_experts] + found[num_experts:2 * num_experts] + found[2 * num_experts:]
        chosen = jnp.where(lax.broadcasted_iota(jnp.int32, (num_experts, span), 0) == idx_ref[here, :], 1.0, 0.0)
        row = lax.broadcasted_iota(jnp.int32, (num_experts, span), 0)
        owner = jnp.where(row < n, row * n_local, (row - n) * n_local + 1)
        g_tok = jnp.sum(jnp.where(owner == idx_ref[here, :], found, 0.0), axis=0, keepdims=True)
        prob = prob_ref[:, cols]
        spread = jnp.sum(prob * aux_vec, axis=0, keepdims=True)
        d_logits = ((gate_rows_ref[here, :] * g_tok) * (chosen - prob) + prob * (aux_vec - spread)
                    + ((2.0 * Z_WEIGHT / total_tok) * norm_ref[here, :]) * prob)
        dl_ref[:, cols] = d_logits
        gwr_acc[...] += jnp.dot(jnp.concatenate(split3(d_logits), axis=0), x_ref[cols, :], preferred_element_type=jnp.float32)
        return carry

    lax.fori_loop(0, pos_ref.shape[0], router, 0)
    part = gwr_acc[0:num_experts, :] + gwr_acc[num_experts:2 * num_experts, :] + gwr_acc[2 * num_experts:, :]
    d_cols = d_model // 128
    for d in range(n):
        for c in range(n_local * d_cols):
            r = d * n_local + c // d_cols
            gwr_s[d, c:c + 1, :] = part[r:r + 1, c % d_cols * 128:(c % d_cols + 1) * 128]
    gwr_r[me] = gwr_s[me]

    def scatter(k, carry):
        scatter_copy(k).start()
        return carry

    lax.fori_loop(1, n, scatter, 0)
    send_grads(sets[3], 2, 3)

    def gathered(k, carry):
        scatter_copy(k).wait()
        return carry

    lax.fori_loop(1, n, gathered, 0)
    mine = gwr_r[0]
    for i in range(1, n):
        mine = mine + gwr_r[i]
    gwr_mine[...] = mine
    gwr_ref[me] = mine

    def spread_all(k, carry):
        spread_copy(k).start()
        return carry

    lax.fori_loop(1, n, spread_all, 0)
    send_grads(sets[3], 3)

    for queues in sets:
        for queue in queues:
            k, e = queue[-1]
            fwd_copy(k, e, 1).wait_send()
            if queues is not sets[3]:
                ret_copy(k, e).wait_send()
    grads_left(sets[3])
    for queue in sets[3]:
        ret_copy(*queue[-1]).wait_send()
    for k, e in near[0]:
        for part in range(2):
            fwd_copy(k, e, part).wait_send()
        ret_copy(k, e).wait_send()
    for c in own_out:
        c.wait()
    for c in totals:
        c.wait()

    def drain(k, carry):
        gate_copy(k).wait_send()
        spread_copy(k).wait()
        for e in range(n_local):
            ret_copy(k, e).wait_recv()
        return carry

    lax.fori_loop(1, n, drain, 0)


def exchange(xd, gates, stats, w_in, w_out, x_tokens, prob, pos_rows, idx_rows, gate_rows, norm_rows, n_dev):
    n_local, d_model, d_ff = w_in.shape
    cap = xd.shape[3]
    any_spec = pl.BlockSpec(memory_space=pl.ANY)
    vmem_spec = pl.BlockSpec(memory_space=pltpu.VMEM)
    pairs = n_dev * n_local
    dma = pltpu.SemaphoreType.DMA
    return pl.pallas_call(
        functools.partial(exchange_kernel, n_dev, n_local, x_tokens.shape[0] * n_dev),
        out_shape=(jax.ShapeDtypeStruct((n_local, d_model, d_ff), jnp.float32),
                   jax.ShapeDtypeStruct((n_local, d_model, d_ff), jnp.float32),
                   jax.ShapeDtypeStruct((n_dev, n_local, cap, d_model), jnp.bfloat16),
                   jax.ShapeDtypeStruct(prob.shape, jnp.float32),
                   jax.ShapeDtypeStruct((n_dev, 8, 128), jnp.float32),
                   jax.ShapeDtypeStruct(stats.shape, jnp.float32)),
        in_specs=[any_spec, any_spec, vmem_spec, any_spec, any_spec, any_spec] + [vmem_spec] * 5,
        out_specs=(any_spec, any_spec, any_spec, vmem_spec, vmem_spec, vmem_spec),
        scratch_shapes=[
            pltpu.VMEM(w_in.shape, jnp.bfloat16),
            pltpu.VMEM(w_out.shape, jnp.bfloat16),
            pltpu.VMEM(w_in.shape, jnp.float32),
            pltpu.VMEM(w_in.shape, jnp.float32),
            pltpu.VMEM(x_tokens.shape, jnp.bfloat16),
            pltpu.VMEM((3 * pairs, d_model), jnp.float32),
            pltpu.VMEM((n_dev, 8, 128), jnp.float32),
            pltpu.VMEM((n_dev, 8, 128), jnp.float32),
            pltpu.VMEM((8, 128), jnp.float32),
            pltpu.VMEM((n_dev, n_local, 2, cap, d_model), jnp.bfloat16),
            pltpu.VMEM((n_dev, 8, 128), jnp.float32),
            pltpu.VMEM((n_dev, 8, 128), jnp.float32),
            pltpu.VMEM((n_dev, 8, 128), jnp.float32),
            pltpu.VMEM((n_dev,) + stats.shape, jnp.float32),
            dma((2 * pairs,)), dma((2 * pairs,)), dma((n_dev,)), dma((n_dev,)),
            dma((pairs,)), dma((pairs,)), dma((n_dev,)), dma((n_dev,)),
            dma((n_dev,)), dma((n_dev,)), dma((n_dev,)), dma((n_dev,)), dma((n_dev,)), dma((n_dev,)),
            dma((n_local + 4,)),
        ],
        compiler_params=pltpu.CompilerParams(has_side_effects=True, vmem_limit_bytes=60 * 1024 * 1024),
        name='exchange',
    )(xd, gates, stats, w_in, w_out, x_tokens, prob, pos_rows, idx_rows, gate_rows, norm_rows)


def solution(mesh):
    n_dev = mesh.shape['ep']

    def expert_layer(x_tokens, w_router, expert_idx, w_in, w_out, grad_y):
        tokens, d_model = x_tokens.shape
        n_local = w_in.shape[0]
        num_experts = n_local * n_dev
        capacity = (5 * tokens + 4 * num_experts - 1) // (4 * num_experts)
        total_tok = tokens * n_dev
        lanes = -(-capacity // 128) * 128
        idx_rows = expert_idx.reshape(-1, ROW_TOKENS)
        prob, slot_rows, pos_rows, gate_rows, norm_rows, stats = route(x_tokens, idx_rows, w_router, capacity)
        slot_rows = slot_rows.reshape(tokens)
        xd, gates = dispatch(slot_rows, x_tokens, grad_y, gate_rows, n_dev, n_local, capacity, lanes)
        gw_in, gw_out_t, back, d_logits, gwr, stats = exchange(xd, gates, stats, w_in, w_out, x_tokens, prob, pos_rows, idx_rows,
                                                               gate_rows, norm_rows, n_dev)
        grad_x, grad_w_in, grad_w_out = combine(slot_rows, back, d_logits, w_router, gw_in, gw_out_t)
        grad_w_router = gwr[:, :n_local * d_model // 128].reshape(num_experts, d_model).T

        load_frac = stats[0, :num_experts] / total_tok
        mean_prob = stats[0, num_experts:2 * num_experts] / total_tok
        aux_loss = AUX_WEIGHT * num_experts * jnp.sum(load_frac * mean_prob)
        z_loss = Z_WEIGHT * stats[0, 2 * num_experts] / total_tok
        return grad_x, grad_w_in, grad_w_out, grad_w_router, aux_loss, z_loss

    return jax.shard_map(expert_layer, mesh=mesh,
                         in_specs=(P('ep', None), P(None, None), P('ep'), P('ep', None, None), P('ep', None, None), P('ep', None)),
                         out_specs=(P('ep', None), P('ep', None, None), P('ep', None, None), P(None, None), P(), P()),
                         check_vma=False)
```

```python
import functools

import jax
import jax.numpy as jnp
from jax import lax
from jax.experimental import pallas as pl
from jax.experimental.pallas import tpu as pltpu
from jax.sharding import PartitionSpec as P

AUX_WEIGHT = 0.01
Z_WEIGHT = 0.001
MESH = pl.DeviceIdType.MESH
F_CHUNK = 512
TOKEN_BLOCK = 256
UNROLL = 32
LANE = 128
F32 = jnp.float32
ROW_GROUP = 32
ROW_TOKENS = 1024
GROUP = 2


def nt_dot(a, b):
    return lax.dot_general(a, b, (((1,), (1,)), ((), ())), preferred_element_type=F32)


def eye_mask(rows, cols):
    return lax.broadcasted_iota(jnp.int32, (rows, cols), 0) == lax.broadcasted_iota(jnp.int32, (rows, cols), 1)


def split3(v):
    hi = v.astype(jnp.bfloat16)
    rest = v - hi.astype(jnp.float32)
    mid = rest.astype(jnp.bfloat16)
    low = (rest - mid.astype(jnp.float32)).astype(jnp.bfloat16)
    return hi, mid, low


def route_kernel(capacity, x_ref, idx_ref, wr_ref, prob_ref, slot_ref, pos_ref, gate_ref, norm_ref, stat_ref, seen, prob_sum, z_sum):
    step = pl.program_id(0)
    num_experts, block = prob_ref.shape

    @pl.when(step == 0)
    def _():
        seen[...] = jnp.zeros_like(seen)
        prob_sum[...] = jnp.zeros_like(prob_sum)
        z_sum[...] = jnp.zeros_like(z_sum)

    parts = nt_dot(jnp.concatenate(split3(wr_ref[...]), axis=0), x_ref[...])
    logits = parts[:num_experts] + parts[num_experts:2 * num_experts] + parts[2 * num_experts:]
    top = jnp.max(logits, axis=0, keepdims=True)
    shifted = jnp.exp(logits - top)
    scale = jnp.sum(shifted, axis=0, keepdims=True)
    prob = shifted / scale
    log_norm = top + jnp.log(scale)
    idx = idx_ref[pl.ds(step, 1), :]
    chosen = jnp.where(lax.broadcasted_iota(jnp.int32, (num_experts, block), 0) == idx, 1.0, 0.0)
    prob_ref[...] = prob
    gate_ref[pl.ds(step, 1), :] = jnp.sum(prob * chosen, axis=0, keepdims=True)
    norm_ref[pl.ds(step, 1), :] = log_norm
    squares = log_norm * log_norm
    for i in range(0, block, LANE):
        prob_sum[...] += prob[:, i:i + LANE]
        z_sum[0:1, :] += squares[:, i:i + LANE]
    upto = jnp.where(lax.broadcasted_iota(jnp.int32, (TOKEN_BLOCK, TOKEN_BLOCK), 0)
                     <= lax.broadcasted_iota(jnp.int32, (TOKEN_BLOCK, TOKEN_BLOCK), 1), 1.0, 0.0).astype(jnp.bfloat16)
    before = seen[:, 0:1]
    slots = []
    places = []
    for i in range(0, block, TOKEN_BLOCK):
        part = chosen[:, i:i + TOKEN_BLOCK]
        count = jnp.dot(part.astype(jnp.bfloat16), upto, preferred_element_type=F32) + before
        position = jnp.sum(part * count, axis=0, keepdims=True).astype(jnp.int32) - 1
        places.append(position)
        slots.append(8 * jnp.where(position < capacity, idx[:, i:i + TOKEN_BLOCK] * capacity + position, num_experts * capacity))
        before = count[:, TOKEN_BLOCK - 1:TOKEN_BLOCK]
    slot_ref[pl.ds(step, 1), :] = jnp.concatenate(slots, axis=1)
    pos_ref[pl.ds(step, 1), :] = jnp.concatenate(places, axis=1)
    seen[...] = jnp.broadcast_to(before, seen.shape)

    @pl.when(step == pl.num_programs(0) - 1)
    def _():
        row = lax.broadcasted_iota(jnp.int32, (num_experts, LANE), 0)
        lane = lax.broadcasted_iota(jnp.int32, (num_experts, LANE), 1)
        probs = jnp.sum(prob_sum[...], axis=1, keepdims=True)
        stat_ref[...] = jnp.zeros_like(stat_ref)
        total = jnp.sum(jnp.where(row == lane, seen[...], 0.0) + jnp.where(row + num_experts == lane, probs, 0.0),
                        axis=0, keepdims=True)
        squares = jnp.sum(z_sum[0:1, :], axis=1, keepdims=True)
        stat_ref[0:1, :] = total + jnp.where(lane[0:1, :] == 2 * num_experts, squares, 0.0)


def route(x_tokens, idx_rows, w_router, capacity):
    tokens, d_model = x_tokens.shape
    num_experts = w_router.shape[1]
    steps, block = idx_rows.shape
    rows = lambda dtype: jax.ShapeDtypeStruct((steps, block), dtype)
    whole = pl.BlockSpec((steps, block), lambda i: (0, 0))
    return pl.pallas_call(
        functools.partial(route_kernel, capacity),
        grid=(steps,),
        out_shape=(jax.ShapeDtypeStruct((num_experts, tokens), jnp.float32), rows(jnp.int32), rows(jnp.int32), rows(jnp.float32), rows(jnp.float32),
                   jax.ShapeDtypeStruct((8, LANE), jnp.float32)),
        in_specs=[pl.BlockSpec((block, d_model), lambda i: (i, 0)), whole,
                  pl.BlockSpec((num_experts, d_model), lambda i: (0, 0))],
        out_specs=(pl.BlockSpec((num_experts, block), lambda i: (0, i)), whole, whole, whole, whole,
                   pl.BlockSpec((8, LANE), lambda i: (0, 0))),
        scratch_shapes=[pltpu.VMEM((num_experts, LANE), jnp.float32), pltpu.VMEM((num_experts, LANE), jnp.float32), pltpu.VMEM((8, LANE), jnp.float32)],
        compiler_params=pltpu.CompilerParams(dimension_semantics=('arbitrary',)),
        name='route',
    )(x_tokens, idx_rows, w_router.T)


def dispatch_kernel(steps, capacity, lane_cols, slot_ref, x_ref, dy_ref, gate_ref, xd_ref, gates_ref, table, stage):
    step = pl.program_id(0)
    block, d_model = x_ref.shape
    cols = d_model // LANE
    group, n_local = xd_ref.shape[:2]

    @pl.when(step == 0)
    def _():
        def clear(i, carry):
            table[pl.ds(pl.multiple_of(i * 512, 512), 512), :] = jnp.zeros((512, LANE), jnp.float32)
            return carry
        lax.fori_loop(0, table.shape[0] // 512, clear, 0)

    @pl.when(step < steps)
    def _():
        for r in range(0, block, ROW_GROUP):
            for c in range(2 * cols):
                rows_ref = x_ref if c < cols else dy_ref
                span = slice(c % cols * LANE, (c % cols + 1) * LANE)
                stage[pl.ds(r * 8 + c, ROW_GROUP, stride=8), :] = rows_ref[r:r + ROW_GROUP, span].astype(jnp.float32)
        eye = eye_mask(LANE, LANE)
        gate_row = gate_ref[pl.ds(step, 1), :]
        for i in range(0, block, LANE):
            gate = jnp.sum(jnp.where(eye, gate_row[:, i:i + LANE], 0.0), axis=1, keepdims=True)
            stage[pl.ds(i * 8 + 2 * cols, LANE, stride=8), :] = jnp.broadcast_to(gate, (LANE, LANE))

        def place(i, carry):
            for u in range(UNROLL):
                t = i * UNROLL + u
                slot = slot_ref[step * block + t]
                table[pl.ds(pl.multiple_of(slot, 8), 8), :] = stage[pl.ds(pl.multiple_of(t * 8, 8), 8), :]
            return carry
        lax.fori_loop(0, block // UNROLL, place, 0)

    @pl.when(step >= steps)
    def _():
        gates_ref[...] = jnp.zeros_like(gates_ref)
        row = lax.broadcasted_iota(jnp.int32, (capacity, LANE), 0)
        lane = lax.broadcasted_iota(jnp.int32, (capacity, LANE), 1)

        def unload(i, carry):
            d = i // n_local
            e = i % n_local
            first = (((step - steps) * group + d) * n_local + e) * (capacity * 8)
            for r in range(0, capacity, ROW_GROUP):
                for c in range(2 * cols):
                    span = slice(c % cols * LANE, (c % cols + 1) * LANE)
                    xd_ref[d, e, c // cols, r:r + ROW_GROUP, span] = table[
                        pl.ds(first + r * 8 + c, ROW_GROUP, stride=8), :].astype(jnp.bfloat16)
            gate = table[pl.ds(first + 2 * cols, capacity, stride=8), :]
            for c in range(lane_cols):
                gates_ref[d, pl.ds(e * lane_cols + c, 1), :] = jnp.sum(
                    jnp.where(row == lane + c * LANE, gate, 0.0), axis=0, keepdims=True)
            return carry
        lax.fori_loop(0, group * n_local, unload, 0)


def dispatch(slot_rows, x_tokens, grad_y, gate_rows, n_dev, n_local, capacity, lanes):
    tokens, d_model = x_tokens.shape
    steps, block = gate_rows.shape
    n_slots = n_dev * n_local * capacity
    table_rows = -(-(n_slots + 1) * 8 // 512) * 512
    tok = lambda i: (jnp.minimum(i, steps - 1), 0)
    dst = lambda i: jnp.maximum(i - steps, 0)
    return pl.pallas_call(
        functools.partial(dispatch_kernel, steps, capacity, lanes // LANE),
        grid=(steps + n_dev // GROUP,),
        out_shape=(jax.ShapeDtypeStruct((n_dev, n_local, 2, capacity, d_model), jnp.bfloat16),
                   jax.ShapeDtypeStruct((n_dev, 8, LANE), jnp.float32)),
        in_specs=[pl.BlockSpec(memory_space=pltpu.SMEM),
                  pl.BlockSpec((block, d_model), tok),
                  pl.BlockSpec((block, d_model), tok),
                  pl.BlockSpec((steps, block), lambda i: (0, 0))],
        out_specs=(pl.BlockSpec((GROUP, n_local, 2, capacity, d_model), lambda i: (dst(i), 0, 0, 0, 0)),
                   pl.BlockSpec((GROUP, 8, LANE), lambda i: (dst(i), 0, 0))),
        scratch_shapes=[pltpu.VMEM((table_rows, LANE), jnp.float32),
                        pltpu.VMEM((block * 8, LANE), jnp.float32)],
        compiler_params=pltpu.CompilerParams(dimension_semantics=('arbitrary',), vmem_limit_bytes=62 * 1024 * 1024),
        name='dispatch',
    )(slot_rows, x_tokens, grad_y, gate_rows)


def combine_kernel(fills, sources, capacity, slot_ref, back_ref, dl_ref, wr_t_ref, gwi_ref, gwo_t_ref,
                   gx_ref, gwi_out_ref, gwo_out_ref, table, stage):
    step = pl.program_id(0)
    block, d_model = gx_ref.shape
    cols = d_model // LANE
    group, n_local = back_ref.shape[:2]
    n_slots = sources * n_local * capacity
    gwi_out_ref[...] = gwi_ref[...]
    gwo_out_ref[0] = gwo_t_ref[0].T

    @pl.when(step == 0)
    def _():
        table[pl.ds(n_slots * 8, 8), :] = jnp.zeros((8, LANE), jnp.float32)

    @pl.when(step < fills)
    def _():
        def load(i, carry):
            d = i // n_local
            e = i % n_local
            first = ((step * group + d) * n_local + e) * (capacity * 8)
            for r in range(0, capacity, ROW_GROUP):
                for c in range(cols):
                    table[pl.ds(first + r * 8 + c, ROW_GROUP, stride=8), :] = back_ref[
                        d, e, r:r + ROW_GROUP, c * LANE:(c + 1) * LANE].astype(jnp.float32)
            return carry
        lax.fori_loop(0, group * n_local, load, 0)

    @pl.when(step >= fills)
    def _():
        part = step - fills

        def pick(i, carry):
            for u in range(UNROLL):
                t = i * UNROLL + u
                slot = slot_ref[part * block + t]
                stage[pl.ds(pl.multiple_of(t * 8, 8), 8), :] = table[pl.ds(pl.multiple_of(slot, 8), 8), :]
            return carry
        lax.fori_loop(0, block // UNROLL, pick, 0)
        hi, mid, low = split3(dl_ref[...])
        left = jnp.concatenate([hi, mid, hi, low, mid, hi], axis=0)
        w_hi, w_mid, w_low = split3(wr_t_ref[...])
        right = jnp.concatenate([w_hi, w_hi, w_mid, w_hi, w_mid, w_low], axis=0)
        dx_router = lax.dot_general(left, right, (((0,), (0,)), ((), ())), preferred_element_type=F32)
        for r in range(0, block, ROW_GROUP):
            for c in range(cols):
                span = slice(c * LANE, (c + 1) * LANE)
                gx_ref[r:r + ROW_GROUP, span] = (stage[pl.ds(r * 8 + c, ROW_GROUP, stride=8), :]
                                                 + dx_router[r:r + ROW_GROUP, span]).astype(jnp.bfloat16)


def combine(slot_rows, back, d_logits, w_router, gw_in, gw_out_t):
    n_dev, n_local, capacity, d_model = back.shape
    num_experts, tokens = d_logits.shape
    d_ff = gw_in.shape[2]
    block = ROW_TOKENS
    blocks = tokens // block
    fills = n_dev // GROUP
    steps = fills + blocks
    n_slots = n_dev * n_local * capacity
    gw_in_rows = gw_in.reshape(n_local * d_model, d_ff)
    in_rows = n_local * d_model // steps
    out_cols = d_ff // 256
    src = lambda i: jnp.minimum(i, fills - 1)
    tok = lambda i: (jnp.maximum(i - fills, 0), 0)
    flip = lambda i: jnp.minimum(i, n_local * out_cols - 1)
    gx, gw_in_out, gw_out = pl.pallas_call(
        functools.partial(combine_kernel, fills, n_dev, capacity),
        grid=(steps,),
        out_shape=(jax.ShapeDtypeStruct((tokens, d_model), jnp.bfloat16),
                   jax.ShapeDtypeStruct((n_local * d_model, d_ff), jnp.float32),
                   jax.ShapeDtypeStruct((n_local, d_ff, d_model), jnp.float32)),
        in_specs=[pl.BlockSpec(memory_space=pltpu.SMEM),
                  pl.BlockSpec((GROUP, n_local, capacity, d_model), lambda i: (src(i), 0, 0, 0)),
                  pl.BlockSpec((num_experts, block), lambda i: (0, jnp.maximum(i - fills, 0))),
                  pl.BlockSpec((num_experts, d_model), lambda i: (0, 0)),
                  pl.BlockSpec((in_rows, d_ff), lambda i: (i, 0)),
                  pl.BlockSpec((1, d_model, 256), lambda i: (flip(i) // out_cols, 0, flip(i) % out_cols))],
        out_specs=(pl.BlockSpec((block, d_model), tok),
                   pl.BlockSpec((in_rows, d_ff), lambda i: (i, 0)),
                   pl.BlockSpec((1, 256, d_model), lambda i: (flip(i) // out_cols, flip(i) % out_cols, 0))),
        scratch_shapes=[pltpu.VMEM(((n_slots + 1) * 8, LANE), jnp.float32),
                        pltpu.VMEM((block * 8, LANE), jnp.float32)],
        compiler_params=pltpu.CompilerParams(dimension_semantics=('arbitrary',), vmem_limit_bytes=63 * 1024 * 1024),
        name='combine',
    )(slot_rows, back, d_logits, w_router.T, gw_in_rows, gw_out_t)
    return gx, gw_in_out.reshape(n_local, d_model, d_ff), gw_out


def flip_bits(me, k, n):
    out = 0
    bit = 1
    while bit < n:
        mine = (me // bit) % 2
        flip = (k // bit) % 2
        out = out + bit * (mine + flip - 2 * mine * flip)
        bit *= 2
    return out


def tile_at(t):
    quarter = t // 4
    edge = (7 - quarter) // 7 + quarter // 7
    turn = (t + 4) % 8
    piece = (1 - edge) * (turn // 2) + edge * (t % 4)
    stage = (t + 4) // 8
    chip = stage * (7 - stage) // 2 + stage // 4
    chip = chip + (1 - edge) * (turn % 2) * (7 - 2 * chip)
    return chip * 2 + piece // 2, piece % 2


def link_sets(n, n_local):
    assert n == 16
    pieces = []
    for chips in ((3, 4), (5, 2), (6, 1), (7,)):
        pieces.append([[(chip * 2 + c, e) for c in range(2) for e in range(n_local)] for chip in chips])
    return pieces


def exchange_kernel(n, n_local, total_tok, xd_ref, gate_ref, stat_ref, w_in_hbm, w_out_hbm,
                    x_hbm, prob_ref, pos_ref, idx_ref, gate_rows_ref, norm_ref,
                    gw_in_hbm, gw_out_t_hbm, back_ref, dl_ref, gwr_ref, stat_out_ref,
                    w_in_ref, w_out_ref, gw_in_ref, gw_out_t_ref, x_ref, gwr_acc, gwr_s, gwr_r, gwr_mine,
                    xr, gate_r, g_s, g_r, stat_r,
                    fwd_send, fwd_recv, gate_send, gate_recv,
                    ret_send, ret_recv, g_send, g_recv, stat_send, stat_recv, a_send, a_recv, b_send, b_recv, loc_sem):
    me = lax.axis_index('ep')
    cap, d_model = xr.shape[3], xr.shape[4]
    d_ff = w_in_ref.shape[2]

    def peer_of(k):
        return flip_bits(me, k, n)

    def fwd_copy(k, e, part):
        sem = (k * n_local + e) * 2 + part
        peer = peer_of(k)
        return pltpu.make_async_remote_copy(
            src_ref=xd_ref.at[peer, e, part], dst_ref=xr.at[k, e, part],
            send_sem=fwd_send.at[sem], recv_sem=fwd_recv.at[sem],
            device_id=(peer,), device_id_type=MESH)

    def gate_copy(k):
        peer = peer_of(k)
        return pltpu.make_async_remote_copy(
            src_ref=gate_ref.at[peer], dst_ref=gate_r.at[k],
            send_sem=gate_send.at[k], recv_sem=gate_recv.at[k],
            device_id=(peer,), device_id_type=MESH)

    def stat_copy(k):
        return pltpu.make_async_remote_copy(
            src_ref=stat_ref, dst_ref=stat_r.at[me],
            send_sem=stat_send.at[k], recv_sem=stat_recv.at[k],
            device_id=(peer_of(k),), device_id_type=MESH)

    def ret_copy(k, e):
        sem = k * n_local + e
        return pltpu.make_async_remote_copy(
            src_ref=xr.at[k, e, 0], dst_ref=back_ref.at[me, e],
            send_sem=ret_send.at[sem], recv_sem=ret_recv.at[sem],
            device_id=(peer_of(k),), device_id_type=MESH)

    def g_copy(k):
        return pltpu.make_async_remote_copy(
            src_ref=g_s.at[k], dst_ref=g_r.at[me],
            send_sem=g_send.at[k], recv_sem=g_recv.at[k],
            device_id=(peer_of(k),), device_id_type=MESH)

    def scatter_copy(k):
        peer = peer_of(k)
        return pltpu.make_async_remote_copy(
            src_ref=gwr_s.at[peer], dst_ref=gwr_r.at[me], send_sem=a_send.at[k], recv_sem=a_recv.at[k],
            device_id=(peer,), device_id_type=MESH)

    def spread_copy(k):
        return pltpu.make_async_remote_copy(
            src_ref=gwr_mine, dst_ref=gwr_ref.at[me], send_sem=b_send.at[k], recv_sem=b_recv.at[k],
            device_id=(peer_of(k),), device_id_type=MESH)

    sets = link_sets(n, n_local)

    def interleave(queues):
        return [queue[i] for i in range(len(queues[0])) for queue in queues]

    def send_rows(queues):
        for k, e in interleave(queues):
            if e == 0:
                gate_copy(k).start()
                stat_copy(k).start()
            for part in range(2):
                fwd_copy(k, e, part).start()

    def rows_left(queues):
        for queue in queues:
            for i, (k, e) in enumerate(queue):
                fwd_copy(k, e, 0).wait_send()
                if i < len(queue) - 1:
                    fwd_copy(k, e, 1).wait_send()

    def send_grads(queues, lo=0, hi=None):
        for k, e in interleave(queues)[lo:hi]:
            ret_copy(k, e).start()

    def grads_left(queues):
        for queue in queues:
            for k, e in queue[:-1]:
                ret_copy(k, e).wait_send()

    near = [[(1, e) for e in range(n_local)]]
    own_in = [pltpu.make_async_copy(xd_ref.at[me, e], xr.at[0, e], loc_sem.at[e]) for e in range(n_local)]
    own_gate = pltpu.make_async_copy(gate_ref.at[me], gate_r.at[0], loc_sem.at[n_local])
    own_out = [pltpu.make_async_copy(xr.at[0, e, 0], back_ref.at[me, e], loc_sem.at[e]) for e in range(n_local)]
    load_x = pltpu.make_async_copy(x_hbm, x_ref, loc_sem.at[n_local + 3])

    send_rows(sets[0])
    send_rows(near)
    for c in own_in:
        c.start()
    own_gate.start()
    weights = [pltpu.make_async_copy(w_in_hbm, w_in_ref, loc_sem.at[n_local + 1]),
               pltpu.make_async_copy(w_out_hbm, w_out_ref, loc_sem.at[n_local + 2])]
    for c in weights:
        c.start()
    load_x.start()
    gwr_s[...] = jnp.zeros_like(gwr_s)
    gw_in_ref[...] = jnp.zeros_like(gw_in_ref)
    gw_out_t_ref[...] = jnp.zeros_like(gw_out_t_ref)
    g_s[...] = jnp.zeros_like(g_s)
    stat_r[me] = stat_ref[...]
    for c in own_in:
        c.wait()
    own_gate.wait()
    for c in weights:
        c.wait()

    lane_cols = -(-cap // LANE)
    lanes = lane_cols * LANE

    def tile(k, e):
        eye = (lax.broadcasted_iota(jnp.int32, (cap, lanes), 0)
               == lax.broadcasted_iota(jnp.int32, (cap, lanes), 1))
        rows = xr[k, e, 0]
        dy = xr[k, e, 1].astype(jnp.float32)
        gate_row = jnp.concatenate([gate_r[k, pl.ds(e * lane_cols + c, 1), :] for c in range(lane_cols)], axis=1)
        gate_col = jnp.sum(jnp.where(eye, gate_row, 0.0), axis=1, keepdims=True)
        grad = (gate_col * dy).astype(jnp.bfloat16)
        rows_t = rows.T
        grad_t = grad.T
        out = jnp.zeros((cap, d_model), jnp.float32)
        d_rows = jnp.zeros((cap, d_model), jnp.float32)
        for f in range(0, d_ff, F_CHUNK):
            fs = pl.ds(f, F_CHUNK)
            w_a = w_in_ref[e, :, fs]
            w_b = w_out_ref[e, fs, :]
            pre = jnp.dot(rows, w_a, preferred_element_type=F32)
            hid = jnp.maximum(pre, 0.0).astype(jnp.bfloat16)
            out = out + jnp.dot(hid, w_b, preferred_element_type=F32)
            d_hid = nt_dot(grad, w_b)
            d_pre = jnp.where(hid.astype(jnp.float32) > 0, d_hid, 0.0).astype(jnp.bfloat16)
            gw_out_t_ref[e, :, fs] += jnp.dot(grad_t, hid, preferred_element_type=F32)
            gw_in_ref[e, :, fs] += jnp.dot(rows_t, d_pre, preferred_element_type=F32)
            d_rows = d_rows + nt_dot(d_pre, w_a)
        out = out.astype(jnp.bfloat16).astype(jnp.float32)
        g_col = jnp.sum(out * dy, axis=1, keepdims=True)
        g_row = jnp.sum(jnp.where(eye, g_col, 0.0), axis=0, keepdims=True)
        for c in range(lane_cols):
            g_s[k, pl.ds(e * lane_cols + c, 1), :] = g_row[:, c * LANE:(c + 1) * LANE]
        xr[k, e, 0] = d_rows.astype(jnp.bfloat16)

    order = [(0, e) for e in range(n_local)] + near[0]
    first = []
    for queues in sets:
        first.append(len(order))
        order = order + interleave(queues)
    assert order == [tile_at(t) for t in range(len(order))]

    def own_back():
        send_grads(near)
        for c in own_out:
            c.start()

    def after_rows(done, then):
        def run():
            rows_left(sets[done])
            then()
        return run

    def after_grads(done, then):
        def run():
            grads_left(sets[done])
            then()
        return run

    events = {
        first[0]: own_back,
        first[1] - 2: after_rows(0, lambda: send_rows(sets[1])),
        first[2] - 2: after_rows(1, lambda: send_grads(sets[0])),
        first[2]: after_grads(0, lambda: send_rows(sets[2])),
        first[3] - 2: after_rows(2, lambda: send_grads(sets[1])),
        first[3]: after_grads(1, lambda: send_rows(sets[3])),
        len(order) - 1: after_rows(3, lambda: send_grads(sets[2], 0, 4)),
    }

    def step(t, carry):
        k, e = tile_at(t)
        for at, run in events.items():
            pl.when(t == at)(run)

        @pl.when(t >= n_local)
        def _():
            @pl.when(e == 0)
            def _():
                gate_copy(k).wait_recv()
            for part in range(2):
                fwd_copy(k, e, part).wait_recv()

        tile(k, e)

        @pl.when(t >= n_local)
        def _():
            @pl.when(e == n_local - 1)
            def _():
                g_copy(k).start()
        return carry

    lax.fori_loop(0, len(order), step, 0)
    send_grads(sets[2], 4)
    totals = [pltpu.make_async_copy(gw_in_ref, gw_in_hbm, loc_sem.at[n_local + 1]),
              pltpu.make_async_copy(gw_out_t_ref, gw_out_t_hbm, loc_sem.at[n_local + 2])]
    for c in totals:
        c.start()
    load_x.wait()
    g_r[me] = g_s[0]
    grads_left(sets[2])
    send_grads(sets[3], 0, 2)

    def arrive(k, carry):
        stat_copy(k).wait()
        g_copy(k).wait()
        return carry

    lax.fori_loop(1, n, arrive, 0)
    stat = stat_r[0]
    for i in range(1, n):
        stat = stat + stat_r[i]
    stat_out_ref[...] = stat
    num_experts = n * n_local
    load = jnp.sum(jnp.where(eye_mask(num_experts, LANE), stat[0:1, :], 0.0), axis=1, keepdims=True)
    aux_vec = (AUX_WEIGHT * num_experts / total_tok) * (load / total_tok)
    g_all = jnp.concatenate([
        jnp.concatenate([g_r[:, e * lane_cols + c, :] for c in range(lane_cols)], axis=1) for e in range(n_local)], axis=0)
    g_parts = jnp.concatenate(split3(g_all), axis=0)
    span = pos_ref.shape[1]
    gwr_acc[...] = jnp.zeros_like(gwr_acc)

    def router(c, carry):
        here = pl.ds(c, 1)
        cols = pl.ds(pl.multiple_of(c * span, span), span)
        place = jnp.where(lax.broadcasted_iota(jnp.int32, (lanes, span), 0) == pos_ref[here, :], 1.0, 0.0)
        found = jnp.dot(g_parts, place.astype(jnp.bfloat16), preferred_element_type=F32)
        found = found[:num_experts] + found[num_experts:2 * num_experts] + found[2 * num_experts:]
        chosen = jnp.where(lax.broadcasted_iota(jnp.int32, (num_experts, span), 0) == idx_ref[here, :], 1.0, 0.0)
        row = lax.broadcasted_iota(jnp.int32, (num_experts, span), 0)
        owner = jnp.where(row < n, row * n_local, (row - n) * n_local + 1)
        g_tok = jnp.sum(jnp.where(owner == idx_ref[here, :], found, 0.0), axis=0, keepdims=True)
        prob = prob_ref[:, cols]
        spread = jnp.sum(prob * aux_vec, axis=0, keepdims=True)
        d_logits = ((gate_rows_ref[here, :] * g_tok) * (chosen - prob) + prob * (aux_vec - spread)
                    + ((2.0 * Z_WEIGHT / total_tok) * norm_ref[here, :]) * prob)
        dl_ref[:, cols] = d_logits
        gwr_acc[...] += jnp.dot(jnp.concatenate(split3(d_logits), axis=0), x_ref[cols, :], preferred_element_type=F32)
        return carry

    lax.fori_loop(0, pos_ref.shape[0], router, 0)
    part = gwr_acc[0:num_experts, :] + gwr_acc[num_experts:2 * num_experts, :] + gwr_acc[2 * num_experts:, :]
    d_cols = d_model // LANE
    for d in range(n):
        for c in range(n_local * d_cols):
            r = d * n_local + c // d_cols
            gwr_s[d, c:c + 1, :] = part[r:r + 1, c % d_cols * LANE:(c % d_cols + 1) * LANE]
    gwr_r[me] = gwr_s[me]

    def scatter(k, carry):
        scatter_copy(k).start()
        return carry

    lax.fori_loop(1, n, scatter, 0)
    send_grads(sets[3], 2, 3)

    def gathered(k, carry):
        scatter_copy(k).wait()
        return carry

    lax.fori_loop(1, n, gathered, 0)
    mine = gwr_r[0]
    for i in range(1, n):
        mine = mine + gwr_r[i]
    gwr_mine[...] = mine
    gwr_ref[me] = mine

    def spread_all(k, carry):
        spread_copy(k).start()
        return carry

    lax.fori_loop(1, n, spread_all, 0)
    send_grads(sets[3], 3)

    for queues in sets:
        for queue in queues:
            k, e = queue[-1]
            fwd_copy(k, e, 1).wait_send()
            if queues is not sets[3]:
                ret_copy(k, e).wait_send()
    grads_left(sets[3])
    for queue in sets[3]:
        ret_copy(*queue[-1]).wait_send()
    for k, e in near[0]:
        for part in range(2):
            fwd_copy(k, e, part).wait_send()
        ret_copy(k, e).wait_send()
    for c in own_out:
        c.wait()
    for c in totals:
        c.wait()

    def drain(k, carry):
        gate_copy(k).wait_send()
        spread_copy(k).wait()
        for e in range(n_local):
            ret_copy(k, e).wait_recv()
        return carry

    lax.fori_loop(1, n, drain, 0)


def exchange(xd, gates, stats, w_in, w_out, x_tokens, prob, pos_rows, idx_rows, gate_rows, norm_rows, n_dev):
    n_local, d_model, d_ff = w_in.shape
    cap = xd.shape[3]
    any_spec = pl.BlockSpec(memory_space=pl.ANY)
    vmem_spec = pl.BlockSpec(memory_space=pltpu.VMEM)
    pairs = n_dev * n_local
    dma = pltpu.SemaphoreType.DMA
    return pl.pallas_call(
        functools.partial(exchange_kernel, n_dev, n_local, x_tokens.shape[0] * n_dev),
        out_shape=(jax.ShapeDtypeStruct((n_local, d_model, d_ff), jnp.float32),
                   jax.ShapeDtypeStruct((n_local, d_model, d_ff), jnp.float32),
                   jax.ShapeDtypeStruct((n_dev, n_local, cap, d_model), jnp.bfloat16),
                   jax.ShapeDtypeStruct(prob.shape, jnp.float32),
                   jax.ShapeDtypeStruct((n_dev, 8, LANE), jnp.float32),
                   jax.ShapeDtypeStruct(stats.shape, jnp.float32)),
        in_specs=[any_spec, any_spec, vmem_spec, any_spec, any_spec, any_spec] + [vmem_spec] * 5,
        out_specs=(any_spec, any_spec, any_spec, vmem_spec, vmem_spec, vmem_spec),
        scratch_shapes=[
            pltpu.VMEM(w_in.shape, jnp.bfloat16),
            pltpu.VMEM(w_out.shape, jnp.bfloat16),
            pltpu.VMEM(w_in.shape, jnp.float32),
            pltpu.VMEM(w_in.shape, jnp.float32),
            pltpu.VMEM(x_tokens.shape, jnp.bfloat16),
            pltpu.VMEM((3 * pairs, d_model), jnp.float32),
            pltpu.VMEM((n_dev, 8, LANE), jnp.float32),
            pltpu.VMEM((n_dev, 8, LANE), jnp.float32),
            pltpu.VMEM((8, LANE), jnp.float32),
            pltpu.VMEM((n_dev, n_local, 2, cap, d_model), jnp.bfloat16),
            pltpu.VMEM((n_dev, 8, LANE), jnp.float32),
            pltpu.VMEM((n_dev, 8, LANE), jnp.float32),
            pltpu.VMEM((n_dev, 8, LANE), jnp.float32),
            pltpu.VMEM((n_dev,) + stats.shape, jnp.float32),
            dma((2 * pairs,)), dma((2 * pairs,)), dma((n_dev,)), dma((n_dev,)),
            dma((pairs,)), dma((pairs,)), dma((n_dev,)), dma((n_dev,)),
            dma((n_dev,)), dma((n_dev,)), dma((n_dev,)), dma((n_dev,)), dma((n_dev,)), dma((n_dev,)),
            dma((n_local + 4,)),
        ],
        compiler_params=pltpu.CompilerParams(has_side_effects=True, vmem_limit_bytes=60 * 1024 * 1024),
        name='exchange',
    )(xd, gates, stats, w_in, w_out, x_tokens, prob, pos_rows, idx_rows, gate_rows, norm_rows)


def solution(mesh):
    n_dev = mesh.shape['ep']

    def expert_layer(x_tokens, w_router, expert_idx, w_in, w_out, grad_y):
        tokens, d_model = x_tokens.shape
        n_local = w_in.shape[0]
        num_experts = n_local * n_dev
        capacity = (5 * tokens + 4 * num_experts - 1) // (4 * num_experts)
        total_tok = tokens * n_dev
        lanes = -(-capacity // LANE) * LANE
        idx_rows = expert_idx.reshape(-1, ROW_TOKENS)
        prob, slot_rows, pos_rows, gate_rows, norm_rows, stats = route(x_tokens, idx_rows, w_router, capacity)
        slot_rows = slot_rows.reshape(tokens)
        xd, gates = dispatch(slot_rows, x_tokens, grad_y, gate_rows, n_dev, n_local, capacity, lanes)
        gw_in, gw_out_t, back, d_logits, gwr, stats = exchange(xd, gates, stats, w_in, w_out, x_tokens, prob, pos_rows, idx_rows,
                                                               gate_rows, norm_rows, n_dev)
        grad_x, grad_w_in, grad_w_out = combine(slot_rows, back, d_logits, w_router, gw_in, gw_out_t)
        grad_w_router = gwr[:, :n_local * d_model // LANE].reshape(num_experts, d_model).T

        load_frac = stats[0, :num_experts] / total_tok
        mean_prob = stats[0, num_experts:2 * num_experts] / total_tok
        aux_loss = AUX_WEIGHT * num_experts * jnp.sum(load_frac * mean_prob)
        z_loss = Z_WEIGHT * stats[0, 2 * num_experts] / total_tok
        return grad_x, grad_w_in, grad_w_out, grad_w_router, aux_loss, z_loss

    return jax.shard_map(expert_layer, mesh=mesh,
                         in_specs=(P('ep', None), P(None, None), P('ep'), P('ep', None, None), P('ep', None, None), P('ep', None)),
                         out_specs=(P('ep', None), P('ep', None, None), P('ep', None, None), P(None, None), P(), P()),
                         check_vma=False)
```

```python
import functools

import jax
import jax.numpy as jnp
from jax import lax
from jax.experimental import pallas as pl
from jax.experimental.pallas import tpu as pltpu
from jax.sharding import PartitionSpec as P

AUX_WEIGHT = 0.01
Z_WEIGHT = 0.001
MESH = pl.DeviceIdType.MESH
F_CHUNK = 512
TOKEN_BLOCK = 256
UNROLL = 32
LANE = 128
F32 = jnp.float32
ROW_GROUP = 32
ROW_TOKENS = 1024
GROUP = 2


def nt_dot(a, b):
    return lax.dot_general(a, b, (((1,), (1,)), ((), ())), preferred_element_type=F32)


def eye_mask(rows, cols):
    return lax.broadcasted_iota(jnp.int32, (rows, cols), 0) == lax.broadcasted_iota(jnp.int32, (rows, cols), 1)


def split3(v):
    hi = v.astype(jnp.bfloat16)
    rest = v - hi.astype(jnp.float32)
    mid = rest.astype(jnp.bfloat16)
    low = (rest - mid.astype(jnp.float32)).astype(jnp.bfloat16)
    return hi, mid, low


def route_kernel(capacity, x_ref, idx_ref, wr_ref, prob_ref, slot_ref, pos_ref, gate_ref, norm_ref, stat_ref, seen, prob_sum, z_sum):
    step = pl.program_id(0)
    num_experts, block = prob_ref.shape

    @pl.when(step == 0)
    def _():
        seen[...] = jnp.zeros_like(seen)
        prob_sum[...] = jnp.zeros_like(prob_sum)
        z_sum[...] = jnp.zeros_like(z_sum)

    parts = nt_dot(jnp.concatenate(split3(wr_ref[...]), axis=0), x_ref[...])
    logits = parts[:num_experts] + parts[num_experts:2 * num_experts] + parts[2 * num_experts:]
    top = jnp.max(logits, axis=0, keepdims=True)
    shifted = jnp.exp(logits - top)
    scale = jnp.sum(shifted, axis=0, keepdims=True)
    prob = shifted / scale
    log_norm = top + jnp.log(scale)
    idx = idx_ref[pl.ds(step, 1), :]
    chosen = jnp.where(lax.broadcasted_iota(jnp.int32, (num_experts, block), 0) == idx, 1.0, 0.0)
    prob_ref[...] = prob
    gate_ref[pl.ds(step, 1), :] = jnp.sum(prob * chosen, axis=0, keepdims=True)
    norm_ref[pl.ds(step, 1), :] = log_norm
    squares = log_norm * log_norm
    for i in range(0, block, LANE):
        prob_sum[...] += prob[:, i:i + LANE]
        z_sum[0:1, :] += squares[:, i:i + LANE]
    upto = jnp.where(lax.broadcasted_iota(jnp.int32, (TOKEN_BLOCK, TOKEN_BLOCK), 0)
                     <= lax.broadcasted_iota(jnp.int32, (TOKEN_BLOCK, TOKEN_BLOCK), 1), 1.0, 0.0).astype(jnp.bfloat16)
    before = seen[:, 0:1]
    slots = []
    places = []
    for i in range(0, block, TOKEN_BLOCK):
        part = chosen[:, i:i + TOKEN_BLOCK]
        count = jnp.dot(part.astype(jnp.bfloat16), upto, preferred_element_type=F32) + before
        position = jnp.sum(part * count, axis=0, keepdims=True).astype(jnp.int32) - 1
        places.append(position)
        slots.append(8 * jnp.where(position < capacity, idx[:, i:i + TOKEN_BLOCK] * capacity + position, num_experts * capacity))
        before = count[:, TOKEN_BLOCK - 1:TOKEN_BLOCK]
    slot_ref[pl.ds(step, 1), :] = jnp.concatenate(slots, axis=1)
    pos_ref[pl.ds(step, 1), :] = jnp.concatenate(places, axis=1)
    seen[...] = jnp.broadcast_to(before, seen.shape)

    @pl.when(step == pl.num_programs(0) - 1)
    def _():
        row = lax.broadcasted_iota(jnp.int32, (num_experts, LANE), 0)
        lane = lax.broadcasted_iota(jnp.int32, (num_experts, LANE), 1)
        probs = jnp.sum(prob_sum[...], axis=1, keepdims=True)
        stat_ref[...] = jnp.zeros_like(stat_ref)
        total = jnp.sum(jnp.where(row == lane, seen[...], 0.0) + jnp.where(row + num_experts == lane, probs, 0.0),
                        axis=0, keepdims=True)
        squares = jnp.sum(z_sum[0:1, :], axis=1, keepdims=True)
        stat_ref[0:1, :] = total + jnp.where(lane[0:1, :] == 2 * num_experts, squares, 0.0)


def route(x_tokens, idx_rows, w_router, capacity):
    tokens, d_model = x_tokens.shape
    num_experts = w_router.shape[1]
    steps, block = idx_rows.shape
    rows = lambda dtype: jax.ShapeDtypeStruct((steps, block), dtype)
    whole = pl.BlockSpec((steps, block), lambda i: (0, 0))
    return pl.pallas_call(
        functools.partial(route_kernel, capacity),
        grid=(steps,),
        out_shape=(jax.ShapeDtypeStruct((num_experts, tokens), jnp.float32), rows(jnp.int32), rows(jnp.int32), rows(jnp.float32), rows(jnp.float32),
                   jax.ShapeDtypeStruct((8, LANE), jnp.float32)),
        in_specs=[pl.BlockSpec((block, d_model), lambda i: (i, 0)), whole,
                  pl.BlockSpec((num_experts, d_model), lambda i: (0, 0))],
        out_specs=(pl.BlockSpec((num_experts, block), lambda i: (0, i)), whole, whole, whole, whole,
                   pl.BlockSpec((8, LANE), lambda i: (0, 0))),
        scratch_shapes=[pltpu.VMEM((num_experts, LANE), jnp.float32), pltpu.VMEM((num_experts, LANE), jnp.float32), pltpu.VMEM((8, LANE), jnp.float32)],
        compiler_params=pltpu.CompilerParams(dimension_semantics=('arbitrary',)),
        name='route',
    )(x_tokens, idx_rows, w_router.T)


def dispatch_kernel(steps, capacity, lane_cols, slot_ref, x_ref, dy_ref, gate_ref, xd_ref, gates_ref, table, stage):
    step = pl.program_id(0)
    block, d_model = x_ref.shape
    cols = d_model // LANE
    group, n_local = xd_ref.shape[:2]

    @pl.when(step == 0)
    def _():
        def clear(i, carry):
            table[pl.ds(pl.multiple_of(i * 512, 512), 512), :] = jnp.zeros((512, LANE), jnp.float32)
            return carry
        lax.fori_loop(0, table.shape[0] // 512, clear, 0)

    @pl.when(step < steps)
    def _():
        for r in range(0, block, ROW_GROUP):
            for c in range(2 * cols):
                rows_ref = x_ref if c < cols else dy_ref
                span = slice(c % cols * LANE, (c % cols + 1) * LANE)
                stage[pl.ds(r * 8 + c, ROW_GROUP, stride=8), :] = rows_ref[r:r + ROW_GROUP, span].astype(jnp.float32)
        eye = eye_mask(LANE, LANE)
        gate_row = gate_ref[pl.ds(step, 1), :]
        for i in range(0, block, LANE):
            gate = jnp.sum(jnp.where(eye, gate_row[:, i:i + LANE], 0.0), axis=1, keepdims=True)
            stage[pl.ds(i * 8 + 2 * cols, LANE, stride=8), :] = jnp.broadcast_to(gate, (LANE, LANE))

        def place(i, carry):
            for u in range(UNROLL):
                t = i * UNROLL + u
                slot = slot_ref[step * block + t]
                table[pl.ds(pl.multiple_of(slot, 8), 8), :] = stage[pl.ds(pl.multiple_of(t * 8, 8), 8), :]
            return carry
        lax.fori_loop(0, block // UNROLL, place, 0)

    @pl.when(step >= steps)
    def _():
        gates_ref[...] = jnp.zeros_like(gates_ref)
        row = lax.broadcasted_iota(jnp.int32, (capacity, LANE), 0)
        lane = lax.broadcasted_iota(jnp.int32, (capacity, LANE), 1)

        def unload(i, carry):
            d = i // n_local
            e = i % n_local
            first = (((step - steps) * group + d) * n_local + e) * (capacity * 8)
            for r in range(0, capacity, ROW_GROUP):
                for c in range(2 * cols):
                    span = slice(c % cols * LANE, (c % cols + 1) * LANE)
                    xd_ref[d, e, c // cols, r:r + ROW_GROUP, span] = table[
                        pl.ds(first + r * 8 + c, ROW_GROUP, stride=8), :].astype(jnp.bfloat16)
            gate = table[pl.ds(first + 2 * cols, capacity, stride=8), :]
            for c in range(lane_cols):
                gates_ref[d, pl.ds(e * lane_cols + c, 1), :] = jnp.sum(
                    jnp.where(row == lane + c * LANE, gate, 0.0), axis=0, keepdims=True)
            return carry
        lax.fori_loop(0, group * n_local, unload, 0)


def dispatch(slot_rows, x_tokens, grad_y, gate_rows, n_dev, n_local, capacity, lanes):
    tokens, d_model = x_tokens.shape
    steps, block = gate_rows.shape
    n_slots = n_dev * n_local * capacity
    table_rows = -(-(n_slots + 1) * 8 // 512) * 512
    tok = lambda i: (jnp.minimum(i, steps - 1), 0)
    dst = lambda i: jnp.maximum(i - steps, 0)
    return pl.pallas_call(
        functools.partial(dispatch_kernel, steps, capacity, lanes // LANE),
        grid=(steps + n_dev // GROUP,),
        out_shape=(jax.ShapeDtypeStruct((n_dev, n_local, 2, capacity, d_model), jnp.bfloat16),
                   jax.ShapeDtypeStruct((n_dev, 8, LANE), jnp.float32)),
        in_specs=[pl.BlockSpec(memory_space=pltpu.SMEM),
                  pl.BlockSpec((block, d_model), tok),
                  pl.BlockSpec((block, d_model), tok),
                  pl.BlockSpec((steps, block), lambda i: (0, 0))],
        out_specs=(pl.BlockSpec((GROUP, n_local, 2, capacity, d_model), lambda i: (dst(i), 0, 0, 0, 0)),
                   pl.BlockSpec((GROUP, 8, LANE), lambda i: (dst(i), 0, 0))),
        scratch_shapes=[pltpu.VMEM((table_rows, LANE), jnp.float32),
                        pltpu.VMEM((block * 8, LANE), jnp.float32)],
        compiler_params=pltpu.CompilerParams(dimension_semantics=('arbitrary',), vmem_limit_bytes=62 * 1024 * 1024),
        name='dispatch',
    )(slot_rows, x_tokens, grad_y, gate_rows)


def combine_kernel(fills, sources, capacity, slot_ref, back_ref, dl_ref, wr_t_ref, gwi_ref, gwo_t_ref,
                   gx_ref, gwi_out_ref, gwo_out_ref, table, stage):
    step = pl.program_id(0)
    block, d_model = gx_ref.shape
    cols = d_model // LANE
    group, n_local = back_ref.shape[:2]
    n_slots = sources * n_local * capacity
    gwi_out_ref[...] = gwi_ref[...]
    gwo_out_ref[0] = gwo_t_ref[0].T

    @pl.when(step == 0)
    def _():
        table[pl.ds(n_slots * 8, 8), :] = jnp.zeros((8, LANE), jnp.float32)

    @pl.when(step < fills)
    def _():
        def load(i, carry):
            d = i // n_local
            e = i % n_local
            first = ((step * group + d) * n_local + e) * (capacity * 8)
            for r in range(0, capacity, ROW_GROUP):
                for c in range(cols):
                    table[pl.ds(first + r * 8 + c, ROW_GROUP, stride=8), :] = back_ref[
                        d, e, r:r + ROW_GROUP, c * LANE:(c + 1) * LANE].astype(jnp.float32)
            return carry
        lax.fori_loop(0, group * n_local, load, 0)

    @pl.when(step >= fills)
    def _():
        part = step - fills

        def pick(i, carry):
            for u in range(UNROLL):
                t = i * UNROLL + u
                slot = slot_ref[part * block + t]
                stage[pl.ds(pl.multiple_of(t * 8, 8), 8), :] = table[pl.ds(pl.multiple_of(slot, 8), 8), :]
            return carry
        lax.fori_loop(0, block // UNROLL, pick, 0)
        hi, mid, low = split3(dl_ref[...])
        left = jnp.concatenate([hi, mid, hi, low, mid, hi], axis=0)
        w_hi, w_mid, w_low = split3(wr_t_ref[...])
        right = jnp.concatenate([w_hi, w_hi, w_mid, w_hi, w_mid, w_low], axis=0)
        dx_router = lax.dot_general(left, right, (((0,), (0,)), ((), ())), preferred_element_type=F32)
        for r in range(0, block, ROW_GROUP):
            for c in range(cols):
                span = slice(c * LANE, (c + 1) * LANE)
                gx_ref[r:r + ROW_GROUP, span] = (stage[pl.ds(r * 8 + c, ROW_GROUP, stride=8), :]
                                                 + dx_router[r:r + ROW_GROUP, span]).astype(jnp.bfloat16)


def combine(slot_rows, back, d_logits, w_router, gw_in, gw_out_t):
    n_dev, n_local, capacity, d_model = back.shape
    num_experts, tokens = d_logits.shape
    d_ff = gw_in.shape[2]
    block = ROW_TOKENS
    blocks = tokens // block
    fills = n_dev // GROUP
    steps = fills + blocks
    n_slots = n_dev * n_local * capacity
    gw_in_rows = gw_in.reshape(n_local * d_model, d_ff)
    in_rows = n_local * d_model // steps
    out_cols = d_ff // 256
    src = lambda i: jnp.minimum(i, fills - 1)
    tok = lambda i: (jnp.maximum(i - fills, 0), 0)
    flip = lambda i: jnp.minimum(i, n_local * out_cols - 1)
    gx, gw_in_out, gw_out = pl.pallas_call(
        functools.partial(combine_kernel, fills, n_dev, capacity),
        grid=(steps,),
        out_shape=(jax.ShapeDtypeStruct((tokens, d_model), jnp.bfloat16),
                   jax.ShapeDtypeStruct((n_local * d_model, d_ff), jnp.float32),
                   jax.ShapeDtypeStruct((n_local, d_ff, d_model), jnp.float32)),
        in_specs=[pl.BlockSpec(memory_space=pltpu.SMEM),
                  pl.BlockSpec((GROUP, n_local, capacity, d_model), lambda i: (src(i), 0, 0, 0)),
                  pl.BlockSpec((num_experts, block), lambda i: (0, jnp.maximum(i - fills, 0))),
                  pl.BlockSpec((num_experts, d_model), lambda i: (0, 0)),
                  pl.BlockSpec((in_rows, d_ff), lambda i: (i, 0)),
                  pl.BlockSpec((1, d_model, 256), lambda i: (flip(i) // out_cols, 0, flip(i) % out_cols))],
        out_specs=(pl.BlockSpec((block, d_model), tok),
                   pl.BlockSpec((in_rows, d_ff), lambda i: (i, 0)),
                   pl.BlockSpec((1, 256, d_model), lambda i: (flip(i) // out_cols, flip(i) % out_cols, 0))),
        scratch_shapes=[pltpu.VMEM(((n_slots + 1) * 8, LANE), jnp.float32),
                        pltpu.VMEM((block * 8, LANE), jnp.float32)],
        compiler_params=pltpu.CompilerParams(dimension_semantics=('arbitrary',), vmem_limit_bytes=63 * 1024 * 1024),
        name='combine',
    )(slot_rows, back, d_logits, w_router.T, gw_in_rows, gw_out_t)
    return gx, gw_in_out.reshape(n_local, d_model, d_ff), gw_out


def flip_bits(me, k, n):
    out = 0
    bit = 1
    while bit < n:
        mine = (me // bit) % 2
        flip = (k // bit) % 2
        out = out + bit * (mine + flip - 2 * mine * flip)
        bit *= 2
    return out


def tile_at(t):
    quarter = t // 4
    edge = (7 - quarter) // 7 + quarter // 7
    turn = (t + 4) % 8
    piece = (1 - edge) * (turn // 2) + edge * (t % 4)
    stage = (t + 4) // 8
    chip = stage * (7 - stage) // 2 + stage // 4
    chip = chip + (1 - edge) * (turn % 2) * (7 - 2 * chip)
    return chip * 2 + piece // 2, piece % 2


def link_sets(n, n_local):
    assert n == 16
    pieces = []
    for chips in ((3, 4), (5, 2), (6, 1), (7,)):
        pieces.append([[(chip * 2 + c, e) for c in range(2) for e in range(n_local)] for chip in chips])
    return pieces


def exchange_kernel(n, n_local, total_tok, xd_ref, gate_ref, stat_ref, w_in_hbm, w_out_hbm,
                    x_hbm, prob_ref, pos_ref, idx_ref, gate_rows_ref, norm_ref,
                    gw_in_hbm, gw_out_t_hbm, back_ref, dl_ref, gwr_ref, stat_out_ref,
                    w_in_ref, w_out_ref, gw_in_ref, gw_out_t_ref, x_ref, gwr_acc, gwr_s, gwr_r, gwr_mine,
                    xr, gate_r, g_s, g_r, stat_r,
                    fwd_send, fwd_recv, gate_send, gate_recv,
                    ret_send, ret_recv, g_send, g_recv, stat_send, stat_recv, a_send, a_recv, b_send, b_recv, loc_sem):
    me = lax.axis_index('ep')
    cap, d_model = xr.shape[3], xr.shape[4]
    d_ff = w_in_ref.shape[2]

    def peer_of(k):
        return flip_bits(me, k, n)

    def fwd_copy(k, e, part):
        sem = (k * n_local + e) * 2 + part
        peer = peer_of(k)
        return pltpu.make_async_remote_copy(
            src_ref=xd_ref.at[peer, e, part], dst_ref=xr.at[k, e, part],
            send_sem=fwd_send.at[sem], recv_sem=fwd_recv.at[sem],
            device_id=(peer,), device_id_type=MESH)

    def gate_copy(k):
        peer = peer_of(k)
        return pltpu.make_async_remote_copy(
            src_ref=gate_ref.at[peer], dst_ref=gate_r.at[k],
            send_sem=gate_send.at[k], recv_sem=gate_recv.at[k],
            device_id=(peer,), device_id_type=MESH)

    def stat_copy(k):
        return pltpu.make_async_remote_copy(
            src_ref=stat_ref, dst_ref=stat_r.at[me],
            send_sem=stat_send.at[k], recv_sem=stat_recv.at[k],
            device_id=(peer_of(k),), device_id_type=MESH)

    def ret_copy(k, e):
        sem = k * n_local + e
        return pltpu.make_async_remote_copy(
            src_ref=xr.at[k, e, 0], dst_ref=back_ref.at[me, e],
            send_sem=ret_send.at[sem], recv_sem=ret_recv.at[sem],
            device_id=(peer_of(k),), device_id_type=MESH)

    def g_copy(k):
        return pltpu.make_async_remote_copy(
            src_ref=g_s.at[k], dst_ref=g_r.at[me],
            send_sem=g_send.at[k], recv_sem=g_recv.at[k],
            device_id=(peer_of(k),), device_id_type=MESH)

    def scatter_copy(k):
        peer = peer_of(k)
        return pltpu.make_async_remote_copy(
            src_ref=gwr_s.at[peer], dst_ref=gwr_r.at[me], send_sem=a_send.at[k], recv_sem=a_recv.at[k],
            device_id=(peer,), device_id_type=MESH)

    def spread_copy(k):
        return pltpu.make_async_remote_copy(
            src_ref=gwr_mine, dst_ref=gwr_ref.at[me], send_sem=b_send.at[k], recv_sem=b_recv.at[k],
            device_id=(peer_of(k),), device_id_type=MESH)

    sets = link_sets(n, n_local)

    def interleave(queues):
        return [queue[i] for i in range(len(queues[0])) for queue in queues]

    def send_rows(queues):
        for k, e in interleave(queues):
            if e == 0:
                gate_copy(k).start()
                stat_copy(k).start()
            for part in range(2):
                fwd_copy(k, e, part).start()

    def rows_left(queues):
        for queue in queues:
            for k, e in queue[:-1]:
                for part in range(2):
                    fwd_copy(k, e, part).wait_send()

    def send_grads(queues, lo=0, hi=None):
        for k, e in interleave(queues)[lo:hi]:
            ret_copy(k, e).start()

    def grads_left(queues):
        for queue in queues:
            for k, e in queue[:-1]:
                ret_copy(k, e).wait_send()

    near = [[(1, e) for e in range(n_local)]]
    own_in = [pltpu.make_async_copy(xd_ref.at[me, e], xr.at[0, e], loc_sem.at[e]) for e in range(n_local)]
    own_gate = pltpu.make_async_copy(gate_ref.at[me], gate_r.at[0], loc_sem.at[n_local])
    own_out = [pltpu.make_async_copy(xr.at[0, e, 0], back_ref.at[me, e], loc_sem.at[e]) for e in range(n_local)]
    load_x = pltpu.make_async_copy(x_hbm, x_ref, loc_sem.at[n_local + 3])

    send_rows(sets[0])
    send_rows(near)
    for c in own_in:
        c.start()
    own_gate.start()
    weights = [pltpu.make_async_copy(w_in_hbm, w_in_ref, loc_sem.at[n_local + 1]),
               pltpu.make_async_copy(w_out_hbm, w_out_ref, loc_sem.at[n_local + 2])]
    for c in weights:
        c.start()
    load_x.start()
    gwr_s[...] = jnp.zeros_like(gwr_s)
    gw_in_ref[...] = jnp.zeros_like(gw_in_ref)
    gw_out_t_ref[...] = jnp.zeros_like(gw_out_t_ref)
    g_s[...] = jnp.zeros_like(g_s)
    stat_r[me] = stat_ref[...]
    for c in own_in:
        c.wait()
    own_gate.wait()
    for c in weights:
        c.wait()

    lane_cols = -(-cap // LANE)
    lanes = lane_cols * LANE

    def tile(k, e):
        eye = (lax.broadcasted_iota(jnp.int32, (cap, lanes), 0)
               == lax.broadcasted_iota(jnp.int32, (cap, lanes), 1))
        rows = xr[k, e, 0]
        dy = xr[k, e, 1].astype(jnp.float32)
        gate_row = jnp.concatenate([gate_r[k, pl.ds(e * lane_cols + c, 1), :] for c in range(lane_cols)], axis=1)
        gate_col = jnp.sum(jnp.where(eye, gate_row, 0.0), axis=1, keepdims=True)
        grad = (gate_col * dy).astype(jnp.bfloat16)
        rows_t = rows.T
        grad_t = grad.T
        out = jnp.zeros((cap, d_model), jnp.float32)
        d_rows = jnp.zeros((cap, d_model), jnp.float32)
        for f in range(0, d_ff, F_CHUNK):
            fs = pl.ds(f, F_CHUNK)
            w_a = w_in_ref[e, :, fs]
            w_b = w_out_ref[e, fs, :]
            pre = jnp.dot(rows, w_a, preferred_element_type=F32)
            hid = jnp.maximum(pre, 0.0).astype(jnp.bfloat16)
            out = out + jnp.dot(hid, w_b, preferred_element_type=F32)
            d_hid = nt_dot(grad, w_b)
            d_pre = jnp.where(hid.astype(jnp.float32) > 0, d_hid, 0.0).astype(jnp.bfloat16)
            gw_out_t_ref[e, :, fs] += jnp.dot(grad_t, hid, preferred_element_type=F32)
            gw_in_ref[e, :, fs] += jnp.dot(rows_t, d_pre, preferred_element_type=F32)
            d_rows = d_rows + nt_dot(d_pre, w_a)
        out = out.astype(jnp.bfloat16).astype(jnp.float32)
        g_col = jnp.sum(out * dy, axis=1, keepdims=True)
        g_row = jnp.sum(jnp.where(eye, g_col, 0.0), axis=0, keepdims=True)
        for c in range(lane_cols):
            g_s[k, pl.ds(e * lane_cols + c, 1), :] = g_row[:, c * LANE:(c + 1) * LANE]
        xr[k, e, 0] = d_rows.astype(jnp.bfloat16)

    order = [(0, e) for e in range(n_local)] + near[0]
    first = []
    for queues in sets:
        first.append(len(order))
        order = order + interleave(queues)
    assert order == [tile_at(t) for t in range(len(order))]

    def own_back():
        send_grads(near)
        for c in own_out:
            c.start()

    def after_rows(done, then):
        def run():
            rows_left(sets[done])
            then()
        return run

    def after_grads(done, then):
        def run():
            grads_left(sets[done])
            then()
        return run

    events = {
        first[0]: own_back,
        first[1] - 2: after_rows(0, lambda: send_rows(sets[1])),
        first[2] - 2: after_rows(1, lambda: send_grads(sets[0])),
        first[2]: after_grads(0, lambda: send_rows(sets[2])),
        first[3] - 2: after_rows(2, lambda: send_grads(sets[1])),
        first[3]: after_grads(1, lambda: send_rows(sets[3])),
        len(order) - 1: after_rows(3, lambda: send_grads(sets[2], 0, 4)),
    }

    def step(t, carry):
        k, e = tile_at(t)
        for at, run in events.items():
            pl.when(t == at)(run)

        @pl.when(t >= n_local)
        def _():
            @pl.when(e == 0)
            def _():
                gate_copy(k).wait_recv()
            for part in range(2):
                fwd_copy(k, e, part).wait_recv()

        tile(k, e)

        @pl.when(t >= n_local)
        def _():
            @pl.when(e == n_local - 1)
            def _():
                g_copy(k).start()
        return carry

    lax.fori_loop(0, len(order), step, 0)
    send_grads(sets[2], 4)
    totals = [pltpu.make_async_copy(gw_in_ref, gw_in_hbm, loc_sem.at[n_local + 1]),
              pltpu.make_async_copy(gw_out_t_ref, gw_out_t_hbm, loc_sem.at[n_local + 2])]
    for c in totals:
        c.start()
    load_x.wait()
    g_r[me] = g_s[0]
    grads_left(sets[2])
    send_grads(sets[3], 0, 2)

    def arrive(k, carry):
        stat_copy(k).wait()
        g_copy(k).wait()
        return carry

    lax.fori_loop(1, n, arrive, 0)
    stat = stat_r[0]
    for i in range(1, n):
        stat = stat + stat_r[i]
    stat_out_ref[...] = stat
    num_experts = n * n_local
    load = jnp.sum(jnp.where(eye_mask(num_experts, LANE), stat[0:1, :], 0.0), axis=1, keepdims=True)
    aux_vec = (AUX_WEIGHT * num_experts / total_tok) * (load / total_tok)
    g_all = jnp.concatenate([
        jnp.concatenate([g_r[:, e * lane_cols + c, :] for c in range(lane_cols)], axis=1) for e in range(n_local)], axis=0)
    g_parts = jnp.concatenate(split3(g_all), axis=0)
    span = pos_ref.shape[1]
    gwr_acc[...] = jnp.zeros_like(gwr_acc)

    def router(c, carry):
        here = pl.ds(c, 1)
        cols = pl.ds(pl.multiple_of(c * span, span), span)
        place = jnp.where(lax.broadcasted_iota(jnp.int32, (lanes, span), 0) == pos_ref[here, :], 1.0, 0.0)
        found = jnp.dot(g_parts, place.astype(jnp.bfloat16), preferred_element_type=F32)
        found = found[:num_experts] + found[num_experts:2 * num_experts] + found[2 * num_experts:]
        chosen = jnp.where(lax.broadcasted_iota(jnp.int32, (num_experts, span), 0) == idx_ref[here, :], 1.0, 0.0)
        row = lax.broadcasted_iota(jnp.int32, (num_experts, span), 0)
        owner = jnp.where(row < n, row * n_local, (row - n) * n_local + 1)
        g_tok = jnp.sum(jnp.where(owner == idx_ref[here, :], found, 0.0), axis=0, keepdims=True)
        prob = prob_ref[:, cols]
        spread = jnp.sum(prob * aux_vec, axis=0, keepdims=True)
        d_logits = ((gate_rows_ref[here, :] * g_tok) * (chosen - prob) + prob * (aux_vec - spread)
                    + ((2.0 * Z_WEIGHT / total_tok) * norm_ref[here, :]) * prob)
        dl_ref[:, cols] = d_logits
        gwr_acc[...] += jnp.dot(jnp.concatenate(split3(d_logits), axis=0), x_ref[cols, :], preferred_element_type=F32)
        return carry

    lax.fori_loop(0, pos_ref.shape[0], router, 0)
    part = gwr_acc[0:num_experts, :] + gwr_acc[num_experts:2 * num_experts, :] + gwr_acc[2 * num_experts:, :]
    d_cols = d_model // LANE
    for d in range(n):
        for c in range(n_local * d_cols):
            r = d * n_local + c // d_cols
            gwr_s[d, c:c + 1, :] = part[r:r + 1, c % d_cols * LANE:(c % d_cols + 1) * LANE]
    gwr_r[me] = gwr_s[me]

    def scatter(k, carry):
        scatter_copy(k).start()
        return carry

    lax.fori_loop(1, n, scatter, 0)
    send_grads(sets[3], 2, 3)

    def gathered(k, carry):
        scatter_copy(k).wait()
        return carry

    lax.fori_loop(1, n, gathered, 0)
    mine = gwr_r[0]
    for i in range(1, n):
        mine = mine + gwr_r[i]
    gwr_mine[...] = mine
    gwr_ref[me] = mine

    def spread_all(k, carry):
        spread_copy(k).start()
        return carry

    lax.fori_loop(1, n, spread_all, 0)
    send_grads(sets[3], 3)

    for queues in sets:
        for queue in queues:
            k, e = queue[-1]
            for part in range(2):
                fwd_copy(k, e, part).wait_send()
            if queues is not sets[3]:
                ret_copy(k, e).wait_send()
    grads_left(sets[3])
    for queue in sets[3]:
        ret_copy(*queue[-1]).wait_send()
    for k, e in near[0]:
        for part in range(2):
            fwd_copy(k, e, part).wait_send()
        ret_copy(k, e).wait_send()
    for c in own_out:
        c.wait()
    for c in totals:
        c.wait()

    def drain(k, carry):
        gate_copy(k).wait_send()
        spread_copy(k).wait()
        for e in range(n_local):
            ret_copy(k, e).wait_recv()
        return carry

    lax.fori_loop(1, n, drain, 0)


def exchange(xd, gates, stats, w_in, w_out, x_tokens, prob, pos_rows, idx_rows, gate_rows, norm_rows, n_dev):
    n_local, d_model, d_ff = w_in.shape
    cap = xd.shape[3]
    any_spec = pl.BlockSpec(memory_space=pl.ANY)
    vmem_spec = pl.BlockSpec(memory_space=pltpu.VMEM)
    pairs = n_dev * n_local
    dma = pltpu.SemaphoreType.DMA
    return pl.pallas_call(
        functools.partial(exchange_kernel, n_dev, n_local, x_tokens.shape[0] * n_dev),
        out_shape=(jax.ShapeDtypeStruct((n_local, d_model, d_ff), jnp.float32),
                   jax.ShapeDtypeStruct((n_local, d_model, d_ff), jnp.float32),
                   jax.ShapeDtypeStruct((n_dev, n_local, cap, d_model), jnp.bfloat16),
                   jax.ShapeDtypeStruct(prob.shape, jnp.float32),
                   jax.ShapeDtypeStruct((n_dev, 8, LANE), jnp.float32),
                   jax.ShapeDtypeStruct(stats.shape, jnp.float32)),
        in_specs=[any_spec, any_spec, vmem_spec, any_spec, any_spec, any_spec] + [vmem_spec] * 5,
        out_specs=(any_spec, any_spec, any_spec, vmem_spec, vmem_spec, vmem_spec),
        scratch_shapes=[
            pltpu.VMEM(w_in.shape, jnp.bfloat16),
            pltpu.VMEM(w_out.shape, jnp.bfloat16),
            pltpu.VMEM(w_in.shape, jnp.float32),
            pltpu.VMEM(w_in.shape, jnp.float32),
            pltpu.VMEM(x_tokens.shape, jnp.bfloat16),
            pltpu.VMEM((3 * pairs, d_model), jnp.float32),
            pltpu.VMEM((n_dev, 8, LANE), jnp.float32),
            pltpu.VMEM((n_dev, 8, LANE), jnp.float32),
            pltpu.VMEM((8, LANE), jnp.float32),
            pltpu.VMEM((n_dev, n_local, 2, cap, d_model), jnp.bfloat16),
            pltpu.VMEM((n_dev, 8, LANE), jnp.float32),
            pltpu.VMEM((n_dev, 8, LANE), jnp.float32),
            pltpu.VMEM((n_dev, 8, LANE), jnp.float32),
            pltpu.VMEM((n_dev,) + stats.shape, jnp.float32),
            dma((2 * pairs,)), dma((2 * pairs,)), dma((n_dev,)), dma((n_dev,)),
            dma((pairs,)), dma((pairs,)), dma((n_dev,)), dma((n_dev,)),
            dma((n_dev,)), dma((n_dev,)), dma((n_dev,)), dma((n_dev,)), dma((n_dev,)), dma((n_dev,)),
            dma((n_local + 4,)),
        ],
        compiler_params=pltpu.CompilerParams(has_side_effects=True, vmem_limit_bytes=60 * 1024 * 1024),
        name='exchange',
    )(xd, gates, stats, w_in, w_out, x_tokens, prob, pos_rows, idx_rows, gate_rows, norm_rows)


def solution(mesh):
    n_dev = mesh.shape['ep']

    def expert_layer(x_tokens, w_router, expert_idx, w_in, w_out, grad_y):
        tokens, d_model = x_tokens.shape
        n_local = w_in.shape[0]
        num_experts = n_local * n_dev
        capacity = (5 * tokens + 4 * num_experts - 1) // (4 * num_experts)
        total_tok = tokens * n_dev
        lanes = -(-capacity // LANE) * LANE
        idx_rows = expert_idx.reshape(-1, ROW_TOKENS)
        prob, slot_rows, pos_rows, gate_rows, norm_rows, stats = route(x_tokens, idx_rows, w_router, capacity)
        slot_rows = slot_rows.reshape(tokens)
        xd, gates = dispatch(slot_rows, x_tokens, grad_y, gate_rows, n_dev, n_local, capacity, lanes)
        gw_in, gw_out_t, back, d_logits, gwr, stats = exchange(xd, gates, stats, w_in, w_out, x_tokens, prob, pos_rows, idx_rows,
                                                               gate_rows, norm_rows, n_dev)
        grad_x, grad_w_in, grad_w_out = combine(slot_rows, back, d_logits, w_router, gw_in, gw_out_t)
        grad_w_router = gwr[:, :n_local * d_model // LANE].reshape(num_experts, d_model).T

        load_frac = stats[0, :num_experts] / total_tok
        mean_prob = stats[0, num_experts:2 * num_experts] / total_tok
        aux_loss = AUX_WEIGHT * num_experts * jnp.sum(load_frac * mean_prob)
        z_loss = Z_WEIGHT * stats[0, 2 * num_experts] / total_tok
        return grad_x, grad_w_in, grad_w_out, grad_w_router, aux_loss, z_loss

    return jax.shard_map(expert_layer, mesh=mesh,
                         in_specs=(P('ep', None), P(None, None), P('ep'), P('ep', None, None), P('ep', None, None), P('ep', None)),
                         out_specs=(P('ep', None), P('ep', None, None), P('ep', None, None), P(None, None), P(), P()),
                         check_vma=False)
```
